32 devices in a mesh: col: 16 (over z, x, core), row: 2 (over y).
Axes of the slice: x: 2, y: 2, z: 4, core: 2. Of those that a mesh axis runs over, the one named last changes fastest.
Arguments:
- hidden: bfloat16 [32768, 768], P(('col', 'row')), may hold values from -6 to 6
- cotangent: bfloat16 [32768, 768], P(('col', 'row')), may hold values from -6 to 6
- rand_blocks: int32 [32, 14, 12, 3], P(('col', 'row')), may hold values from 1 to 14, as said below
- w_query: bfloat16 [768, 768], P('col', 'row'), may hold values from -0.21875 to 0.21875
- w_key: bfloat16 [768, 768], P('col', 'row'), may hold values from -0.21875 to 0.21875
- w_value: bfloat16 [768, 768], P('col', 'row'), may hold values from -0.21875 to 0.21875
- w_out: bfloat16 [768, 768], P('row', 'col'), may hold values from -2.5 to 2.5
- w_up: bfloat16 [768, 3072], P('col', 'row'), may hold values from -0.21875 to 0.21875
- w_down: bfloat16 [3072, 768], P('row', 'col'), may hold values from -0.109375 to 0.109375
- query_bias: bfloat16 [768], P('row'), may hold values from -3 to 3
- value_bias: bfloat16 [768], P('row'), may hold values from -3 to 3
- out_bias: bfloat16 [768], P('row'), may hold values from -2 to 2
- up_bias: bfloat16 [3072], P('row'), may hold values from -3 to 3
- down_bias: bfloat16 [768], P('row'), may hold values from -2 to 2
- norm1_gain: bfloat16 [768], P('row'), may hold values from 0.5 to 1.5
- norm1_shift: bfloat16 [768], P('row'), may hold values from -2 to 2
- norm2_gain: bfloat16 [768], P('row'), may hold values from 0.5 to 1.5
- norm2_shift: bfloat16 [768], P('row'), may hold values from -2 to 2
Outputs:
- output: float32 [32768, 768], P(('col', 'row'))
- hidden_grad: float32 [32768, 768], P(('col', 'row'))
- grad_query: float32 [768, 768], P('col', 'row')
- grad_key: float32 [768, 768], P('col', 'row')
- grad_value: float32 [768, 768], P('col', 'row')
- grad_out: float32 [768, 768], P('row', 'col')
- grad_up: float32 [768, 3072], P('col', 'row')
- grad_down: float32 [3072, 768], P('row', 'col')
- grad_query_bias: float32 [768], P('row')
- grad_value_bias: float32 [768], P('row')
- grad_out_bias: float32 [768], P('row')
- grad_up_bias: float32 [3072], P('row')
- grad_down_bias: float32 [768], P('row')
- grad_norm1_gain: float32 [768], P('row')
- grad_norm1_shift: float32 [768], P('row')
- grad_norm2_gain: float32 [768], P('row')
- grad_norm2_shift: float32 [768], P('row')
The draws below stay inside these ranges and needn't reach their ends.
Inputs may be any that keep to these rules, and one draw needn't show every extreme that they name: `rand_blocks`: for sequence s, middle query block i (entry i - 1 of the second dimension) and head h, the 3 entries are different blocks, none of them 0, 15, i - 1, i or i + 1.
All inputs are finite; a program needn't handle non-finite values.
Results may differ from the reference program's by a relative error of at most 0.019.
Values may be sent and summed in bfloat16 or wider, within the bound.
A program may use at most 384 MiB of HBM per device.

```python
import math
import jax
import jax.numpy as jnp
from jax import lax

D = 768
H = 12
FF = 3072
BLK = 64
RAND = 3
LENGTH = 1024
SEQS = 32
TOKENS = 32768


def draw_rand_blocks(key, part):
    blocks = LENGTH // BLK
    rows = jnp.arange(1, blocks - 1, dtype=jnp.int32)
    columns = jnp.arange(blocks, dtype=jnp.int32)
    scores = jax.random.randint(key, (SEQS, blocks - 2, H, blocks), 0, 1 << 20, dtype=jnp.int32)
    scores = scores * blocks + columns
    near = jnp.abs(columns[None, :] - rows[:, None]) <= 1
    edge = (columns == 0) | (columns == blocks - 1)
    banned = near | edge[None, :]
    scores = jnp.where(banned[None, :, None, :], -1, scores)
    picked_scores, picked = lax.top_k(scores, RAND)
    return picked.astype(jnp.int32)


def block_scale(key, shape, split, least, largest):
    loudness, own = 1.0, jax.random.fold_in(key, 6)
    for axis_at, parts in split:
        heights = jnp.exp(jax.random.uniform(jax.random.fold_in(own, axis_at), (parts,), jnp.float32, least / len(split), largest / len(split)))
        loudness = loudness * jnp.repeat(heights, shape[axis_at] // parts).reshape([-1 if axis == axis_at else 1 for axis in range(len(shape))])
    return loudness


def gaussian(stream_key, extent, deviation, most, cuts=(), kind=jnp.bfloat16):
    loudness = block_scale(stream_key, extent, cuts, -0.22, 0.18) if cuts else 1.0
    array = jax.random.normal(stream_key, extent, jnp.float32) * deviation * loudness
    return jnp.minimum(jnp.maximum(array, -most), most).astype(kind)


def setup_inputs(seed: int = 0) -> dict:
    splits = jax.random.split(jax.random.key(seed), 19)
    hidden = gaussian(splits[0], (TOKENS, D), 1.0, 6.0, ((0, 32),))
    cotangent = gaussian(splits[1], (TOKENS, D), 1.0, 6.0, ((0, 32),))
    rand_blocks = draw_rand_blocks(jax.random.fold_in(splits[18], 71), 0)
    w_query = gaussian(splits[3], (D, D), D ** -0.5, 0.21875, ((0, 16), (1, 2)))
    w_key = gaussian(splits[4], (D, D), D ** -0.5, 0.21875, ((0, 16), (1, 2)))
    w_value = gaussian(splits[5], (D, D), D ** -0.5, 0.21875, ((0, 16), (1, 2)))
    w_out = gaussian(splits[6], (D, D), (max(D // 128, 1)) ** -0.5, 2.5, ((0, 2), (1, 16)))
    w_up = gaussian(splits[7], (D, FF), D ** -0.5, 0.21875, ((0, 16), (1, 2)))
    w_down = gaussian(splits[8], (FF, D), FF ** -0.5, 0.109375, ((0, 2), (1, 16)))
    query_bias = gaussian(splits[9], (D,), 0.5, 3.0, ((0, 2),))
    value_bias = gaussian(splits[10], (D,), 0.5, 3.0, ((0, 2),))
    out_bias = gaussian(splits[11], (D,), 0.3, 2.0, ((0, 2),))
    up_bias = gaussian(splits[12], (FF,), 0.5, 3.0, ((0, 2),))
    down_bias = gaussian(splits[13], (D,), 0.3, 2.0, ((0, 2),))
    norm1_gain = jnp.clip(1.0 + 0.1 * jax.random.normal(splits[14], (D,), jnp.float32), 0.5, 1.5).astype(jnp.bfloat16)
    norm1_shift = gaussian(splits[15], (D,), 0.3, 2.0, ((0, 2),))
    norm2_gain = jnp.clip(1.0 + 0.1 * jax.random.normal(splits[16], (D,), jnp.float32), 0.5, 1.5).astype(jnp.bfloat16)
    norm2_shift = gaussian(splits[17], (D,), 0.3, 2.0, ((0, 2),))
    return {"hidden": hidden, "cotangent": cotangent, "rand_blocks": rand_blocks, "w_query": w_query, "w_key": w_key, "w_value": w_value, "w_out": w_out, "w_up": w_up, "w_down": w_down, "query_bias": query_bias, "value_bias": value_bias, "out_bias": out_bias, "up_bias": up_bias, "down_bias": down_bias, "norm1_gain": norm1_gain, "norm1_shift": norm1_shift, "norm2_gain": norm2_gain, "norm2_shift": norm2_shift}


EPS = 1e-12
NEG = -1e+30

@jax.custom_vjp
def low(v):
    return lax.optimization_barrier(v.astype(jnp.bfloat16)).astype(jnp.float32)

@jax.custom_vjp
def low_back(v):
    return v

def low_keep(v):
    return (low(v), None)

def low_pass(kept, grad):
    return (grad,)

def back_keep(v):
    return (v, None)

def back_low(kept, grad):
    return (low(grad),)
low.defvjp(low_keep, low_pass)
low_back.defvjp(back_keep, back_low)

def both_round(value):
    return low_back(low(value))

def product(left, right):
    return jnp.dot(left, right, precision=lax.Precision.HIGHEST, preferred_element_type=jnp.float32)

def contract(form, left, right):
    return jnp.einsum(form, left, right, precision=lax.Precision.HIGHEST, preferred_element_type=jnp.float32)

def softmax_rows(scores):
    top = lax.optimization_barrier(jnp.max(scores, axis=-1, keepdims=True))
    shifted = jnp.exp(scores - top)
    return shifted / lax.optimization_barrier(jnp.sum(shifted, axis=-1, keepdims=True))

def split_heads(field):
    sequences = field.shape[0]
    return field.reshape(sequences, LENGTH // BLK, BLK, H, D // H).transpose(0, 3, 1, 2, 4)

def key_slots(rand_blocks, blocks):
    rows = jnp.arange(1, blocks - 1, dtype=jnp.int32)
    fixed = jnp.stack([jnp.zeros_like(rows), jnp.full_like(rows, blocks - 1), rows - 1, rows, rows + 1], axis=1)
    chosen = jnp.transpose(rand_blocks, (0, 2, 1, 3)).astype(jnp.int32)
    fixed = jnp.broadcast_to(fixed, chosen.shape[:3] + (5,))
    slots = jnp.concatenate([fixed, chosen], axis=3)
    always = rows >= 0
    keep = jnp.stack([always, always, rows - 1 != 0, always, rows + 1 != blocks - 1] + [always] * chosen.shape[3], axis=1)
    return (slots, keep)

def pick_blocks(heads_field, slots):
    sequences, heads_count, blocks = heads_field.shape[:3]
    flat = heads_field.reshape(sequences, heads_count, blocks, -1)
    taken = jnp.take_along_axis(flat, slots.reshape(sequences, heads_count, -1, 1), axis=2)
    return taken.reshape(sequences, heads_count, slots.shape[2], slots.shape[3] * BLK, -1)

def attend(query, key, value, rand_blocks):
    blocks = LENGTH // BLK
    scale = (D // H) ** (-0.5)
    sequences = query.shape[0]
    query_heads, key_heads, value_heads = (split_heads(query), split_heads(key), split_heads(value))
    slots, keep = key_slots(rand_blocks, blocks)
    near_keys = pick_blocks(key_heads, slots)
    near_values = pick_blocks(value_heads, slots)
    middle = low_back(contract('shmqd,shmkd->shmqk', query_heads[:, :, 1:blocks - 1], near_keys) * scale)
    middle = jnp.where(jnp.repeat(keep, BLK, axis=1)[:, None, :], middle, NEG)
    middle_weights = low(softmax_rows(middle))
    end_queries = jnp.stack([query_heads[:, :, 0], query_heads[:, :, blocks - 1]], axis=2)
    all_keys = key_heads.reshape(sequences, H, LENGTH, D // H)
    all_values = value_heads.reshape(sequences, H, LENGTH, D // H)
    ends = low_back(contract('shgqd,shkd->shgqk', end_queries, all_keys) * scale)
    ends_weights = low(softmax_rows(ends))
    middle_context = contract('shmqk,shmkd->shmqd', middle_weights, near_values)
    ends_context = contract('shgqk,shkd->shgqd', ends_weights, all_values)
    context = jnp.concatenate([ends_context[:, :, :1], middle_context, ends_context[:, :, 1:]], axis=2)
    return context.transpose(0, 2, 3, 1, 4).reshape(sequences, LENGTH, D)

def layer_norm(total_in, gain, shift):
    mean = lax.optimization_barrier(jnp.mean(total_in, axis=-1, keepdims=True))
    centred = total_in - mean
    variance = lax.optimization_barrier(jnp.mean(centred * centred, axis=-1, keepdims=True))
    return centred * lax.rsqrt(variance + EPS) * gain + shift

def forward(inputs, params, rand_part):
    w_query, w_key, w_value, w_out, w_up, w_down, query_bias, value_bias, out_bias, up_bias, down_bias, norm1_gain, norm1_shift, norm2_gain, norm2_shift = params
    sequences = rand_part.shape[0]
    query = both_round(product(inputs, w_query) + query_bias)
    key = both_round(product(inputs, w_key))
    value = both_round(product(inputs, w_value) + value_bias)
    seq_shape = (sequences, LENGTH, D)
    context = attend(query.reshape(seq_shape), key.reshape(seq_shape), value.reshape(seq_shape), rand_part)
    context = both_round(context.reshape(sequences * LENGTH, D))
    attention = low_back(product(context, w_out) + out_bias)
    first = layer_norm(inputs + attention, norm1_gain, norm1_shift)
    before = low_back(product(low(first), w_up) + up_bias)
    activated = low(jax.nn.gelu(before, approximate=False))
    branch = low_back(product(activated, w_down) + down_bias)
    return layer_norm(first + branch, norm2_gain, norm2_shift)

def reference(hidden, cotangent, rand_blocks, w_query, w_key, w_value, w_out, w_up, w_down, query_bias, value_bias, out_bias, up_bias, down_bias, norm1_gain, norm1_shift, norm2_gain, norm2_shift):
    weights = tuple((item.astype(jnp.float32) for item in (w_query, w_key, w_value, w_out, w_up, w_down, query_bias, value_bias, out_bias, up_bias, down_bias, norm1_gain, norm1_shift, norm2_gain, norm2_shift)))
    group = math.gcd(SEQS, max(1, 4096 // LENGTH))
    rounds = SEQS // group
    inputs_all = hidden.astype(jnp.float32).reshape(rounds, group * LENGTH, D)
    cotangent_all = cotangent.astype(jnp.float32).reshape(rounds, group * LENGTH, D)
    rand_all = rand_blocks.reshape(rounds, group, LENGTH // BLK - 2, H, RAND)

    def one_round(totals, item):
        inputs_part, cotangent_part, rand_part = item
        result, pullback = jax.vjp(lambda inputs, params: forward(inputs, params, rand_part), inputs_part, weights)
        input_grad, param_grads = pullback(cotangent_part)
        return (tuple((total + grad for total, grad in zip(totals, param_grads))), (result, input_grad))
    start = tuple((jnp.zeros_like(item) for item in weights))
    totals, (results, input_grads) = lax.scan(one_round, start, (inputs_all, cotangent_all, rand_all))
    return (results.reshape(TOKENS, D), input_grads.reshape(TOKENS, D), totals[0], totals[1], totals[2], totals[3], totals[4], totals[5], totals[6], totals[7], totals[8], totals[9], totals[10], totals[11], totals[12], totals[13], totals[14])
```

```python
import functools

import jax
import jax.numpy as jnp
from jax import lax
from jax.experimental import pallas as pl
from jax.experimental.pallas import tpu as pltpu
from jax.sharding import PartitionSpec as P

D = 768
H = 12
FF = 3072
BLK = 64
LENGTH = 1024
BLOCKS = LENGTH // BLK
HD = D // H
RAND = 3
EPS = 1e-12
NEG = -1e30
VMEM_BYTES = 64 * 1000 * 1000

HALF = D // 2
FHALF = FF // 2
QKV_W = 3 * HALF
REST_W = HALF + 2 * FHALF
VEC_W = 8 * HALF + FHALF
V_QB, V_VB, V_OB, V_UB = 0, HALF, 2 * HALF, 3 * HALF
V_DB = V_UB + FHALF
V_G1, V_S1, V_G2, V_S2 = V_DB + HALF, V_DB + 2 * HALF, V_DB + 3 * HALF, V_DB + 4 * HALF

f32 = jnp.float32
bf16 = jnp.bfloat16


def dot(a, b):
    return jnp.dot(a, b, preferred_element_type=f32)


def dot_nt(a, b):
    return lax.dot_general(a, b, (((1,), (1,)), ((), ())), preferred_element_type=f32)


def dot_tn(a, b):
    return lax.dot_general(a, b, (((0,), (0,)), ((), ())), preferred_element_type=f32)


def params(**kw):
    return pltpu.CompilerParams(vmem_limit_bytes=VMEM_BYTES, **kw)


def qkv_kernel(x_ref, w_ref, vec_ref, q_ref, k_ref, v_ref):
    r = pl.program_id(0)
    j = pl.program_id(1)
    acc = dot(x_ref[...], w_ref[0])
    vec = vec_ref[0]

    @pl.when(j == 0)
    def _():
        q_ref[...] = ((acc + vec[:, V_QB : V_QB + HALF]).astype(bf16).astype(f32) * 0.125).astype(bf16)

    @pl.when(j == 1)
    def _():
        k_ref[...] = acc.astype(bf16)

    @pl.when(j == 2)
    def _():
        v_ref[...] = (acc + vec[:, V_VB : V_VB + HALF]).astype(bf16)


def qkv(x, w, vec):
    out = jax.ShapeDtypeStruct((LENGTH, D), bf16)
    col = pl.BlockSpec((LENGTH, HALF), lambda r, j: (0, r))
    return pl.pallas_call(
        qkv_kernel,
        grid=(2, 3),
        in_specs=[
            pl.BlockSpec((LENGTH, D), lambda r, j: (0, 0)),
            pl.BlockSpec((1, D, HALF), lambda r, j: (r, 0, j)),
            pl.BlockSpec((1, 1, VEC_W), lambda r, j: (r, 0, 0)),
        ],
        out_specs=[col, col, col],
        out_shape=[out, out, out],
        compiler_params=params(),
        name="qkv",
    )(x, w, vec)


def softmax_bf16(s):
    top = jnp.max(s, axis=-1, keepdims=True)
    e = jnp.exp(s - top)
    total = jnp.sum(e, axis=-1, keepdims=True)
    return (e * (1.0 / total)).astype(bf16)


def head_mask(a, rows):
    lane = lax.broadcasted_iota(jnp.int32, (rows, 2 * HD), 1)
    return (lane < HD) if a == 0 else (lane >= HD)


def only_head(a, x):
    return jnp.where(head_mask(a, x.shape[0]), x, jnp.zeros_like(x))


def key_rows(ref, rand_ref, head, i):
    near = ref[pl.ds(pl.multiple_of((i - 1) * BLK, BLK), 3 * BLK), :]
    parts = [ref[0:BLK, :], ref[LENGTH - BLK :, :], near]
    for n in range(RAND):
        b = rand_ref[((i - 1) * H + head) * RAND + n]
        parts.append(ref[pl.ds(pl.multiple_of(b * BLK, BLK), BLK), :])
    return jnp.concatenate(parts, axis=0)


def edge_mask(s, i):
    col = lax.broadcasted_iota(jnp.int32, s.shape, 1)
    start = jnp.where(i == 1, 2 * BLK, jnp.where(i == BLOCKS - 2, 4 * BLK, -BLK))
    return jnp.where((col >= start) & (col < start + BLK), NEG, s)


def attend_kernel(rand_ref, q_ref, k_ref, v_ref, c_ref, pm_ref, pe_ref):
    pair = pl.program_id(0)
    kall = k_ref[...]
    vall = v_ref[...]
    qe = jnp.concatenate([q_ref[0:BLK, :], q_ref[LENGTH - BLK :, :]], axis=0)
    ends = []
    for a in range(2):
        p = softmax_bf16(dot_nt(only_head(a, qe), kall))
        pe_ref[a] = p
        ends.append(dot(p, vall))
    ce = jnp.where(head_mask(0, 2 * BLK), ends[0], ends[1]).astype(bf16)
    c_ref[0:BLK, :] = ce[:BLK]
    c_ref[LENGTH - BLK :, :] = ce[BLK:]

    def block(i):
        row = pl.multiple_of(i * BLK, BLK)
        qi = q_ref[pl.ds(row, BLK), :]
        outs = []
        for a in range(2):
            kk = key_rows(k_ref, rand_ref, pair * 2 + a, i)
            vv = key_rows(v_ref, rand_ref, pair * 2 + a, i)
            p = softmax_bf16(edge_mask(dot_nt(only_head(a, qi), kk), i))
            pm_ref[a, i - 1] = p
            outs.append(dot(p, vv))
        c_ref[pl.ds(row, BLK), :] = jnp.where(head_mask(0, BLK), outs[0], outs[1]).astype(bf16)

    @pl.loop(0, (BLOCKS - 2) // 2)
    def _(n):
        block(1 + 2 * n)
        block(2 + 2 * n)


def attend(q, k, v, rand):
    pair = pl.BlockSpec((LENGTH, 2 * HD), lambda h, r: (0, h))
    return pl.pallas_call(
        attend_kernel,
        grid_spec=pltpu.PrefetchScalarGridSpec(
            num_scalar_prefetch=1,
            grid=(H // 2,),
            in_specs=[pair, pair, pair],
            out_specs=[
                pair,
                pl.BlockSpec((2, BLOCKS - 2, BLK, 8 * BLK), lambda h, r: (h, 0, 0, 0)),
                pl.BlockSpec((2, 2 * BLK, LENGTH), lambda h, r: (h, 0, 0)),
            ],
        ),
        out_shape=[
            jax.ShapeDtypeStruct((LENGTH, D), bf16),
            jax.ShapeDtypeStruct((H, BLOCKS - 2, BLK, 8 * BLK), bf16),
            jax.ShapeDtypeStruct((H, 2 * BLK, LENGTH), bf16),
        ],
        compiler_params=params(),
        name="attend",
    )(rand, q, k, v)


def score_grad(p, dots):
    pf = p.astype(f32)
    along = jnp.sum(dots * pf, axis=-1, keepdims=True)
    return (pf * (dots - along)).astype(bf16)


def attend_back_kernel(
    rand_ref, q_ref, k_ref, v_ref, d_ref, pm_ref, pe_ref, dq_ref, dk_ref, dv_ref, dk_s, dv_s
):
    pair = pl.program_id(0)
    kall = k_ref[...]
    vall = v_ref[...]
    qe = jnp.concatenate([q_ref[0:BLK, :], q_ref[LENGTH - BLK :, :]], axis=0)
    de = jnp.concatenate([d_ref[0:BLK, :], d_ref[LENGTH - BLK :, :]], axis=0)
    dss, dqs = [], []
    for a in range(2):
        ds = score_grad(pe_ref[a], dot_nt(only_head(a, de), vall))
        dss.append(ds)
        dqs.append(dot(ds, kall))
    dqe = (jnp.where(head_mask(0, 2 * BLK), dqs[0], dqs[1]) * 0.125).astype(bf16)
    dq_ref[0:BLK, :] = dqe[:BLK]
    dq_ref[LENGTH - BLK :, :] = dqe[BLK:]
    q2 = jnp.concatenate([only_head(0, qe), only_head(1, qe)], axis=0)
    d2 = jnp.concatenate([only_head(0, de), only_head(1, de)], axis=0)
    dk_s[...] = dot_tn(jnp.concatenate(dss, axis=0), q2)
    dv_s[...] = dot_tn(jnp.concatenate([pe_ref[0], pe_ref[1]], axis=0), d2)

    def block(i):
        row = pl.multiple_of(i * BLK, BLK)
        qi = q_ref[pl.ds(row, BLK), :]
        di = d_ref[pl.ds(row, BLK), :]
        dss, dqs, ps, qm, dm = [], [], [], [], []
        for a in range(2):
            kk = key_rows(k_ref, rand_ref, pair * 2 + a, i)
            vv = key_rows(v_ref, rand_ref, pair * 2 + a, i)
            p = pm_ref[a, i - 1]
            dm.append(only_head(a, di))
            qm.append(only_head(a, qi))
            ds = score_grad(p, dot_nt(dm[a], vv))
            ps.append(p)
            dss.append(ds)
            dqs.append(dot(ds, kk))
        dq_ref[pl.ds(row, BLK), :] = (
            jnp.where(head_mask(0, BLK), dqs[0], dqs[1]) * 0.125
        ).astype(bf16)
        q2 = jnp.concatenate(qm, axis=0)
        d2 = jnp.concatenate(dm, axis=0)
        fixed = 5 * BLK
        for acc, left, right, each in ((dk_s, dss, q2, qm), (dv_s, ps, d2, dm)):
            both = dot_tn(jnp.concatenate([x[:, :fixed] for x in left], axis=0), right)
            acc[0:BLK, :] += both[0:BLK]
            acc[LENGTH - BLK :, :] += both[BLK : 2 * BLK]
            acc[pl.ds(pl.multiple_of((i - 1) * BLK, BLK), 3 * BLK), :] += both[2 * BLK :]
            for a in range(2):
                own = dot_tn(left[a][:, fixed:], each[a])
                for n in range(RAND):
                    b = rand_ref[((i - 1) * H + pair * 2 + a) * RAND + n]
                    acc[pl.ds(pl.multiple_of(b * BLK, BLK), BLK), :] += own[n * BLK : (n + 1) * BLK]

    @pl.loop(1, BLOCKS - 1)
    def _(i):
        block(i)

    dk_ref[...] = dk_s[...].astype(bf16)
    dv_ref[...] = dv_s[...].astype(bf16)


def attend_back(q, k, v, d, pm, pe, rand):
    pair = pl.BlockSpec((LENGTH, 2 * HD), lambda h, r: (0, h))
    out = jax.ShapeDtypeStruct((LENGTH, D), bf16)
    return pl.pallas_call(
        attend_back_kernel,
        grid_spec=pltpu.PrefetchScalarGridSpec(
            num_scalar_prefetch=1,
            grid=(H // 2,),
            in_specs=[
                pair,
                pair,
                pair,
                pair,
                pl.BlockSpec((2, BLOCKS - 2, BLK, 8 * BLK), lambda h, r: (h, 0, 0, 0)),
                pl.BlockSpec((2, 2 * BLK, LENGTH), lambda h, r: (h, 0, 0)),
            ],
            out_specs=[pair, pair, pair],
            scratch_shapes=[
                pltpu.VMEM((LENGTH, 2 * HD), f32),
                pltpu.VMEM((LENGTH, 2 * HD), f32),
            ],
        ),
        out_shape=[out, out, out],
        compiler_params=params(),
        name="attend_back",
    )(rand, q, k, v, d, pm, pe)


TOK = 256
TSTEPS = LENGTH // TOK
FC = 768
TILES = REST_W // HALF


def gelu_parts(x):
    z = jnp.abs(x) * 0.7071067811865476
    t = 1.0 / (1.0 + 0.5 * z)
    poly = 0.17087277
    for c in (
        -0.82215223,
        1.48851587,
        -1.13520398,
        0.27886807,
        -0.18628806,
        0.09678418,
        0.37409196,
        1.00002368,
        -1.26551223,
    ):
        poly = poly * t + c
    tail = 0.5 * t * jnp.exp(poly - z * z)
    cdf = jnp.where(x >= 0, 1.0 - tail, tail)
    pdf = jnp.exp(-0.5 * x * x) * 0.3989422804014327
    return cdf, pdf


def norm(z, gain, shift):
    mean = jnp.mean(z, axis=1, keepdims=True)
    cen = z - mean
    var = jnp.mean(cen * cen, axis=1, keepdims=True)
    inv = lax.rsqrt(var + EPS)
    unit = cen * inv
    return unit * gain + shift, unit, inv


def norm_back(grad, unit, inv, gain):
    g = grad * gain
    return inv * (
        g - jnp.mean(g, axis=1, keepdims=True) - unit * jnp.mean(g * unit, axis=1, keepdims=True)
    )


def mid_kernel(
    ctx_ref,
    hid_ref,
    cot_ref,
    w_ref,
    vec_ref,
    out_ref,
    resid_ref,
    dctx_ref,
    dw_ref,
    vs_ref,
    act_s,
    bg_s,
    dg_s,
    flT_s,
    brT_s,
    agT_s,
):
    step = pl.program_id(0)

    def vec(off, width=HALF):
        return jnp.concatenate(
            [vec_ref[0, :, off : off + width], vec_ref[1, :, off : off + width]], axis=1
        )

    def add_vec(off, value, width=HALF):
        total = jnp.sum(value, axis=0, keepdims=True)
        vs_ref[0, :, off : off + width] += total[:, :width]
        vs_ref[1, :, off : off + width] += total[:, width:]

    @pl.when(step == 0)
    def _():
        vs_ref[...] = jnp.zeros_like(vs_ref)

    @pl.when(step < TSTEPS)
    def _():
        rows = pl.ds(pl.multiple_of(step * TOK, TOK), TOK)
        ctx = ctx_ref[rows, :]
        att = dot_nt(ctx[:, :HALF], w_ref[0, :, :HALF]) + dot_nt(
            ctx[:, HALF:], w_ref[1, :, :HALF]
        )
        z = hid_ref[...].astype(f32) + (att + vec(V_OB))
        gain1 = vec(V_G1)
        first, unit1, inv1 = norm(z, gain1, vec(V_S1))
        low = first.astype(bf16)
        flT_s[:, rows] = low.T
        branch = None
        for r in range(2):
            for c in range(0, FHALF, FC):
                at = r * FHALF + c
                before = (
                    dot(low, w_ref[r, :, HALF + c : HALF + c + FC])
                    + vec_ref[r, :, V_UB + c : V_UB + c + FC]
                )
                cdf, pdf = gelu_parts(before)
                act = (before * cdf).astype(bf16)
                act_s[rows, at : at + FC] = act
                dg_s[:, at : at + FC] = cdf + before * pdf
                part = dot_nt(act, w_ref[r, :, HALF + FHALF + c : HALF + FHALF + c + FC])
                branch = part if branch is None else branch + part
        gain2 = vec(V_G2)
        output, unit2, inv2 = norm(first + (branch + vec(V_DB)), gain2, vec(V_S2))
        out_ref[...] = output
        cot = cot_ref[...].astype(f32)
        grad2 = norm_back(cot, unit2, inv2, gain2)
        add_vec(V_G2, cot * unit2)
        add_vec(V_S2, cot)
        bgrad = grad2.astype(bf16)
        add_vec(V_DB, bgrad.astype(f32))
        brT_s[:, rows] = bgrad.T
        fgrad = grad2
        for r in range(2):
            for c in range(0, FHALF, FC):
                at = r * FHALF + c
                dact = dot(bgrad, w_ref[r, :, HALF + FHALF + c : HALF + FHALF + c + FC])
                dbef = (dact * dg_s[:, at : at + FC]).astype(bf16)
                bg_s[rows, at : at + FC] = dbef
                vs_ref[r, :, V_UB + c : V_UB + c + FC] += jnp.sum(
                    dbef.astype(f32), axis=0, keepdims=True
                )
                fgrad = fgrad + dot_nt(dbef, w_ref[r, :, HALF + c : HALF + c + FC])
        add_vec(V_G1, fgrad * unit1)
        add_vec(V_S1, fgrad)
        resid = norm_back(fgrad, unit1, inv1, gain1)
        resid_ref[...] = resid
        agrad = resid.astype(bf16)
        add_vec(V_OB, agrad.astype(f32))
        agT_s[:, rows] = agrad.T
        for r in range(2):
            dctx_ref[:, r * HALF : (r + 1) * HALF] = dot(agrad, w_ref[r, :, :HALF]).astype(bf16)

    idx = step - TSTEPS
    r = idx // TILES
    j = idx % TILES

    @pl.when((idx >= 0) & (j == 0))
    def _():
        cols = pl.ds(pl.multiple_of(r * HALF, HALF), HALF)
        dw_ref[0] = dot(agT_s[...], ctx_ref[:, cols]).astype(bf16)

    @pl.when((idx >= 0) & (j >= 1) & (j <= 4))
    def _():
        cols = pl.ds(pl.multiple_of(r * FHALF + (j - 1) * HALF, HALF), HALF)
        dw_ref[0] = dot(flT_s[...], bg_s[:, cols]).astype(bf16)

    @pl.when((idx >= 0) & (j >= 5))
    def _():
        cols = pl.ds(pl.multiple_of(r * FHALF + (j - 5) * HALF, HALF), HALF)
        dw_ref[0] = dot(brT_s[...], act_s[:, cols]).astype(bf16)


def middle(ctx, hid, cot, w, vec):
    def tok(s):
        return (jnp.minimum(s, TSTEPS - 1), 0)

    def tile(s):
        idx = jnp.maximum(s - TSTEPS, 0)
        return (idx // TILES, 0, idx % TILES)

    rows = pl.BlockSpec((TOK, D), tok)
    return pl.pallas_call(
        mid_kernel,
        grid=(TSTEPS + 2 * TILES,),
        in_specs=[
            pl.BlockSpec((LENGTH, D), lambda s: (0, 0), pipeline_mode=pl.Buffered(1)),
            rows,
            rows,
            pl.BlockSpec((2, D, REST_W), lambda s: (0, 0, 0), pipeline_mode=pl.Buffered(1)),
            pl.BlockSpec((2, 1, VEC_W), lambda s: (0, 0, 0), pipeline_mode=pl.Buffered(1)),
        ],
        out_specs=[
            rows,
            rows,
            rows,
            pl.BlockSpec((1, D, HALF), tile),
            pl.BlockSpec((2, 1, VEC_W), lambda s: (0, 0, 0)),
        ],
        out_shape=[
            jax.ShapeDtypeStruct((LENGTH, D), f32),
            jax.ShapeDtypeStruct((LENGTH, D), f32),
            jax.ShapeDtypeStruct((LENGTH, D), bf16),
            jax.ShapeDtypeStruct((2, D, REST_W), bf16),
            jax.ShapeDtypeStruct((2, 1, VEC_W), f32),
        ],
        scratch_shapes=[
            pltpu.VMEM((LENGTH, FF), bf16),
            pltpu.VMEM((LENGTH, FF), bf16),
            pltpu.VMEM((TOK, FF), f32),
            pltpu.VMEM((D, LENGTH), bf16),
            pltpu.VMEM((D, LENGTH), bf16),
            pltpu.VMEM((D, LENGTH), bf16),
        ],
        compiler_params=params(),
        name="middle",
    )(ctx, hid, cot, w, vec)


LTOK = 512
LSTEPS = LENGTH // LTOK


def last_kernel(hid_ref, dq_ref, dk_ref, dv_ref, resid_ref, w_ref, hg_ref, dw_ref, vs_ref, hT_s):
    step = pl.program_id(0)

    @pl.when(step == 0)
    def _():
        hT_s[...] = hid_ref[...].T
        for ref, off in ((dq_ref, 0), (dv_ref, HALF)):
            total = jnp.sum(ref[...].astype(f32), axis=0, keepdims=True)
            vs_ref[0, :, off : off + HALF] = total[:, :HALF]
            vs_ref[1, :, off : off + HALF] = total[:, HALF:]

    @pl.when(step < LSTEPS)
    def _():
        rows = pl.ds(pl.multiple_of(step * LTOK, LTOK), LTOK)
        acc = resid_ref[...]
        for m, ref in enumerate((dq_ref, dk_ref, dv_ref)):
            for r in range(2):
                acc = acc + dot_nt(
                    ref[rows, r * HALF : (r + 1) * HALF],
                    w_ref[r, :, m * HALF : (m + 1) * HALF],
                )
        hg_ref[...] = acc

    idx = step - LSTEPS
    cols = pl.ds(pl.multiple_of(jnp.maximum(idx, 0) // 3 * HALF, HALF), HALF)
    for m, ref in enumerate((dq_ref, dk_ref, dv_ref)):

        @pl.when((idx >= 0) & (idx % 3 == m))
        def _(ref=ref):
            dw_ref[0] = dot(hT_s[...], ref[:, cols]).astype(bf16)


def last(hid, dq, dk, dv, resid, w):
    whole = pl.BlockSpec((LENGTH, D), lambda s: (0, 0), pipeline_mode=pl.Buffered(1))
    rows = pl.BlockSpec((LTOK, D), lambda s: (jnp.minimum(s, LSTEPS - 1), 0))

    def tile(s):
        idx = jnp.maximum(s - LSTEPS, 0)
        return (idx // 3, 0, idx % 3)

    return pl.pallas_call(
        last_kernel,
        grid=(LSTEPS + 6,),
        in_specs=[
            whole,
            whole,
            whole,
            whole,
            rows,
            pl.BlockSpec((2, D, QKV_W), lambda s: (0, 0, 0), pipeline_mode=pl.Buffered(1)),
        ],
        out_specs=[
            rows,
            pl.BlockSpec((1, D, HALF), tile),
            pl.BlockSpec((2, 1, 2 * HALF), lambda s: (0, 0, 0)),
        ],
        out_shape=[
            jax.ShapeDtypeStruct((LENGTH, D), f32),
            jax.ShapeDtypeStruct((2, D, QKV_W), bf16),
            jax.ShapeDtypeStruct((2, 1, 2 * HALF), f32),
        ],
        scratch_shapes=[pltpu.VMEM((D, LENGTH), bf16)],
        compiler_params=params(),
        name="last",
    )(hid, dq, dk, dv, resid, w)


def gather_parts(parts, rows_n, cols_n):
    packed = jnp.concatenate(parts, axis=1)
    every = lax.all_gather(packed, ("row", "col"), axis=0, tiled=True)
    every = every.reshape(rows_n, D, packed.shape[1])
    if rows_n == 2:
        return every
    pieces, at = [], 0
    for part in parts:
        width = part.shape[1]
        one = every[:, :, at : at + width].reshape(2, rows_n // 2, D, width)
        pieces.append(one.transpose(0, 2, 1, 3).reshape(2, D, rows_n // 2 * width))
        at += width
    return jnp.concatenate(pieces, axis=2)


def scatter_parts(full, halves, rows_n, cols_n):
    widths = [h * 2 // rows_n for h in halves]
    if rows_n != 2:
        pieces, at = [], 0
        for half, width in zip(halves, widths):
            one = full[:, :, at : at + half].reshape(2, D, rows_n // 2, width)
            pieces.append(one.transpose(0, 2, 1, 3).reshape(rows_n, D, width))
            at += half
        full = jnp.concatenate(pieces, axis=2)
    flat = full.reshape(rows_n * D, sum(widths))
    mine = lax.psum_scatter(flat, ("row", "col"), scatter_dimension=0, tiled=True)
    mine = mine.astype(f32)
    out, at = [], 0
    for width in widths:
        out.append(mine[:, at : at + width])
        at += width
    return out


VEC_HALVES = (HALF, HALF, HALF, FHALF, HALF, HALF, HALF, HALF, HALF)


def on_device(
    rows_n,
    cols_n,
    hidden,
    cotangent,
    rand_blocks,
    w_query,
    w_key,
    w_value,
    w_out,
    w_up,
    w_down,
    *vectors,
):
    vec = lax.all_gather(jnp.concatenate(vectors).astype(f32), "row", axis=0, tiled=False)
    if rows_n != 2:
        pieces, at = [], 0
        for half in VEC_HALVES:
            width = half * 2 // rows_n
            pieces.append(vec[:, at : at + width].reshape(2, half))
            at += width
        vec = jnp.concatenate(pieces, axis=1)
    vec = vec.reshape(2, 1, VEC_W)
    w1 = gather_parts([w_query, w_key, w_value], rows_n, cols_n)
    w2 = gather_parts([w_out.T, w_up, w_down.T], rows_n, cols_n)
    rand = rand_blocks.reshape(-1)
    q, k, v = qkv(hidden, w1, vec)
    ctx, pm, pe = attend(q, k, v, rand)
    output, resid, dctx, dw2, vs2 = middle(ctx, hidden, cotangent, w2, vec)
    dq, dk, dv = attend_back(q, k, v, dctx, pm, pe, rand)
    hgrad, dw1, vs1 = last(hidden, dq, dk, dv, resid, w1)
    g_out, g_up, g_down = scatter_parts(dw2, (HALF, FHALF, FHALF), rows_n, cols_n)
    g_q, g_k, g_v = scatter_parts(dw1, (HALF, HALF, HALF), rows_n, cols_n)
    vs = jnp.concatenate([vs1, vs2[:, :, 2 * HALF :]], axis=2).reshape(2, VEC_W)
    vs = lax.psum(vs, ("col", "row"))
    row = lax.axis_index("row")
    sums, at = [], 0
    for half in VEC_HALVES:
        width = half * 2 // rows_n
        both = vs[:, at : at + half].reshape(rows_n, width)
        sums.append(lax.dynamic_index_in_dim(both, row, 0, keepdims=False))
        at += half
    return (output, hgrad, g_q, g_k, g_v, g_out.T, g_up, g_down.T, *sums)


def solution(mesh):
    rows_n, cols_n = mesh.shape["row"], mesh.shape["col"]
    tokens = P(("col", "row"), None)
    placed = (
        tokens,
        tokens,
        P(("col", "row"), None, None, None),
        P("col", "row"),
        P("col", "row"),
        P("col", "row"),
        P("row", "col"),
        P("col", "row"),
        P("row", "col"),
    ) + (P("row"),) * 9
    return jax.shard_map(
        functools.partial(on_device, rows_n, cols_n),
        mesh=mesh,
        in_specs=placed,
        out_specs=(
            tokens,
            tokens,
            P("col", "row"),
            P("col", "row"),
            P("col", "row"),
            P("row", "col"),
            P("col", "row"),
            P("row", "col"),
        )
        + (P("row"),) * 9,
        check_vma=False,
    )
```

```python
import functools

import jax
import jax.numpy as jnp
from jax import lax
from jax.experimental import pallas as pl
from jax.experimental.pallas import tpu as pltpu
from jax.sharding import PartitionSpec as P

D = 768
H = 12
FF = 3072
BLK = 64
LENGTH = 1024
BLOCKS = LENGTH // BLK
HD = D // H
RAND = 3
EPS = 1e-12
NEG = -1e30
VMEM_BYTES = 64 * 1000 * 1000

HALF = D // 2
FHALF = FF // 2
QKV_W = 3 * HALF
REST_W = HALF + 2 * FHALF
VEC_W = 8 * HALF + FHALF
V_QB, V_VB, V_OB, V_UB = 0, HALF, 2 * HALF, 3 * HALF
V_DB = V_UB + FHALF
V_G1, V_S1, V_G2, V_S2 = V_DB + HALF, V_DB + 2 * HALF, V_DB + 3 * HALF, V_DB + 4 * HALF

f32 = jnp.float32
bf16 = jnp.bfloat16


def dot(a, b):
    return jnp.dot(a, b, preferred_element_type=f32)


def dot_nt(a, b):
    return lax.dot_general(a, b, (((1,), (1,)), ((), ())), preferred_element_type=f32)


def dot_tn(a, b):
    return lax.dot_general(a, b, (((0,), (0,)), ((), ())), preferred_element_type=f32)


def params(**kw):
    return pltpu.CompilerParams(vmem_limit_bytes=VMEM_BYTES, **kw)


def qkv_kernel(x_ref, w_ref, vec_ref, q_ref, k_ref, v_ref):
    r = pl.program_id(0)
    j = pl.program_id(1)
    acc = dot(x_ref[...], w_ref[0])
    vec = vec_ref[0]

    @pl.when(j == 0)
    def _():
        q_ref[...] = ((acc + vec[:, V_QB : V_QB + HALF]).astype(bf16).astype(f32) * 0.125).astype(bf16)

    @pl.when(j == 1)
    def _():
        k_ref[...] = acc.astype(bf16)

    @pl.when(j == 2)
    def _():
        v_ref[...] = (acc + vec[:, V_VB : V_VB + HALF]).astype(bf16)


def qkv(x, w, vec):
    out = jax.ShapeDtypeStruct((LENGTH, D), bf16)
    col = pl.BlockSpec((LENGTH, HALF), lambda r, j: (0, r))
    return pl.pallas_call(
        qkv_kernel,
        grid=(2, 3),
        in_specs=[
            pl.BlockSpec((LENGTH, D), lambda r, j: (0, 0)),
            pl.BlockSpec((1, D, HALF), lambda r, j: (r, 0, j)),
            pl.BlockSpec((1, 1, VEC_W), lambda r, j: (r, 0, 0)),
        ],
        out_specs=[col, col, col],
        out_shape=[out, out, out],
        compiler_params=params(),
        name="qkv",
    )(x, w, vec)


QT = 256
QTILES = LENGTH // QT


def head_lanes(a, x):
    lane = lax.broadcasted_iota(jnp.int32, x.shape, 1)
    return jnp.where((lane < HD) if a == 0 else (lane >= HD), x, jnp.zeros_like(x))


def both_heads(top, low):
    row = lax.broadcasted_iota(jnp.int32, top.shape, 0)
    return jnp.where(row < HD, top, low)


def hidden_pairs(rand):
    rows = jnp.arange(BLOCKS)[:, None]
    cols = jnp.arange(BLOCKS)[None, :]
    edge = (rows == 0) | (rows == BLOCKS - 1) | (cols == 0) | (cols == BLOCKS - 1)
    near = jnp.abs(rows - cols) <= 1
    chosen = (rand[:, :, :, None] == jnp.arange(BLOCKS)).any(axis=2)
    chosen = jnp.pad(chosen.transpose(1, 2, 0), ((0, 0), (0, 0), (1, 1)))
    table = jnp.where(chosen | (edge | near)[None], 0.0, NEG).astype(f32)
    return jnp.repeat(table, BLK, axis=2)


def attend_kernel(q_ref, k_ref, v_ref, hide_ref, c_ref, p_ref):
    kall = k_ref[...]
    vT = v_ref[...].T

    @pl.loop(0, QTILES)
    def _(n):
        at = pl.ds(pl.multiple_of(n * QT, QT), QT)
        q = q_ref[at, :]
        outs = []
        for a in range(2):
            s = dot_nt(kall, head_lanes(a, q)).reshape(BLOCKS, BLK, QT)
            s = (s + hide_ref[a, :, at][:, None, :]).reshape(LENGTH, QT)
            e = jnp.exp(s - jnp.max(s, axis=0, keepdims=True))
            p = (e * (1.0 / jnp.sum(e, axis=0, keepdims=True))).astype(bf16)
            p_ref[a, :, at] = p
            outs.append(dot(vT, p))
        c_ref[at, :] = both_heads(*outs).T.astype(bf16)


def attend(q, k, v, hide):
    pair = pl.BlockSpec((LENGTH, 2 * HD), lambda h: (0, h))
    return pl.pallas_call(
        attend_kernel,
        grid=(H // 2,),
        in_specs=[pair, pair, pair, pl.BlockSpec((2, BLOCKS, LENGTH), lambda h: (h, 0, 0))],
        out_specs=[pair, pl.BlockSpec((2, LENGTH, LENGTH), lambda h: (h, 0, 0))],
        out_shape=[
            jax.ShapeDtypeStruct((LENGTH, D), bf16),
            jax.ShapeDtypeStruct((H, LENGTH, LENGTH), bf16),
        ],
        compiler_params=params(),
        name="attend",
    )(q, k, v, hide)


def attend_back_kernel(q_ref, k_ref, v_ref, d_ref, p_ref, dq_ref, dk_ref, dv_ref, ds_s):
    vall = v_ref[...]
    kT = k_ref[...].T

    @pl.loop(0, QTILES)
    def _(n):
        at = pl.ds(pl.multiple_of(n * QT, QT), QT)
        d = d_ref[at, :]
        outs = []
        for a in range(2):
            dots = dot_nt(vall, head_lanes(a, d))
            p = p_ref[a, :, at].astype(f32)
            ds = (p * (dots - jnp.sum(dots * p, axis=0, keepdims=True))).astype(bf16)
            ds_s[a, :, at] = ds
            outs.append(dot(kT, ds))
        dq_ref[at, :] = (both_heads(*outs).T * 0.125).astype(bf16)

    dk_ref[...] = (
        dot(ds_s[0], head_lanes(0, q_ref[...])) + dot(ds_s[1], head_lanes(1, q_ref[...]))
    ).astype(bf16)
    dv_ref[...] = (
        dot(p_ref[0], head_lanes(0, d_ref[...])) + dot(p_ref[1], head_lanes(1, d_ref[...]))
    ).astype(bf16)


def attend_back(q, k, v, d, p):
    pair = pl.BlockSpec((LENGTH, 2 * HD), lambda h: (0, h))
    out = jax.ShapeDtypeStruct((LENGTH, D), bf16)
    return pl.pallas_call(
        attend_back_kernel,
        grid=(H // 2,),
        in_specs=[pair, pair, pair, pair, pl.BlockSpec((2, LENGTH, LENGTH), lambda h: (h, 0, 0))],
        out_specs=[pair, pair, pair],
        out_shape=[out, out, out],
        scratch_shapes=[pltpu.VMEM((2, LENGTH, LENGTH), bf16)],
        compiler_params=params(),
        name="attend_back",
    )(q, k, v, d, p)


TOK = 256
TSTEPS = LENGTH // TOK
FC = 768
TILES = REST_W // HALF


def gelu_parts(x):
    z = jnp.abs(x) * 0.7071067811865476
    t = 1.0 / (1.0 + 0.5 * z)
    poly = 0.17087277
    for c in (
        -0.82215223,
        1.48851587,
        -1.13520398,
        0.27886807,
        -0.18628806,
        0.09678418,
        0.37409196,
        1.00002368,
        -1.26551223,
    ):
        poly = poly * t + c
    tail = 0.5 * t * jnp.exp(poly - z * z)
    cdf = jnp.where(x >= 0, 1.0 - tail, tail)
    pdf = jnp.exp(-0.5 * x * x) * 0.3989422804014327
    return cdf, pdf


def norm(z, gain, shift):
    mean = jnp.mean(z, axis=1, keepdims=True)
    cen = z - mean
    var = jnp.mean(cen * cen, axis=1, keepdims=True)
    inv = lax.rsqrt(var + EPS)
    unit = cen * inv
    return unit * gain + shift, unit, inv


def norm_back(grad, unit, inv, gain):
    g = grad * gain
    return inv * (
        g - jnp.mean(g, axis=1, keepdims=True) - unit * jnp.mean(g * unit, axis=1, keepdims=True)
    )


def mid_kernel(
    ctx_ref,
    hid_ref,
    cot_ref,
    w_ref,
    vec_ref,
    out_ref,
    resid_ref,
    dctx_ref,
    dw_ref,
    vs_ref,
    act_s,
    bg_s,
    dg_s,
    flT_s,
    brT_s,
    agT_s,
):
    step = pl.program_id(0)

    def vec(off, width=HALF):
        return jnp.concatenate(
            [vec_ref[0, :, off : off + width], vec_ref[1, :, off : off + width]], axis=1
        )

    def add_vec(off, value, width=HALF):
        total = jnp.sum(value, axis=0, keepdims=True)
        vs_ref[0, :, off : off + width] += total[:, :width]
        vs_ref[1, :, off : off + width] += total[:, width:]

    @pl.when(step == 0)
    def _():
        vs_ref[...] = jnp.zeros_like(vs_ref)

    @pl.when(step < TSTEPS)
    def _():
        rows = pl.ds(pl.multiple_of(step * TOK, TOK), TOK)
        ctx = ctx_ref[rows, :]
        att = dot_nt(ctx[:, :HALF], w_ref[0, :, :HALF]) + dot_nt(
            ctx[:, HALF:], w_ref[1, :, :HALF]
        )
        z = hid_ref[...].astype(f32) + (att + vec(V_OB))
        gain1 = vec(V_G1)
        first, unit1, inv1 = norm(z, gain1, vec(V_S1))
        low = first.astype(bf16)
        flT_s[:, rows] = low.T
        branch = None
        for r in range(2):
            for c in range(0, FHALF, FC):
                at = r * FHALF + c
                before = (
                    dot(low, w_ref[r, :, HALF + c : HALF + c + FC])
                    + vec_ref[r, :, V_UB + c : V_UB + c + FC]
                )
                cdf, pdf = gelu_parts(before)
                act = (before * cdf).astype(bf16)
                act_s[rows, at : at + FC] = act
                dg_s[:, at : at + FC] = cdf + before * pdf
                part = dot_nt(act, w_ref[r, :, HALF + FHALF + c : HALF + FHALF + c + FC])
                branch = part if branch is None else branch + part
        gain2 = vec(V_G2)
        output, unit2, inv2 = norm(first + (branch + vec(V_DB)), gain2, vec(V_S2))
        out_ref[...] = output
        cot = cot_ref[...].astype(f32)
        grad2 = norm_back(cot, unit2, inv2, gain2)
        add_vec(V_G2, cot * unit2)
        add_vec(V_S2, cot)
        bgrad = grad2.astype(bf16)
        add_vec(V_DB, bgrad.astype(f32))
        brT_s[:, rows] = bgrad.T
        fgrad = grad2
        for r in range(2):
            for c in range(0, FHALF, FC):
                at = r * FHALF + c
                dact = dot(bgrad, w_ref[r, :, HALF + FHALF + c : HALF + FHALF + c + FC])
                dbef = (dact * dg_s[:, at : at + FC]).astype(bf16)
                bg_s[rows, at : at + FC] = dbef
                vs_ref[r, :, V_UB + c : V_UB + c + FC] += jnp.sum(
                    dbef.astype(f32), axis=0, keepdims=True
                )
                fgrad = fgrad + dot_nt(dbef, w_ref[r, :, HALF + c : HALF + c + FC])
        add_vec(V_G1, fgrad * unit1)
        add_vec(V_S1, fgrad)
        resid = norm_back(fgrad, unit1, inv1, gain1)
        resid_ref[...] = resid
        agrad = resid.astype(bf16)
        add_vec(V_OB, agrad.astype(f32))
        agT_s[:, rows] = agrad.T
        for r in range(2):
            dctx_ref[:, r * HALF : (r + 1) * HALF] = dot(agrad, w_ref[r, :, :HALF]).astype(bf16)

    idx = step - TSTEPS
    r = idx // TILES
    j = idx % TILES

    @pl.when((idx >= 0) & (j == 0))
    def _():
        cols = pl.ds(pl.multiple_of(r * HALF, HALF), HALF)
        dw_ref[0] = dot(agT_s[...], ctx_ref[:, cols]).astype(bf16)

    @pl.when((idx >= 0) & (j >= 1) & (j <= 4))
    def _():
        cols = pl.ds(pl.multiple_of(r * FHALF + (j - 1) * HALF, HALF), HALF)
        dw_ref[0] = dot(flT_s[...], bg_s[:, cols]).astype(bf16)

    @pl.when((idx >= 0) & (j >= 5))
    def _():
        cols = pl.ds(pl.multiple_of(r * FHALF + (j - 5) * HALF, HALF), HALF)
        dw_ref[0] = dot(brT_s[...], act_s[:, cols]).astype(bf16)


def middle(ctx, hid, cot, w, vec):
    def tok(s):
        return (jnp.minimum(s, TSTEPS - 1), 0)

    def tile(s):
        idx = jnp.maximum(s - TSTEPS, 0)
        return (idx // TILES, 0, idx % TILES)

    rows = pl.BlockSpec((TOK, D), tok)
    return pl.pallas_call(
        mid_kernel,
        grid=(TSTEPS + 2 * TILES,),
        in_specs=[
            pl.BlockSpec((LENGTH, D), lambda s: (0, 0), pipeline_mode=pl.Buffered(1)),
            rows,
            rows,
            pl.BlockSpec((2, D, REST_W), lambda s: (0, 0, 0), pipeline_mode=pl.Buffered(1)),
            pl.BlockSpec((2, 1, VEC_W), lambda s: (0, 0, 0), pipeline_mode=pl.Buffered(1)),
        ],
        out_specs=[
            rows,
            rows,
            rows,
            pl.BlockSpec((1, D, HALF), tile),
            pl.BlockSpec((2, 1, VEC_W), lambda s: (0, 0, 0)),
        ],
        out_shape=[
            jax.ShapeDtypeStruct((LENGTH, D), f32),
            jax.ShapeDtypeStruct((LENGTH, D), f32),
            jax.ShapeDtypeStruct((LENGTH, D), bf16),
            jax.ShapeDtypeStruct((2, D, REST_W), bf16),
            jax.ShapeDtypeStruct((2, 1, VEC_W), f32),
        ],
        scratch_shapes=[
            pltpu.VMEM((LENGTH, FF), bf16),
            pltpu.VMEM((LENGTH, FF), bf16),
            pltpu.VMEM((TOK, FF), f32),
            pltpu.VMEM((D, LENGTH), bf16),
            pltpu.VMEM((D, LENGTH), bf16),
            pltpu.VMEM((D, LENGTH), bf16),
        ],
        compiler_params=params(),
        name="middle",
    )(ctx, hid, cot, w, vec)


LTOK = 512
LSTEPS = LENGTH // LTOK


def last_kernel(hid_ref, dq_ref, dk_ref, dv_ref, resid_ref, w_ref, hg_ref, dw_ref, vs_ref, hT_s):
    step = pl.program_id(0)

    @pl.when(step == 0)
    def _():
        hT_s[...] = hid_ref[...].T
        for ref, off in ((dq_ref, 0), (dv_ref, HALF)):
            total = jnp.sum(ref[...].astype(f32), axis=0, keepdims=True)
            vs_ref[0, :, off : off + HALF] = total[:, :HALF]
            vs_ref[1, :, off : off + HALF] = total[:, HALF:]

    @pl.when(step < LSTEPS)
    def _():
        rows = pl.ds(pl.multiple_of(step * LTOK, LTOK), LTOK)
        acc = resid_ref[...]
        for m, ref in enumerate((dq_ref, dk_ref, dv_ref)):
            for r in range(2):
                acc = acc + dot_nt(
                    ref[rows, r * HALF : (r + 1) * HALF],
                    w_ref[r, :, m * HALF : (m + 1) * HALF],
                )
        hg_ref[...] = acc

    idx = step - LSTEPS
    cols = pl.ds(pl.multiple_of(jnp.maximum(idx, 0) // 3 * HALF, HALF), HALF)
    for m, ref in enumerate((dq_ref, dk_ref, dv_ref)):

        @pl.when((idx >= 0) & (idx % 3 == m))
        def _(ref=ref):
            dw_ref[0] = dot(hT_s[...], ref[:, cols]).astype(bf16)


def last(hid, dq, dk, dv, resid, w):
    whole = pl.BlockSpec((LENGTH, D), lambda s: (0, 0), pipeline_mode=pl.Buffered(1))
    rows = pl.BlockSpec((LTOK, D), lambda s: (jnp.minimum(s, LSTEPS - 1), 0))

    def tile(s):
        idx = jnp.maximum(s - LSTEPS, 0)
        return (idx // 3, 0, idx % 3)

    return pl.pallas_call(
        last_kernel,
        grid=(LSTEPS + 6,),
        in_specs=[
            whole,
            whole,
            whole,
            whole,
            rows,
            pl.BlockSpec((2, D, QKV_W), lambda s: (0, 0, 0), pipeline_mode=pl.Buffered(1)),
        ],
        out_specs=[
            rows,
            pl.BlockSpec((1, D, HALF), tile),
            pl.BlockSpec((2, 1, 2 * HALF), lambda s: (0, 0, 0)),
        ],
        out_shape=[
            jax.ShapeDtypeStruct((LENGTH, D), f32),
            jax.ShapeDtypeStruct((2, D, QKV_W), bf16),
            jax.ShapeDtypeStruct((2, 1, 2 * HALF), f32),
        ],
        scratch_shapes=[pltpu.VMEM((D, LENGTH), bf16)],
        compiler_params=params(),
        name="last",
    )(hid, dq, dk, dv, resid, w)


def gather_parts(parts, rows_n, cols_n):
    packed = jnp.concatenate(parts, axis=1)
    every = lax.all_gather(packed, ("row", "col"), axis=0, tiled=True)
    every = every.reshape(rows_n, D, packed.shape[1])
    if rows_n == 2:
        return every
    pieces, at = [], 0
    for part in parts:
        width = part.shape[1]
        one = every[:, :, at : at + width].reshape(2, rows_n // 2, D, width)
        pieces.append(one.transpose(0, 2, 1, 3).reshape(2, D, rows_n // 2 * width))
        at += width
    return jnp.concatenate(pieces, axis=2)


def scatter_parts(full, halves, rows_n, cols_n):
    widths = [h * 2 // rows_n for h in halves]
    if rows_n != 2:
        pieces, at = [], 0
        for half, width in zip(halves, widths):
            one = full[:, :, at : at + half].reshape(2, D, rows_n // 2, width)
            pieces.append(one.transpose(0, 2, 1, 3).reshape(rows_n, D, width))
            at += half
        full = jnp.concatenate(pieces, axis=2)
    flat = full.reshape(rows_n * D, sum(widths))
    mine = lax.psum_scatter(flat, ("row", "col"), scatter_dimension=0, tiled=True)
    mine = mine.astype(f32)
    out, at = [], 0
    for width in widths:
        out.append(mine[:, at : at + width])
        at += width
    return out


VEC_HALVES = (HALF, HALF, HALF, FHALF, HALF, HALF, HALF, HALF, HALF)


def on_device(
    rows_n,
    cols_n,
    hidden,
    cotangent,
    rand_blocks,
    w_query,
    w_key,
    w_value,
    w_out,
    w_up,
    w_down,
    *vectors,
):
    vec = lax.all_gather(jnp.concatenate(vectors).astype(f32), "row", axis=0, tiled=False)
    if rows_n != 2:
        pieces, at = [], 0
        for half in VEC_HALVES:
            width = half * 2 // rows_n
            pieces.append(vec[:, at : at + width].reshape(2, half))
            at += width
        vec = jnp.concatenate(pieces, axis=1)
    vec = vec.reshape(2, 1, VEC_W)
    w1 = gather_parts([w_query, w_key, w_value], rows_n, cols_n)
    w2 = gather_parts([w_out.T, w_up, w_down.T], rows_n, cols_n)
    hide = hidden_pairs(rand_blocks[0])
    q, k, v = qkv(hidden, w1, vec)
    ctx, p = attend(q, k, v, hide)
    output, resid, dctx, dw2, vs2 = middle(ctx, hidden, cotangent, w2, vec)
    dq, dk, dv = attend_back(q, k, v, dctx, p)
    hgrad, dw1, vs1 = last(hidden, dq, dk, dv, resid, w1)
    g_out, g_up, g_down = scatter_parts(dw2, (HALF, FHALF, FHALF), rows_n, cols_n)
    g_q, g_k, g_v = scatter_parts(dw1, (HALF, HALF, HALF), rows_n, cols_n)
    vs = jnp.concatenate([vs1, vs2[:, :, 2 * HALF :]], axis=2).reshape(2, VEC_W)
    vs = lax.psum(vs, ("col", "row"))
    row = lax.axis_index("row")
    sums, at = [], 0
    for half in VEC_HALVES:
        width = half * 2 // rows_n
        both = vs[:, at : at + half].reshape(rows_n, width)
        sums.append(lax.dynamic_index_in_dim(both, row, 0, keepdims=False))
        at += half
    return (output, hgrad, g_q, g_k, g_v, g_out.T, g_up, g_down.T, *sums)


def solution(mesh):
    rows_n, cols_n = mesh.shape["row"], mesh.shape["col"]
    tokens = P(("col", "row"), None)
    placed = (
        tokens,
        tokens,
        P(("col", "row"), None, None, None),
        P("col", "row"),
        P("col", "row"),
        P("col", "row"),
        P("row", "col"),
        P("col", "row"),
        P("row", "col"),
    ) + (P("row"),) * 9
    return jax.shard_map(
        functools.partial(on_device, rows_n, cols_n),
        mesh=mesh,
        in_specs=placed,
        out_specs=(
            tokens,
            tokens,
            P("col", "row"),
            P("col", "row"),
            P("col", "row"),
            P("row", "col"),
            P("col", "row"),
            P("row", "col"),
        )
        + (P("row"),) * 9,
        check_vma=False,
    )
```

```python
import functools

import jax
import jax.numpy as jnp
from jax import lax
from jax.experimental import pallas as pl
from jax.experimental.pallas import tpu as pltpu
from jax.sharding import PartitionSpec as P

D = 768
H = 12
FF = 3072
BLK = 64
LENGTH = 1024
BLOCKS = LENGTH // BLK
HD = D // H
RAND = 3
EPS = 1e-12
NEG = -1e30
VMEM_BYTES = 64 * 1000 * 1000

HALF = D // 2
FHALF = FF // 2
QKV_W = 3 * HALF
REST_W = HALF + 2 * FHALF
VEC_W = 8 * HALF + FHALF
V_QB, V_VB, V_OB, V_UB = 0, HALF, 2 * HALF, 3 * HALF
V_DB = V_UB + FHALF
V_G1, V_S1, V_G2, V_S2 = V_DB + HALF, V_DB + 2 * HALF, V_DB + 3 * HALF, V_DB + 4 * HALF

f32 = jnp.float32
bf16 = jnp.bfloat16


def dot(a, b):
    return jnp.dot(a, b, preferred_element_type=f32)


def dot_nt(a, b):
    return lax.dot_general(a, b, (((1,), (1,)), ((), ())), preferred_element_type=f32)


def dot_tn(a, b):
    return lax.dot_general(a, b, (((0,), (0,)), ((), ())), preferred_element_type=f32)


def params(**kw):
    return pltpu.CompilerParams(vmem_limit_bytes=VMEM_BYTES, **kw)


def qkv_kernel(x_ref, w_ref, vec_ref, q_ref, k_ref, v_ref):
    r = pl.program_id(0)
    j = pl.program_id(1)
    acc = dot(x_ref[...], w_ref[0])
    vec = vec_ref[0]

    @pl.when(j == 0)
    def _():
        q_ref[...] = ((acc + vec[:, V_QB : V_QB + HALF]).astype(bf16).astype(f32) * 0.125).astype(bf16)

    @pl.when(j == 1)
    def _():
        k_ref[...] = acc.astype(bf16)

    @pl.when(j == 2)
    def _():
        v_ref[...] = (acc + vec[:, V_VB : V_VB + HALF]).astype(bf16)


def qkv(x, w, vec):
    out = jax.ShapeDtypeStruct((LENGTH, D), bf16)
    col = pl.BlockSpec((LENGTH, HALF), lambda r, j: (0, r))
    return pl.pallas_call(
        qkv_kernel,
        grid=(2, 3),
        in_specs=[
            pl.BlockSpec((LENGTH, D), lambda r, j: (0, 0)),
            pl.BlockSpec((1, D, HALF), lambda r, j: (r, 0, j)),
            pl.BlockSpec((1, 1, VEC_W), lambda r, j: (r, 0, 0)),
        ],
        out_specs=[col, col, col],
        out_shape=[out, out, out],
        compiler_params=params(),
        name="qkv",
    )(x, w, vec)


MESH = pl.DeviceIdType.MESH


class Place:
    def __init__(self, zs):
        c = lax.axis_index("col")
        y = lax.axis_index("row")
        self.zs = zs
        self.core, self.x, self.y, self.z = c % 2, c // 2 % 2, y, c // 4
        self.by_core = {"col": c + 1 - 2 * self.core, "row": y}
        self.by_x = {"col": c + 2 - 4 * self.x, "row": y}
        self.by_y = {"col": c, "row": 1 - y}
        self.within = c % 4

    def ahead(self, d):
        return (self.z + d) % self.zs

    def by_z(self, d):
        return {"col": self.ahead(d) * 4 + self.within, "row": self.y}


def greet(partners):
    barrier = pltpu.get_barrier_semaphore()
    for to in partners:
        pl.semaphore_signal(barrier, inc=1, device_id=to, device_id_type=MESH)
    pl.semaphore_wait(barrier, len(partners))


def remote(src, dst, send, recv, i, to):
    return pltpu.make_async_remote_copy(
        src_ref=src,
        dst_ref=dst,
        send_sem=send.at[i],
        recv_sem=recv.at[i],
        device_id=to,
        device_id_type=MESH,
    )


def add_low(a, b):
    return (a.astype(f32) + b.astype(f32)).astype(bf16)


def plane_scratch(zs, rows, width):
    half = zs // 2
    return [
        pltpu.VMEM((2, zs, 2, rows, width), bf16),
        pltpu.VMEM((2, zs, 2, rows, width), bf16),
        pltpu.VMEM((2, half, rows, width), bf16),
        pltpu.VMEM((half, 2, rows, width), bf16),
        pltpu.VMEM((half, rows, width), bf16),
        pltpu.VMEM((half, rows, width), bf16),
        pltpu.SemaphoreType.DMA((5,)),
        pltpu.SemaphoreType.DMA((5,)),
        pltpu.SemaphoreType.DMA,
    ]


class PlaneSum:
    def __init__(self, at, g, own, b1, b2x, b2y, b3y, b3x, send, recv, local):
        half = at.zs // 2
        self.at, self.half = at, half
        self.own, self.b1, self.b2x, self.b2y, self.b3y, self.b3x = own, b1, b2x, b2y, b3y, b3x
        self.g, self.send, self.recv, self.local = g, send, recv, local

    def keep(self):
        return pltpu.make_async_copy(self.g.at[:, :, :, self.at.core], self.own, self.local)

    def to_core(self):
        at = self.at
        return remote(self.g.at[:, :, :, 1 - at.core], self.b1, self.send, self.recv, 0, at.by_core)

    def second(self):
        at, half, sems = self.at, self.half, (self.send, self.recv)
        return (
            remote(self.b1.at[:, 0:half, 1 - at.x], self.b2x, *sems, 1, at.by_x),
            remote(self.b1.at[1 - at.y, half:], self.b2y, *sems, 2, at.by_y),
        )

    def third(self):
        at, sems = self.at, (self.send, self.recv)
        return (
            remote(self.b2x.at[1 - at.y], self.b3y, *sems, 3, at.by_y),
            remote(self.b2y.at[:, 1 - at.x], self.b3x, *sems, 4, at.by_x),
        )

    def stage1(self):
        self.keep().start()
        self.to_core().start()

    def stage2(self):
        self.keep().wait()
        self.to_core().wait()
        b1, own = self.b1, self.own

        @pl.loop(0, self.at.zs)
        def _(z):
            for y in range(2):
                for x in range(2):
                    b1[y, z, x] = add_low(b1[y, z, x], own[y, z, x])

        for copy in self.second():
            copy.start()

    def stage3(self):
        for copy in self.second():
            copy.wait()
        b1, b2x, b2y, half = self.b1, self.b2x, self.b2y, self.half

        @pl.loop(0, half)
        def _(z):
            for n in range(2):
                b2x[n, z] = add_low(b2x[n, z], b1[n, z, self.at.x])
                b2y[z, n] = add_low(b2y[z, n], b1[self.at.y, half + z, n])

        for copy in self.third():
            copy.start()

    def finish(self, out):
        for copy in self.third():
            copy.wait()
        half = self.half

        @pl.loop(0, half)
        def _(z):
            out[z] = add_low(self.b3y[z], self.b2x[self.at.y, z])
            out[half + z] = add_low(self.b3x[z], self.b2y[z, self.at.x])


def line_scratch(zs, rows, width):
    return [
        pltpu.VMEM((zs - 1, rows, width), bf16),
        pltpu.SemaphoreType.DMA((zs - 1,)),
        pltpu.SemaphoreType.DMA((zs - 1,)),
    ]


class LineSum:
    def __init__(self, at, h, held, send, recv):
        self.at, self.h, self.held = at, h, held
        self.copies = [
            remote(h.at[at.ahead(d)], held.at[d - 1], send, recv, d - 1, at.by_z(d))
            for d in range(1, at.zs)
        ]

    def start(self):
        for copy in self.copies:
            copy.start()

    def finish(self, out):
        for copy in self.copies:
            copy.wait()
        total = self.h[self.at.z].astype(f32)
        for d in range(1, self.at.zs):
            total = total + self.held[d - 1].astype(f32)
        out[...] = total


def final_kernel(zs, g_ref, h_ref, v_ref, o1_ref, o2_ref, vo_ref, mid, *scratch):
    plane, (v1, v2, v3, v4, va, vb, vsend, vrecv), line1, line2 = (
        scratch[:9],
        scratch[9:17],
        scratch[17:20],
        scratch[20:23],
    )
    at = Place(zs)
    greet([at.by_core, at.by_x, at.by_y] + [at.by_z(d) for d in range(1, zs)])
    first = PlaneSum(at, g_ref, *plane)
    second = LineSum(at, h_ref, *line2)
    first.stage1()
    vec1 = remote(v_ref, v1, vsend, vrecv, 0, at.by_core)
    vec1.start()
    second.start()
    vec1.wait()
    va[...] = v_ref[...] + v1[...]
    vec2 = remote(va, v2, vsend, vrecv, 1, at.by_x)
    vec2.start()
    first.stage2()
    vec2.wait()
    vb[...] = va[...] + v2[...]
    vec3 = remote(vb.at[1 - at.y], v3, vsend, vrecv, 2, at.by_y)
    vec3.start()
    first.stage3()
    vec3.wait()
    v4[0] = vb[at.y] + v3[...]
    vec4 = [
        remote(v4.at[0], v4.at[d], vsend, vrecv, 2 + d, at.by_z(d)) for d in range(1, zs)
    ]
    for copy in vec4:
        copy.start()
    first.finish(mid)
    third = LineSum(at, mid, *line1)
    third.start()
    for copy in vec4:
        copy.wait()
    total = v4[at.z % zs]
    for z in range(1, zs):
        total = total + v4[(at.z + zs - z) % zs]
    vo_ref[...] = total
    second.finish(o2_ref)
    third.finish(o1_ref)


def final(zs, g, h, v):
    rows, w1 = g.shape[4:]
    w2 = h.shape[2]
    width = v.shape[2]
    vmem = pl.BlockSpec(memory_space=pltpu.VMEM)
    return pl.pallas_call(
        functools.partial(final_kernel, zs),
        in_specs=[pl.BlockSpec(memory_space=pl.ANY), vmem, vmem],
        out_specs=[vmem, vmem, vmem],
        out_shape=[
            jax.ShapeDtypeStruct((rows, w1), f32),
            jax.ShapeDtypeStruct((rows, w2), f32),
            jax.ShapeDtypeStruct((1, width), f32),
        ],
        scratch_shapes=[
            pltpu.VMEM((zs, rows, w1), bf16),
            *plane_scratch(zs, rows, w1),
            pltpu.VMEM((2, 1, width), f32),
            pltpu.VMEM((2, 1, width), f32),
            pltpu.VMEM((1, width), f32),
            pltpu.VMEM((zs, 1, width), f32),
            pltpu.VMEM((2, 1, width), f32),
            pltpu.VMEM((2, 1, width), f32),
            pltpu.SemaphoreType.DMA((zs + 2,)),
            pltpu.SemaphoreType.DMA((zs + 2,)),
            *line_scratch(zs, rows, w1),
            *line_scratch(zs, rows, w2),
        ],
        compiler_params=params(collective_id=1, has_side_effects=True),
        name="final",
    )(g, h, v)


QT = 256
QTILES = LENGTH // QT


def head_lanes(a, x):
    lane = lax.broadcasted_iota(jnp.int32, x.shape, 1)
    return jnp.where((lane < HD) if a == 0 else (lane >= HD), x, jnp.zeros_like(x))


def both_heads(top, low):
    row = lax.broadcasted_iota(jnp.int32, top.shape, 0)
    return jnp.where(row < HD, top, low)


def hidden_pairs(rand):
    rows = jnp.arange(BLOCKS)[:, None]
    cols = jnp.arange(BLOCKS)[None, :]
    edge = (rows == 0) | (rows == BLOCKS - 1) | (cols == 0) | (cols == BLOCKS - 1)
    near = jnp.abs(rows - cols) <= 1
    chosen = (rand[:, :, :, None] == jnp.arange(BLOCKS)).any(axis=2)
    chosen = jnp.pad(chosen.transpose(1, 2, 0), ((0, 0), (0, 0), (1, 1)))
    table = jnp.where(chosen | (edge | near)[None], 0.0, NEG).astype(f32)
    return jnp.repeat(table, BLK, axis=2)


def attend_kernel(q_ref, k_ref, v_ref, hide_ref, c_ref, p_ref):
    kall = k_ref[...]
    vT = v_ref[...].T

    @pl.loop(0, QTILES)
    def _(n):
        at = pl.ds(pl.multiple_of(n * QT, QT), QT)
        q = q_ref[at, :]
        outs = []
        for a in range(2):
            s = dot_nt(kall, head_lanes(a, q)).reshape(BLOCKS, BLK, QT)
            s = (s + hide_ref[a, :, at][:, None, :]).reshape(LENGTH, QT)
            e = jnp.exp(s - jnp.max(s, axis=0, keepdims=True))
            p = (e * (1.0 / jnp.sum(e, axis=0, keepdims=True))).astype(bf16)
            p_ref[a, :, at] = p
            outs.append(dot(vT, p))
        c_ref[at, :] = both_heads(*outs).T.astype(bf16)


def attend(q, k, v, hide):
    pair = pl.BlockSpec((LENGTH, 2 * HD), lambda h: (0, h))
    return pl.pallas_call(
        attend_kernel,
        grid=(H // 2,),
        in_specs=[pair, pair, pair, pl.BlockSpec((2, BLOCKS, LENGTH), lambda h: (h, 0, 0))],
        out_specs=[pair, pl.BlockSpec((2, LENGTH, LENGTH), lambda h: (h, 0, 0))],
        out_shape=[
            jax.ShapeDtypeStruct((LENGTH, D), bf16),
            jax.ShapeDtypeStruct((H, LENGTH, LENGTH), bf16),
        ],
        compiler_params=params(),
        name="attend",
    )(q, k, v, hide)


def attend_sum_kernel(zs, q_ref, k_ref, v_ref, d_ref, p_ref, g_ref, dq_ref, dk_ref, dv_ref, h_ref, ds_s, *plane):
    step = pl.program_id(0)
    at = Place(zs)

    @pl.when(step == 0)
    def _():
        greet([at.by_core, at.by_x, at.by_y])
        PlaneSum(at, g_ref, *plane).stage1()

    @pl.when(step == 2)
    def _():
        PlaneSum(at, g_ref, *plane).stage2()

    @pl.when(step == 5)
    def _():
        PlaneSum(at, g_ref, *plane).stage3()

    attend_back_kernel(q_ref, k_ref, v_ref, d_ref, p_ref, dq_ref, dk_ref, dv_ref, ds_s)

    @pl.when(step == 5)
    def _():
        PlaneSum(at, g_ref, *plane).finish(h_ref)


def attend_back_kernel(q_ref, k_ref, v_ref, d_ref, p_ref, dq_ref, dk_ref, dv_ref, ds_s):
    vall = v_ref[...]
    kT = k_ref[...].T

    @pl.loop(0, QTILES)
    def _(n):
        at = pl.ds(pl.multiple_of(n * QT, QT), QT)
        d = d_ref[at, :]
        outs = []
        for a in range(2):
            dots = dot_nt(vall, head_lanes(a, d))
            p = p_ref[a, :, at].astype(f32)
            ds = (p * (dots - jnp.sum(dots * p, axis=0, keepdims=True))).astype(bf16)
            ds_s[a, :, at] = ds
            outs.append(dot(kT, ds))
        dq_ref[at, :] = (both_heads(*outs).T * 0.125).astype(bf16)

    dk_ref[...] = (
        dot(ds_s[0], head_lanes(0, q_ref[...])) + dot(ds_s[1], head_lanes(1, q_ref[...]))
    ).astype(bf16)
    dv_ref[...] = (
        dot(p_ref[0], head_lanes(0, d_ref[...])) + dot(p_ref[1], head_lanes(1, d_ref[...]))
    ).astype(bf16)


def attend_back(q, k, v, d, p, zs=0, g=None):
    pair = pl.BlockSpec((LENGTH, 2 * HD), lambda h: (0, h))
    out = jax.ShapeDtypeStruct((LENGTH, D), bf16)
    if zs:
        held = (zs,) + g.shape[4:]
        return pl.pallas_call(
            functools.partial(attend_sum_kernel, zs),
            grid=(H // 2,),
            in_specs=[
                pair,
                pair,
                pair,
                pair,
                pl.BlockSpec((2, LENGTH, LENGTH), lambda h: (h, 0, 0)),
                pl.BlockSpec(memory_space=pl.ANY),
            ],
            out_specs=[pair, pair, pair, pl.BlockSpec(held, lambda h: (0, 0, 0))],
            out_shape=[out, out, out, jax.ShapeDtypeStruct(held, bf16)],
            scratch_shapes=[pltpu.VMEM((2, LENGTH, LENGTH), bf16), *plane_scratch(*held)],
            compiler_params=params(collective_id=2, has_side_effects=True),
            name="attend_sum",
        )(q, k, v, d, p, g)
    return pl.pallas_call(
        attend_back_kernel,
        grid=(H // 2,),
        in_specs=[pair, pair, pair, pair, pl.BlockSpec((2, LENGTH, LENGTH), lambda h: (h, 0, 0))],
        out_specs=[pair, pair, pair],
        out_shape=[out, out, out],
        scratch_shapes=[pltpu.VMEM((2, LENGTH, LENGTH), bf16)],
        compiler_params=params(),
        name="attend_back",
    )(q, k, v, d, p)


TOK = 256
TSTEPS = LENGTH // TOK
FC = 768
TILES = REST_W // HALF


def gelu_parts(x):
    z = jnp.abs(x) * 0.7071067811865476
    t = 1.0 / (1.0 + 0.5 * z)
    poly = 0.17087277
    for c in (
        -0.82215223,
        1.48851587,
        -1.13520398,
        0.27886807,
        -0.18628806,
        0.09678418,
        0.37409196,
        1.00002368,
        -1.26551223,
    ):
        poly = poly * t + c
    tail = 0.5 * t * jnp.exp(poly - z * z)
    cdf = jnp.where(x >= 0, 1.0 - tail, tail)
    pdf = jnp.exp(-0.5 * x * x) * 0.3989422804014327
    return cdf, pdf


def norm(z, gain, shift):
    mean = jnp.mean(z, axis=1, keepdims=True)
    cen = z - mean
    var = jnp.mean(cen * cen, axis=1, keepdims=True)
    inv = lax.rsqrt(var + EPS)
    unit = cen * inv
    return unit * gain + shift, unit, inv


def norm_back(grad, unit, inv, gain):
    g = grad * gain
    return inv * (
        g - jnp.mean(g, axis=1, keepdims=True) - unit * jnp.mean(g * unit, axis=1, keepdims=True)
    )


def mid_kernel(
    ctx_ref,
    hid_ref,
    cot_ref,
    w_ref,
    vec_ref,
    out_ref,
    resid_ref,
    dctx_ref,
    dw_ref,
    vs_ref,
    act_s,
    bg_s,
    dg_s,
    flT_s,
    brT_s,
    agT_s,
):
    step = pl.program_id(0)

    def vec(off, width=HALF):
        return jnp.concatenate(
            [vec_ref[0, :, off : off + width], vec_ref[1, :, off : off + width]], axis=1
        )

    def add_vec(off, value, width=HALF):
        total = jnp.sum(value, axis=0, keepdims=True)
        vs_ref[0, :, off : off + width] += total[:, :width]
        vs_ref[1, :, off : off + width] += total[:, width:]

    @pl.when(step == 0)
    def _():
        vs_ref[...] = jnp.zeros_like(vs_ref)

    @pl.when(step < TSTEPS)
    def _():
        rows = pl.ds(pl.multiple_of(step * TOK, TOK), TOK)
        ctx = ctx_ref[rows, :]
        att = dot_nt(ctx[:, :HALF], w_ref[0, :, :HALF]) + dot_nt(
            ctx[:, HALF:], w_ref[1, :, :HALF]
        )
        z = hid_ref[...].astype(f32) + (att + vec(V_OB))
        gain1 = vec(V_G1)
        first, unit1, inv1 = norm(z, gain1, vec(V_S1))
        low = first.astype(bf16)
        flT_s[:, rows] = low.T
        branch = None
        for r in range(2):
            for c in range(0, FHALF, FC):
                at = r * FHALF + c
                before = (
                    dot(low, w_ref[r, :, HALF + c : HALF + c + FC])
                    + vec_ref[r, :, V_UB + c : V_UB + c + FC]
                )
                cdf, pdf = gelu_parts(before)
                act = (before * cdf).astype(bf16)
                act_s[rows, at : at + FC] = act
                dg_s[:, at : at + FC] = cdf + before * pdf
                part = dot_nt(act, w_ref[r, :, HALF + FHALF + c : HALF + FHALF + c + FC])
                branch = part if branch is None else branch + part
        gain2 = vec(V_G2)
        output, unit2, inv2 = norm(first + (branch + vec(V_DB)), gain2, vec(V_S2))
        out_ref[...] = output
        cot = cot_ref[...].astype(f32)
        grad2 = norm_back(cot, unit2, inv2, gain2)
        add_vec(V_G2, cot * unit2)
        add_vec(V_S2, cot)
        bgrad = grad2.astype(bf16)
        add_vec(V_DB, bgrad.astype(f32))
        brT_s[:, rows] = bgrad.T
        fgrad = grad2
        for r in range(2):
            for c in range(0, FHALF, FC):
                at = r * FHALF + c
                dact = dot(bgrad, w_ref[r, :, HALF + FHALF + c : HALF + FHALF + c + FC])
                dbef = (dact * dg_s[:, at : at + FC]).astype(bf16)
                bg_s[rows, at : at + FC] = dbef
                vs_ref[r, :, V_UB + c : V_UB + c + FC] += jnp.sum(
                    dbef.astype(f32), axis=0, keepdims=True
                )
                fgrad = fgrad + dot_nt(dbef, w_ref[r, :, HALF + c : HALF + c + FC])
        add_vec(V_G1, fgrad * unit1)
        add_vec(V_S1, fgrad)
        resid = norm_back(fgrad, unit1, inv1, gain1)
        resid_ref[...] = resid
        agrad = resid.astype(bf16)
        add_vec(V_OB, agrad.astype(f32))
        agT_s[:, rows] = agrad.T
        for r in range(2):
            dctx_ref[:, r * HALF : (r + 1) * HALF] = dot(agrad, w_ref[r, :, :HALF]).astype(bf16)

    idx = step - TSTEPS
    r = idx // TILES
    j = idx % TILES

    @pl.when((idx >= 0) & (j == 0))
    def _():
        cols = pl.ds(pl.multiple_of(r * HALF, HALF), HALF)
        dw_ref[0] = dot(agT_s[...], ctx_ref[:, cols]).astype(bf16)

    @pl.when((idx >= 0) & (j >= 1) & (j <= 4))
    def _():
        cols = pl.ds(pl.multiple_of(r * FHALF + (j - 1) * HALF, HALF), HALF)
        dw_ref[0] = dot(flT_s[...], bg_s[:, cols]).astype(bf16)

    @pl.when((idx >= 0) & (j >= 5))
    def _():
        cols = pl.ds(pl.multiple_of(r * FHALF + (j - 5) * HALF, HALF), HALF)
        dw_ref[0] = dot(brT_s[...], act_s[:, cols]).astype(bf16)


def middle(ctx, hid, cot, w, vec):
    def tok(s):
        return (jnp.minimum(s, TSTEPS - 1), 0)

    def tile(s):
        idx = jnp.maximum(s - TSTEPS, 0)
        return (idx // TILES, 0, idx % TILES)

    rows = pl.BlockSpec((TOK, D), tok)
    return pl.pallas_call(
        mid_kernel,
        grid=(TSTEPS + 2 * TILES,),
        in_specs=[
            pl.BlockSpec((LENGTH, D), lambda s: (0, 0), pipeline_mode=pl.Buffered(1)),
            rows,
            rows,
            pl.BlockSpec((2, D, REST_W), lambda s: (0, 0, 0), pipeline_mode=pl.Buffered(1)),
            pl.BlockSpec((2, 1, VEC_W), lambda s: (0, 0, 0), pipeline_mode=pl.Buffered(1)),
        ],
        out_specs=[
            rows,
            rows,
            rows,
            pl.BlockSpec((1, D, HALF), tile),
            pl.BlockSpec((2, 1, VEC_W), lambda s: (0, 0, 0)),
        ],
        out_shape=[
            jax.ShapeDtypeStruct((LENGTH, D), f32),
            jax.ShapeDtypeStruct((LENGTH, D), f32),
            jax.ShapeDtypeStruct((LENGTH, D), bf16),
            jax.ShapeDtypeStruct((2, D, REST_W), bf16),
            jax.ShapeDtypeStruct((2, 1, VEC_W), f32),
        ],
        scratch_shapes=[
            pltpu.VMEM((LENGTH, FF), bf16),
            pltpu.VMEM((LENGTH, FF), bf16),
            pltpu.VMEM((TOK, FF), f32),
            pltpu.VMEM((D, LENGTH), bf16),
            pltpu.VMEM((D, LENGTH), bf16),
            pltpu.VMEM((D, LENGTH), bf16),
        ],
        compiler_params=params(),
        name="middle",
    )(ctx, hid, cot, w, vec)


LTOK = 512
LSTEPS = LENGTH // LTOK


def last_kernel(hid_ref, dq_ref, dk_ref, dv_ref, resid_ref, w_ref, hg_ref, dw_ref, vs_ref, hT_s):
    step = pl.program_id(0)

    @pl.when(step == 0)
    def _():
        hT_s[...] = hid_ref[...].T
        for ref, off in ((dq_ref, 0), (dv_ref, HALF)):
            total = jnp.sum(ref[...].astype(f32), axis=0, keepdims=True)
            vs_ref[0, :, off : off + HALF] = total[:, :HALF]
            vs_ref[1, :, off : off + HALF] = total[:, HALF:]

    @pl.when(step < LSTEPS)
    def _():
        rows = pl.ds(pl.multiple_of(step * LTOK, LTOK), LTOK)
        acc = resid_ref[...]
        for m, ref in enumerate((dq_ref, dk_ref, dv_ref)):
            for r in range(2):
                acc = acc + dot_nt(
                    ref[rows, r * HALF : (r + 1) * HALF],
                    w_ref[r, :, m * HALF : (m + 1) * HALF],
                )
        hg_ref[...] = acc

    idx = step - LSTEPS
    cols = pl.ds(pl.multiple_of(jnp.maximum(idx, 0) // 3 * HALF, HALF), HALF)
    for m, ref in enumerate((dq_ref, dk_ref, dv_ref)):

        @pl.when((idx >= 0) & (idx % 3 == m))
        def _(ref=ref):
            dw_ref[0] = dot(hT_s[...], ref[:, cols]).astype(bf16)


def last(hid, dq, dk, dv, resid, w):
    whole = pl.BlockSpec((LENGTH, D), lambda s: (0, 0), pipeline_mode=pl.Buffered(1))
    rows = pl.BlockSpec((LTOK, D), lambda s: (jnp.minimum(s, LSTEPS - 1), 0))

    def tile(s):
        idx = jnp.maximum(s - LSTEPS, 0)
        return (idx // 3, 0, idx % 3)

    return pl.pallas_call(
        last_kernel,
        grid=(LSTEPS + 6,),
        in_specs=[
            whole,
            whole,
            whole,
            whole,
            rows,
            pl.BlockSpec((2, D, QKV_W), lambda s: (0, 0, 0), pipeline_mode=pl.Buffered(1)),
        ],
        out_specs=[
            rows,
            pl.BlockSpec((1, D, HALF), tile),
            pl.BlockSpec((2, 1, 2 * HALF), lambda s: (0, 0, 0)),
        ],
        out_shape=[
            jax.ShapeDtypeStruct((LENGTH, D), f32),
            jax.ShapeDtypeStruct((2, D, QKV_W), bf16),
            jax.ShapeDtypeStruct((2, 1, 2 * HALF), f32),
        ],
        scratch_shapes=[pltpu.VMEM((D, LENGTH), bf16)],
        compiler_params=params(),
        name="last",
    )(hid, dq, dk, dv, resid, w)


def gather_parts(parts, rows_n, cols_n):
    packed = jnp.concatenate(parts, axis=1)
    every = lax.all_gather(packed, ("row", "col"), axis=0, tiled=True)
    every = every.reshape(rows_n, D, packed.shape[1])
    if rows_n == 2:
        return every
    pieces, at = [], 0
    for part in parts:
        width = part.shape[1]
        one = every[:, :, at : at + width].reshape(2, rows_n // 2, D, width)
        pieces.append(one.transpose(0, 2, 1, 3).reshape(2, D, rows_n // 2 * width))
        at += width
    return jnp.concatenate(pieces, axis=2)


def scatter_parts(full, halves, rows_n, cols_n):
    widths = [h * 2 // rows_n for h in halves]
    if rows_n != 2:
        pieces, at = [], 0
        for half, width in zip(halves, widths):
            one = full[:, :, at : at + half].reshape(2, D, rows_n // 2, width)
            pieces.append(one.transpose(0, 2, 1, 3).reshape(rows_n, D, width))
            at += half
        full = jnp.concatenate(pieces, axis=2)
    flat = full.reshape(rows_n * D, sum(widths))
    mine = lax.psum_scatter(flat, ("row", "col"), scatter_dimension=0, tiled=True)
    mine = mine.astype(f32)
    out, at = [], 0
    for width in widths:
        out.append(mine[:, at : at + width])
        at += width
    return out


VEC_HALVES = (HALF, HALF, HALF, FHALF, HALF, HALF, HALF, HALF, HALF)


def on_device(
    rows_n,
    cols_n,
    hidden,
    cotangent,
    rand_blocks,
    w_query,
    w_key,
    w_value,
    w_out,
    w_up,
    w_down,
    *vectors,
):
    vec = lax.all_gather(jnp.concatenate(vectors).astype(f32), "row", axis=0, tiled=False)
    if rows_n != 2:
        pieces, at = [], 0
        for half in VEC_HALVES:
            width = half * 2 // rows_n
            pieces.append(vec[:, at : at + width].reshape(2, half))
            at += width
        vec = jnp.concatenate(pieces, axis=1)
    vec = vec.reshape(2, 1, VEC_W)
    w1 = gather_parts([w_query, w_key, w_value], rows_n, cols_n)
    w2 = gather_parts([w_out.T, w_up, w_down.T], rows_n, cols_n)
    hide = hidden_pairs(rand_blocks[0])
    q, k, v = qkv(hidden, w1, vec)
    ctx, p = attend(q, k, v, hide)
    output, resid, dctx, dw2, vs2 = middle(ctx, hidden, cotangent, w2, vec)
    zs = cols_n // 4
    staged = rows_n == 2 and cols_n % 8 == 0
    if staged:
        spread = (2, zs, 2, 2, D // cols_n)
        g2 = dw2.reshape(spread + (REST_W,))
        dq, dk, dv, h2 = attend_back(q, k, v, dctx, p, zs, g2)
    else:
        dq, dk, dv = attend_back(q, k, v, dctx, p)
    hgrad, dw1, vs1 = last(hidden, dq, dk, dv, resid, w1)
    vs = jnp.concatenate([vs1, vs2[:, :, 2 * HALF :]], axis=2)
    if staged:
        m1, m2, vs = final(zs, dw1.reshape(spread + (QKV_W,)), h2, vs)
        g_q, g_k, g_v = (m1[:, n * HALF : (n + 1) * HALF] for n in range(3))
        g_out = m2[:, :HALF].T
        g_up = m2[:, HALF : HALF + FHALF]
        g_down = m2[:, HALF + FHALF :].T
        sums, at = [], 0
        for width in VEC_HALVES:
            sums.append(vs[0, at : at + width])
            at += width
        return (output, hgrad, g_q, g_k, g_v, g_out, g_up, g_down, *sums)
    g_out, g_up, g_down = scatter_parts(dw2, (HALF, FHALF, FHALF), rows_n, cols_n)
    g_q, g_k, g_v = scatter_parts(dw1, (HALF, HALF, HALF), rows_n, cols_n)
    vs = lax.psum(vs.reshape(2, VEC_W), ("col", "row"))
    row = lax.axis_index("row")
    sums, at = [], 0
    for half in VEC_HALVES:
        width = half * 2 // rows_n
        both = vs[:, at : at + half].reshape(rows_n, width)
        sums.append(lax.dynamic_index_in_dim(both, row, 0, keepdims=False))
        at += half
    return (output, hgrad, g_q, g_k, g_v, g_out.T, g_up, g_down.T, *sums)


def solution(mesh):
    rows_n, cols_n = mesh.shape["row"], mesh.shape["col"]
    tokens = P(("col", "row"), None)
    placed = (
        tokens,
        tokens,
        P(("col", "row"), None, None, None),
        P("col", "row"),
        P("col", "row"),
        P("col", "row"),
        P("row", "col"),
        P("col", "row"),
        P("row", "col"),
    ) + (P("row"),) * 9
    return jax.shard_map(
        functools.partial(on_device, rows_n, cols_n),
        mesh=mesh,
        in_specs=placed,
        out_specs=(
            tokens,
            tokens,
            P("col", "row"),
            P("col", "row"),
            P("col", "row"),
            P("row", "col"),
            P("col", "row"),
            P("row", "col"),
        )
        + (P("row"),) * 9,
        check_vma=False,
    )
```

```python
import functools

import jax
import jax.numpy as jnp
from jax import lax
from jax.experimental import pallas as pl
from jax.experimental.pallas import tpu as pltpu
from jax.sharding import PartitionSpec as P

D = 768
H = 12
FF = 3072
BLK = 64
LENGTH = 1024
BLOCKS = LENGTH // BLK
HD = D // H
RAND = 3
EPS = 1e-12
NEG = -1e30
VMEM_BYTES = 64 * 1000 * 1000

HALF = D // 2
FHALF = FF // 2
QKV_W = 3 * HALF
REST_W = HALF + 2 * FHALF
VEC_W = 8 * HALF + FHALF
V_QB, V_VB, V_OB, V_UB = 0, HALF, 2 * HALF, 3 * HALF
V_DB = V_UB + FHALF
V_G1, V_S1, V_G2, V_S2 = V_DB + HALF, V_DB + 2 * HALF, V_DB + 3 * HALF, V_DB + 4 * HALF

f32 = jnp.float32
bf16 = jnp.bfloat16


def dot(a, b):
    return jnp.dot(a, b, preferred_element_type=f32)


def dot_nt(a, b):
    return lax.dot_general(a, b, (((1,), (1,)), ((), ())), preferred_element_type=f32)


def dot_tn(a, b):
    return lax.dot_general(a, b, (((0,), (0,)), ((), ())), preferred_element_type=f32)


def params(**kw):
    return pltpu.CompilerParams(vmem_limit_bytes=VMEM_BYTES, **kw)


def qkv_kernel(x_ref, w_ref, vec_ref, q_ref, k_ref, v_ref):
    r = pl.program_id(0)
    j = pl.program_id(1)
    acc = dot(x_ref[...], w_ref[0])
    vec = vec_ref[0]

    @pl.when(j == 0)
    def _():
        q_ref[...] = ((acc + vec[:, V_QB : V_QB + HALF]).astype(bf16).astype(f32) * 0.125).astype(bf16)

    @pl.when(j == 1)
    def _():
        k_ref[...] = acc.astype(bf16)

    @pl.when(j == 2)
    def _():
        v_ref[...] = (acc + vec[:, V_VB : V_VB + HALF]).astype(bf16)


def qkv(x, w, vec):
    out = jax.ShapeDtypeStruct((LENGTH, D), bf16)
    col = pl.BlockSpec((LENGTH, HALF), lambda r, j: (0, r))
    return pl.pallas_call(
        qkv_kernel,
        grid=(2, 3),
        in_specs=[
            pl.BlockSpec((LENGTH, D), lambda r, j: (0, 0)),
            pl.BlockSpec((1, D, HALF), lambda r, j: (r, 0, j)),
            pl.BlockSpec((1, 1, VEC_W), lambda r, j: (r, 0, 0)),
        ],
        out_specs=[col, col, col],
        out_shape=[out, out, out],
        compiler_params=params(),
        name="qkv",
    )(x, w, vec)


MESH = pl.DeviceIdType.MESH


class Place:
    def __init__(self, zs):
        c = lax.axis_index("col")
        y = lax.axis_index("row")
        self.zs = zs
        self.core, self.x, self.y, self.z = c % 2, c // 2 % 2, y, c // 4
        self.by_core = {"col": c + 1 - 2 * self.core, "row": y}
        self.by_x = {"col": c + 2 - 4 * self.x, "row": y}
        self.by_y = {"col": c, "row": 1 - y}
        self.within = c % 4

    def ahead(self, d):
        return (self.z + d) % self.zs

    def by_z(self, d):
        return {"col": self.ahead(d) * 4 + self.within, "row": self.y}


def greet(partners):
    barrier = pltpu.get_barrier_semaphore()
    for to in partners:
        pl.semaphore_signal(barrier, inc=1, device_id=to, device_id_type=MESH)
    pl.semaphore_wait(barrier, len(partners))


def remote(src, dst, send, recv, i, to):
    return pltpu.make_async_remote_copy(
        src_ref=src,
        dst_ref=dst,
        send_sem=send.at[i],
        recv_sem=recv.at[i],
        device_id=to,
        device_id_type=MESH,
    )


def add_low(a, b):
    return (a.astype(f32) + b.astype(f32)).astype(bf16)


def plane_scratch(zs, rows, width):
    half = zs // 2
    return [
        pltpu.VMEM((2, zs, 2, rows, width), bf16),
        pltpu.VMEM((2, zs, 2, rows, width), bf16),
        pltpu.VMEM((2, half, rows, width), bf16),
        pltpu.VMEM((half, 2, rows, width), bf16),
        pltpu.VMEM((half, rows, width), bf16),
        pltpu.VMEM((half, rows, width), bf16),
        pltpu.SemaphoreType.DMA((5,)),
        pltpu.SemaphoreType.DMA((5,)),
        pltpu.SemaphoreType.DMA,
    ]


class PlaneSum:
    def __init__(self, at, g, own, b1, b2x, b2y, b3y, b3x, send, recv, local):
        half = at.zs // 2
        self.at, self.half = at, half
        self.own, self.b1, self.b2x, self.b2y, self.b3y, self.b3x = own, b1, b2x, b2y, b3y, b3x
        self.g, self.send, self.recv, self.local = g, send, recv, local

    def keep(self):
        return pltpu.make_async_copy(self.g.at[:, :, :, self.at.core], self.own, self.local)

    def to_core(self):
        at = self.at
        return remote(self.g.at[:, :, :, 1 - at.core], self.b1, self.send, self.recv, 0, at.by_core)

    def second(self):
        at, half, sems = self.at, self.half, (self.send, self.recv)
        return (
            remote(self.b1.at[:, 0:half, 1 - at.x], self.b2x, *sems, 1, at.by_x),
            remote(self.b1.at[1 - at.y, half:], self.b2y, *sems, 2, at.by_y),
        )

    def third(self):
        at, sems = self.at, (self.send, self.recv)
        return (
            remote(self.b2x.at[1 - at.y], self.b3y, *sems, 3, at.by_y),
            remote(self.b2y.at[:, 1 - at.x], self.b3x, *sems, 4, at.by_x),
        )

    def stage1(self):
        self.keep().start()
        self.to_core().start()

    def stage2(self):
        self.keep().wait()
        self.to_core().wait()
        b1, own = self.b1, self.own

        @pl.loop(0, self.at.zs)
        def _(z):
            for y in range(2):
                for x in range(2):
                    b1[y, z, x] = add_low(b1[y, z, x], own[y, z, x])

        for copy in self.second():
            copy.start()

    def stage3(self):
        for copy in self.second():
            copy.wait()
        b1, b2x, b2y, half = self.b1, self.b2x, self.b2y, self.half

        @pl.loop(0, half)
        def _(z):
            for n in range(2):
                b2x[n, z] = add_low(b2x[n, z], b1[n, z, self.at.x])
                b2y[z, n] = add_low(b2y[z, n], b1[self.at.y, half + z, n])

        for copy in self.third():
            copy.start()

    def finish(self, out):
        for copy in self.third():
            copy.wait()
        half = self.half

        @pl.loop(0, half)
        def _(z):
            out[z] = add_low(self.b3y[z], self.b2x[self.at.y, z])
            out[half + z] = add_low(self.b3x[z], self.b2y[z, self.at.x])


def line_scratch(zs, rows, width):
    return [
        pltpu.VMEM((zs - 1, rows, width), bf16),
        pltpu.SemaphoreType.DMA((zs - 1,)),
        pltpu.SemaphoreType.DMA((zs - 1,)),
    ]


class LineSum:
    def __init__(self, at, h, held, send, recv):
        self.at, self.h, self.held = at, h, held
        self.copies = [
            remote(h.at[at.ahead(d)], held.at[d - 1], send, recv, d - 1, at.by_z(d))
            for d in range(1, at.zs)
        ]

    def start(self):
        for copy in self.copies:
            copy.start()

    def finish(self, out):
        for copy in self.copies:
            copy.wait()
        total = self.h[self.at.z].astype(f32)
        for d in range(1, self.at.zs):
            total = total + self.held[d - 1].astype(f32)
        out[...] = total


def final_kernel(zs, g_ref, h_ref, v_ref, o1_ref, o2_ref, vo_ref, mid, *scratch):
    plane, (v1, v2, v3, v4, va, vb, vsend, vrecv), line1, line2 = (
        scratch[:9],
        scratch[9:17],
        scratch[17:20],
        scratch[20:23],
    )
    at = Place(zs)
    greet([at.by_core, at.by_x, at.by_y] + [at.by_z(d) for d in range(1, zs)])
    first = PlaneSum(at, g_ref, *plane)
    second = LineSum(at, h_ref, *line2)
    first.stage1()
    vec1 = remote(v_ref, v1, vsend, vrecv, 0, at.by_core)
    vec1.start()
    second.start()
    vec1.wait()
    va[...] = v_ref[...] + v1[...]
    vec2 = remote(va, v2, vsend, vrecv, 1, at.by_x)
    vec2.start()
    first.stage2()
    vec2.wait()
    vb[...] = va[...] + v2[...]
    vec3 = remote(vb.at[1 - at.y], v3, vsend, vrecv, 2, at.by_y)
    vec3.start()
    first.stage3()
    vec3.wait()
    v4[0] = vb[at.y] + v3[...]
    vec4 = [
        remote(v4.at[0], v4.at[d], vsend, vrecv, 2 + d, at.by_z(d)) for d in range(1, zs)
    ]
    for copy in vec4:
        copy.start()
    first.finish(mid)
    third = LineSum(at, mid, *line1)
    third.start()
    for copy in vec4:
        copy.wait()
    total = v4[at.z % zs]
    for z in range(1, zs):
        total = total + v4[(at.z + zs - z) % zs]
    vo_ref[...] = total
    second.finish(o2_ref)
    third.finish(o1_ref)


def final(zs, g, h, v):
    rows, w1 = g.shape[4:]
    w2 = h.shape[2]
    width = v.shape[2]
    vmem = pl.BlockSpec(memory_space=pltpu.VMEM)
    return pl.pallas_call(
        functools.partial(final_kernel, zs),
        in_specs=[pl.BlockSpec(memory_space=pl.ANY), vmem, vmem],
        out_specs=[vmem, vmem, vmem],
        out_shape=[
            jax.ShapeDtypeStruct((rows, w1), f32),
            jax.ShapeDtypeStruct((rows, w2), f32),
            jax.ShapeDtypeStruct((1, width), f32),
        ],
        scratch_shapes=[
            pltpu.VMEM((zs, rows, w1), bf16),
            *plane_scratch(zs, rows, w1),
            pltpu.VMEM((2, 1, width), f32),
            pltpu.VMEM((2, 1, width), f32),
            pltpu.VMEM((1, width), f32),
            pltpu.VMEM((zs, 1, width), f32),
            pltpu.VMEM((2, 1, width), f32),
            pltpu.VMEM((2, 1, width), f32),
            pltpu.SemaphoreType.DMA((zs + 2,)),
            pltpu.SemaphoreType.DMA((zs + 2,)),
            *line_scratch(zs, rows, w1),
            *line_scratch(zs, rows, w2),
        ],
        compiler_params=params(collective_id=1, has_side_effects=True),
        name="final",
    )(g, h, v)


class PlaneGather:
    def __init__(self, at, h, g, send, recv):
        self.at, self.h, self.g, self.send, self.recv = at, h, g, send, recv

    def move(self, i, to, src, *where):
        dst = self.g.at[where]
        return remote(dst if src is None else src, dst, self.send, self.recv, i, to)

    def stage1(self):
        at, half = self.at, self.at.zs // 2
        y, x, core = at.y, at.x, at.core
        every, low, high = slice(None), slice(0, half), slice(half, at.zs)
        return (
            self.move(0, at.by_y, self.h.at[low], y, low, x, core),
            self.move(1, at.by_x, self.h.at[high], y, high, x, core),
            self.move(2, at.by_core, self.h, y, every, x, core),
        )

    def stage2(self):
        at, half = self.at, self.at.zs // 2
        y, x, core = at.y, at.x, at.core
        every, low, high = slice(None), slice(0, half), slice(half, at.zs)
        return (
            self.move(3, at.by_x, None, every, low, x, core),
            self.move(4, at.by_y, None, y, high, every, core),
            self.move(5, at.by_core, None, 1 - y, low, x, core),
            self.move(6, at.by_core, None, y, high, 1 - x, core),
        )

    def stage3(self):
        at, half = self.at, self.at.zs // 2
        y, x, core = at.y, at.x, at.core
        every, low, high = slice(None), slice(0, half), slice(half, at.zs)
        return (
            self.move(7, at.by_core, None, every, low, 1 - x, core),
            self.move(8, at.by_core, None, 1 - y, high, every, core),
        )


def start_all(copies):
    for copy in copies:
        copy.start()


def wait_all(copies):
    for copy in copies:
        copy.wait()


def front_kernel(
    zs, x_ref, s1_ref, s2_ref, vec_ref, q_ref, k_ref, v_ref, g_ref, h_ref, vo_ref, line,
    psend, precv, lsend, lrecv, vsend, vrecv, local,
):
    at = Place(zs)
    greet([at.by_core, at.by_x, at.by_y] + [at.by_z(d) for d in range(1, zs)])
    along = [
        remote(s1_ref, line.at[at.z], lsend, lrecv, d - 1, at.by_z(d)) for d in range(1, zs)
    ]
    start_all(along)
    vec = remote(vec_ref, vo_ref.at[at.y], vsend, vrecv, 0, at.by_y)
    vec.start()
    mine = [
        pltpu.make_async_copy(s1_ref, line.at[at.z], local.at[0]),
        pltpu.make_async_copy(s2_ref, h_ref.at[at.z], local.at[1]),
        pltpu.make_async_copy(vec_ref, vo_ref.at[at.y], local.at[2]),
    ]
    start_all(mine)
    wait_all(mine)
    wait_all(along)
    after = [
        remote(s2_ref, h_ref.at[at.z], lsend, lrecv, zs - 2 + d, at.by_z(d)) for d in range(1, zs)
    ]
    start_all(after)
    gather = PlaneGather(at, line, g_ref, psend, precv)
    keep = pltpu.make_async_copy(line, g_ref.at[at.y, :, at.x, at.core], local.at[3])
    keep.start()
    one = gather.stage1()
    start_all(one)
    keep.wait()
    wait_all(one)
    two = gather.stage2()
    start_all(two)
    wait_all(two)
    three = gather.stage3()
    start_all(three)
    vec.wait()
    wait_all(three)

    @pl.loop(0, LENGTH // QROWS)
    def _(n):
        rows = pl.ds(pl.multiple_of(n * QROWS, QROWS), QROWS)
        x = x_ref[rows, :]
        for r in range(2):
            w = g_ref[r].reshape(D, QKV_W)
            out = slice(r * HALF, (r + 1) * HALF)
            q = dot(x, w[:, :HALF]) + vo_ref[r, :, V_QB : V_QB + HALF]
            q_ref[rows, out] = (q.astype(bf16).astype(f32) * 0.125).astype(bf16)
            k_ref[rows, out] = dot(x, w[:, HALF : 2 * HALF]).astype(bf16)
            v = dot(x, w[:, 2 * HALF :]) + vo_ref[r, :, V_VB : V_VB + HALF]
            v_ref[rows, out] = v.astype(bf16)

    wait_all(after)


QROWS = 256


def front(zs, x, s1, s2, vec):
    rows = s1.shape[0]
    w1, w2 = s1.shape[1], s2.shape[1]
    vmem = pl.BlockSpec(memory_space=pltpu.VMEM)
    out = jax.ShapeDtypeStruct((LENGTH, D), bf16)
    return pl.pallas_call(
        functools.partial(front_kernel, zs),
        in_specs=[vmem] * 4,
        out_specs=[vmem] * 6,
        out_shape=[
            out,
            out,
            out,
            jax.ShapeDtypeStruct((2, zs, 2, 2, rows, w1), bf16),
            jax.ShapeDtypeStruct((zs, rows, w2), bf16),
            jax.ShapeDtypeStruct((2, 1, VEC_W), f32),
        ],
        scratch_shapes=[
            pltpu.VMEM((zs, rows, w1), bf16),
            pltpu.SemaphoreType.DMA((9,)),
            pltpu.SemaphoreType.DMA((9,)),
            pltpu.SemaphoreType.DMA((2 * zs - 2,)),
            pltpu.SemaphoreType.DMA((2 * zs - 2,)),
            pltpu.SemaphoreType.DMA((1,)),
            pltpu.SemaphoreType.DMA((1,)),
            pltpu.SemaphoreType.DMA((4,)),
        ],
        compiler_params=params(collective_id=3, has_side_effects=True),
        name="front",
    )(x, s1, s2, vec)


QT = 256
QTILES = LENGTH // QT


def head_lanes(a, x):
    lane = lax.broadcasted_iota(jnp.int32, x.shape, 1)
    return jnp.where((lane < HD) if a == 0 else (lane >= HD), x, jnp.zeros_like(x))


def both_heads(top, low):
    row = lax.broadcasted_iota(jnp.int32, top.shape, 0)
    return jnp.where(row < HD, top, low)


def hidden_pairs(rand):
    rows = jnp.arange(BLOCKS)[:, None]
    cols = jnp.arange(BLOCKS)[None, :]
    edge = (rows == 0) | (rows == BLOCKS - 1) | (cols == 0) | (cols == BLOCKS - 1)
    near = jnp.abs(rows - cols) <= 1
    chosen = (rand[:, :, :, None] == jnp.arange(BLOCKS)).any(axis=2)
    chosen = jnp.pad(chosen.transpose(1, 2, 0), ((0, 0), (0, 0), (1, 1)))
    table = jnp.where(chosen | (edge | near)[None], 0.0, NEG).astype(f32)
    return jnp.repeat(table, BLK, axis=2)


def attend_kernel(q_ref, k_ref, v_ref, hide_ref, c_ref, p_ref):
    kall = k_ref[...]
    vT = v_ref[...].T

    @pl.loop(0, QTILES)
    def _(n):
        at = pl.ds(pl.multiple_of(n * QT, QT), QT)
        q = q_ref[at, :]
        outs = []
        for a in range(2):
            s = dot_nt(kall, head_lanes(a, q)).reshape(BLOCKS, BLK, QT)
            s = (s + hide_ref[a, :, at][:, None, :]).reshape(LENGTH, QT)
            e = jnp.exp(s - jnp.max(s, axis=0, keepdims=True))
            p = (e * (1.0 / jnp.sum(e, axis=0, keepdims=True))).astype(bf16)
            p_ref[a, :, at] = p
            outs.append(dot(vT, p))
        c_ref[at, :] = both_heads(*outs).T.astype(bf16)


def attend_gather_kernel(zs, q_ref, k_ref, v_ref, hide_ref, h_ref, c_ref, p_ref, g_ref, send, recv, local):
    step = pl.program_id(0)
    at = Place(zs)
    gather = PlaneGather(at, h_ref, g_ref, send, recv)

    def keep():
        return pltpu.make_async_copy(h_ref, g_ref.at[at.y, :, at.x, at.core], local)

    @pl.when(step == 0)
    def _():
        greet([at.by_core, at.by_x, at.by_y])
        start_all(gather.stage1())
        keep().start()

    @pl.when(step == 2)
    def _():
        keep().wait()
        wait_all(gather.stage1())
        start_all(gather.stage2())

    attend_kernel(q_ref, k_ref, v_ref, hide_ref, c_ref, p_ref)

    @pl.when(step == H // 2 - 1)
    def _():
        wait_all(gather.stage2())
        start_all(gather.stage3())
        wait_all(gather.stage3())


def attend(q, k, v, hide, zs=0, h2=None):
    pair = pl.BlockSpec((LENGTH, 2 * HD), lambda h: (0, h))
    if zs:
        return pl.pallas_call(
            functools.partial(attend_gather_kernel, zs),
            grid=(H // 2,),
            in_specs=[
                pair,
                pair,
                pair,
                pl.BlockSpec((2, BLOCKS, LENGTH), lambda h: (h, 0, 0)),
                pl.BlockSpec(memory_space=pltpu.VMEM),
            ],
            out_specs=[
                pair,
                pl.BlockSpec((2, LENGTH, LENGTH), lambda h: (h, 0, 0)),
                pl.BlockSpec(memory_space=pl.ANY),
            ],
            out_shape=[
                jax.ShapeDtypeStruct((LENGTH, D), bf16),
                jax.ShapeDtypeStruct((H, LENGTH, LENGTH), bf16),
                jax.ShapeDtypeStruct((2, zs, 2, 2) + h2.shape[1:], bf16),
            ],
            scratch_shapes=[
                pltpu.SemaphoreType.DMA((9,)),
                pltpu.SemaphoreType.DMA((9,)),
                pltpu.SemaphoreType.DMA,
            ],
            compiler_params=params(collective_id=4, has_side_effects=True),
            name="attend_gather",
        )(q, k, v, hide, h2)
    return pl.pallas_call(
        attend_kernel,
        grid=(H // 2,),
        in_specs=[pair, pair, pair, pl.BlockSpec((2, BLOCKS, LENGTH), lambda h: (h, 0, 0))],
        out_specs=[pair, pl.BlockSpec((2, LENGTH, LENGTH), lambda h: (h, 0, 0))],
        out_shape=[
            jax.ShapeDtypeStruct((LENGTH, D), bf16),
            jax.ShapeDtypeStruct((H, LENGTH, LENGTH), bf16),
        ],
        compiler_params=params(),
        name="attend",
    )(q, k, v, hide)


def attend_sum_kernel(zs, q_ref, k_ref, v_ref, d_ref, p_ref, g_ref, dq_ref, dk_ref, dv_ref, h_ref, ds_s, *plane):
    step = pl.program_id(0)
    at = Place(zs)

    @pl.when(step == 0)
    def _():
        greet([at.by_core, at.by_x, at.by_y])
        PlaneSum(at, g_ref, *plane).stage1()

    @pl.when(step == 2)
    def _():
        PlaneSum(at, g_ref, *plane).stage2()

    @pl.when(step == 5)
    def _():
        PlaneSum(at, g_ref, *plane).stage3()

    attend_back_kernel(q_ref, k_ref, v_ref, d_ref, p_ref, dq_ref, dk_ref, dv_ref, ds_s)

    @pl.when(step == 5)
    def _():
        PlaneSum(at, g_ref, *plane).finish(h_ref)


def attend_back_kernel(q_ref, k_ref, v_ref, d_ref, p_ref, dq_ref, dk_ref, dv_ref, ds_s):
    vall = v_ref[...]
    kT = k_ref[...].T

    @pl.loop(0, QTILES)
    def _(n):
        at = pl.ds(pl.multiple_of(n * QT, QT), QT)
        d = d_ref[at, :]
        outs = []
        for a in range(2):
            dots = dot_nt(vall, head_lanes(a, d))
            p = p_ref[a, :, at].astype(f32)
            ds = (p * (dots - jnp.sum(dots * p, axis=0, keepdims=True))).astype(bf16)
            ds_s[a, :, at] = ds
            outs.append(dot(kT, ds))
        dq_ref[at, :] = (both_heads(*outs).T * 0.125).astype(bf16)

    dk_ref[...] = (
        dot(ds_s[0], head_lanes(0, q_ref[...])) + dot(ds_s[1], head_lanes(1, q_ref[...]))
    ).astype(bf16)
    dv_ref[...] = (
        dot(p_ref[0], head_lanes(0, d_ref[...])) + dot(p_ref[1], head_lanes(1, d_ref[...]))
    ).astype(bf16)


def attend_back(q, k, v, d, p, zs=0, g=None):
    pair = pl.BlockSpec((LENGTH, 2 * HD), lambda h: (0, h))
    out = jax.ShapeDtypeStruct((LENGTH, D), bf16)
    if zs:
        held = (zs,) + g.shape[4:]
        return pl.pallas_call(
            functools.partial(attend_sum_kernel, zs),
            grid=(H // 2,),
            in_specs=[
                pair,
                pair,
                pair,
                pair,
                pl.BlockSpec((2, LENGTH, LENGTH), lambda h: (h, 0, 0)),
                pl.BlockSpec(memory_space=pl.ANY),
            ],
            out_specs=[pair, pair, pair, pl.BlockSpec(held, lambda h: (0, 0, 0))],
            out_shape=[out, out, out, jax.ShapeDtypeStruct(held, bf16)],
            scratch_shapes=[pltpu.VMEM((2, LENGTH, LENGTH), bf16), *plane_scratch(*held)],
            compiler_params=params(collective_id=2, has_side_effects=True),
            name="attend_sum",
        )(q, k, v, d, p, g)
    return pl.pallas_call(
        attend_back_kernel,
        grid=(H // 2,),
        in_specs=[pair, pair, pair, pair, pl.BlockSpec((2, LENGTH, LENGTH), lambda h: (h, 0, 0))],
        out_specs=[pair, pair, pair],
        out_shape=[out, out, out],
        scratch_shapes=[pltpu.VMEM((2, LENGTH, LENGTH), bf16)],
        compiler_params=params(),
        name="attend_back",
    )(q, k, v, d, p)


TOK = 256
TSTEPS = LENGTH // TOK
FC = 768
TILES = REST_W // HALF


def gelu_parts(x):
    z = jnp.abs(x) * 0.7071067811865476
    t = 1.0 / (1.0 + 0.5 * z)
    poly = 0.17087277
    for c in (
        -0.82215223,
        1.48851587,
        -1.13520398,
        0.27886807,
        -0.18628806,
        0.09678418,
        0.37409196,
        1.00002368,
        -1.26551223,
    ):
        poly = poly * t + c
    tail = 0.5 * t * jnp.exp(poly - z * z)
    cdf = jnp.where(x >= 0, 1.0 - tail, tail)
    pdf = jnp.exp(-0.5 * x * x) * 0.3989422804014327
    return cdf, pdf


def norm(z, gain, shift):
    mean = jnp.mean(z, axis=1, keepdims=True)
    cen = z - mean
    var = jnp.mean(cen * cen, axis=1, keepdims=True)
    inv = lax.rsqrt(var + EPS)
    unit = cen * inv
    return unit * gain + shift, unit, inv


def norm_back(grad, unit, inv, gain):
    g = grad * gain
    return inv * (
        g - jnp.mean(g, axis=1, keepdims=True) - unit * jnp.mean(g * unit, axis=1, keepdims=True)
    )


def mid_kernel(
    ctx_ref,
    hid_ref,
    cot_ref,
    w_ref,
    vec_ref,
    out_ref,
    resid_ref,
    dctx_ref,
    dw_ref,
    vs_ref,
    act_s,
    bg_s,
    dg_s,
    flT_s,
    brT_s,
    agT_s,
):
    step = pl.program_id(0)

    def vec(off, width=HALF):
        return jnp.concatenate(
            [vec_ref[0, :, off : off + width], vec_ref[1, :, off : off + width]], axis=1
        )

    def add_vec(off, value, width=HALF):
        total = jnp.sum(value, axis=0, keepdims=True)
        vs_ref[0, :, off : off + width] += total[:, :width]
        vs_ref[1, :, off : off + width] += total[:, width:]

    @pl.when(step == 0)
    def _():
        vs_ref[...] = jnp.zeros_like(vs_ref)

    @pl.when(step < TSTEPS)
    def _():
        rows = pl.ds(pl.multiple_of(step * TOK, TOK), TOK)
        ctx = ctx_ref[rows, :]
        att = dot_nt(ctx[:, :HALF], w_ref[0, :, :HALF]) + dot_nt(
            ctx[:, HALF:], w_ref[1, :, :HALF]
        )
        z = hid_ref[...].astype(f32) + (att + vec(V_OB))
        gain1 = vec(V_G1)
        first, unit1, inv1 = norm(z, gain1, vec(V_S1))
        low = first.astype(bf16)
        flT_s[:, rows] = low.T
        branch = None
        for r in range(2):
            for c in range(0, FHALF, FC):
                at = r * FHALF + c
                before = (
                    dot(low, w_ref[r, :, HALF + c : HALF + c + FC])
                    + vec_ref[r, :, V_UB + c : V_UB + c + FC]
                )
                cdf, pdf = gelu_parts(before)
                act = (before * cdf).astype(bf16)
                act_s[rows, at : at + FC] = act
                dg_s[:, at : at + FC] = cdf + before * pdf
                part = dot_nt(act, w_ref[r, :, HALF + FHALF + c : HALF + FHALF + c + FC])
                branch = part if branch is None else branch + part
        gain2 = vec(V_G2)
        output, unit2, inv2 = norm(first + (branch + vec(V_DB)), gain2, vec(V_S2))
        out_ref[...] = output
        cot = cot_ref[...].astype(f32)
        grad2 = norm_back(cot, unit2, inv2, gain2)
        add_vec(V_G2, cot * unit2)
        add_vec(V_S2, cot)
        bgrad = grad2.astype(bf16)
        add_vec(V_DB, bgrad.astype(f32))
        brT_s[:, rows] = bgrad.T
        fgrad = grad2
        for r in range(2):
            for c in range(0, FHALF, FC):
                at = r * FHALF + c
                dact = dot(bgrad, w_ref[r, :, HALF + FHALF + c : HALF + FHALF + c + FC])
                dbef = (dact * dg_s[:, at : at + FC]).astype(bf16)
                bg_s[rows, at : at + FC] = dbef
                vs_ref[r, :, V_UB + c : V_UB + c + FC] += jnp.sum(
                    dbef.astype(f32), axis=0, keepdims=True
                )
                fgrad = fgrad + dot_nt(dbef, w_ref[r, :, HALF + c : HALF + c + FC])
        add_vec(V_G1, fgrad * unit1)
        add_vec(V_S1, fgrad)
        resid = norm_back(fgrad, unit1, inv1, gain1)
        resid_ref[...] = resid
        agrad = resid.astype(bf16)
        add_vec(V_OB, agrad.astype(f32))
        agT_s[:, rows] = agrad.T
        for r in range(2):
            dctx_ref[:, r * HALF : (r + 1) * HALF] = dot(agrad, w_ref[r, :, :HALF]).astype(bf16)

    idx = step - TSTEPS
    r = idx // TILES
    j = idx % TILES

    @pl.when((idx >= 0) & (j == 0))
    def _():
        cols = pl.ds(pl.multiple_of(r * HALF, HALF), HALF)
        dw_ref[0] = dot(agT_s[...], ctx_ref[:, cols]).astype(bf16)

    @pl.when((idx >= 0) & (j >= 1) & (j <= 4))
    def _():
        cols = pl.ds(pl.multiple_of(r * FHALF + (j - 1) * HALF, HALF), HALF)
        dw_ref[0] = dot(flT_s[...], bg_s[:, cols]).astype(bf16)

    @pl.when((idx >= 0) & (j >= 5))
    def _():
        cols = pl.ds(pl.multiple_of(r * FHALF + (j - 5) * HALF, HALF), HALF)
        dw_ref[0] = dot(brT_s[...], act_s[:, cols]).astype(bf16)


def middle(ctx, hid, cot, w, vec):
    def tok(s):
        return (jnp.minimum(s, TSTEPS - 1), 0)

    def tile(s):
        idx = jnp.maximum(s - TSTEPS, 0)
        return (idx // TILES, 0, idx % TILES)

    rows = pl.BlockSpec((TOK, D), tok)
    return pl.pallas_call(
        mid_kernel,
        grid=(TSTEPS + 2 * TILES,),
        in_specs=[
            pl.BlockSpec((LENGTH, D), lambda s: (0, 0), pipeline_mode=pl.Buffered(1)),
            rows,
            rows,
            pl.BlockSpec((2, D, REST_W), lambda s: (0, 0, 0), pipeline_mode=pl.Buffered(1)),
            pl.BlockSpec((2, 1, VEC_W), lambda s: (0, 0, 0), pipeline_mode=pl.Buffered(1)),
        ],
        out_specs=[
            rows,
            rows,
            rows,
            pl.BlockSpec((1, D, HALF), tile),
            pl.BlockSpec((2, 1, VEC_W), lambda s: (0, 0, 0)),
        ],
        out_shape=[
            jax.ShapeDtypeStruct((LENGTH, D), f32),
            jax.ShapeDtypeStruct((LENGTH, D), f32),
            jax.ShapeDtypeStruct((LENGTH, D), bf16),
            jax.ShapeDtypeStruct((2, D, REST_W), bf16),
            jax.ShapeDtypeStruct((2, 1, VEC_W), f32),
        ],
        scratch_shapes=[
            pltpu.VMEM((LENGTH, FF), bf16),
            pltpu.VMEM((LENGTH, FF), bf16),
            pltpu.VMEM((TOK, FF), f32),
            pltpu.VMEM((D, LENGTH), bf16),
            pltpu.VMEM((D, LENGTH), bf16),
            pltpu.VMEM((D, LENGTH), bf16),
        ],
        compiler_params=params(),
        name="middle",
    )(ctx, hid, cot, w, vec)


LTOK = 512
LSTEPS = LENGTH // LTOK


def last_kernel(hid_ref, dq_ref, dk_ref, dv_ref, resid_ref, w_ref, hg_ref, dw_ref, vs_ref, hT_s):
    step = pl.program_id(0)

    @pl.when(step == 0)
    def _():
        hT_s[...] = hid_ref[...].T
        for ref, off in ((dq_ref, 0), (dv_ref, HALF)):
            total = jnp.sum(ref[...].astype(f32), axis=0, keepdims=True)
            vs_ref[0, :, off : off + HALF] = total[:, :HALF]
            vs_ref[1, :, off : off + HALF] = total[:, HALF:]

    @pl.when(step < LSTEPS)
    def _():
        rows = pl.ds(pl.multiple_of(step * LTOK, LTOK), LTOK)
        acc = resid_ref[...]
        for m, ref in enumerate((dq_ref, dk_ref, dv_ref)):
            for r in range(2):
                acc = acc + dot_nt(
                    ref[rows, r * HALF : (r + 1) * HALF],
                    w_ref[r, :, m * HALF : (m + 1) * HALF],
                )
        hg_ref[...] = acc

    idx = step - LSTEPS
    cols = pl.ds(pl.multiple_of(jnp.maximum(idx, 0) // 3 * HALF, HALF), HALF)
    for m, ref in enumerate((dq_ref, dk_ref, dv_ref)):

        @pl.when((idx >= 0) & (idx % 3 == m))
        def _(ref=ref):
            dw_ref[0] = dot(hT_s[...], ref[:, cols]).astype(bf16)


def last(hid, dq, dk, dv, resid, w):
    whole = pl.BlockSpec((LENGTH, D), lambda s: (0, 0), pipeline_mode=pl.Buffered(1))
    rows = pl.BlockSpec((LTOK, D), lambda s: (jnp.minimum(s, LSTEPS - 1), 0))

    def tile(s):
        idx = jnp.maximum(s - LSTEPS, 0)
        return (idx // 3, 0, idx % 3)

    return pl.pallas_call(
        last_kernel,
        grid=(LSTEPS + 6,),
        in_specs=[
            whole,
            whole,
            whole,
            whole,
            rows,
            pl.BlockSpec((2, D, QKV_W), lambda s: (0, 0, 0), pipeline_mode=pl.Buffered(1)),
        ],
        out_specs=[
            rows,
            pl.BlockSpec((1, D, HALF), tile),
            pl.BlockSpec((2, 1, 2 * HALF), lambda s: (0, 0, 0)),
        ],
        out_shape=[
            jax.ShapeDtypeStruct((LENGTH, D), f32),
            jax.ShapeDtypeStruct((2, D, QKV_W), bf16),
            jax.ShapeDtypeStruct((2, 1, 2 * HALF), f32),
        ],
        scratch_shapes=[pltpu.VMEM((D, LENGTH), bf16)],
        compiler_params=params(),
        name="last",
    )(hid, dq, dk, dv, resid, w)


def gather_parts(parts, rows_n, cols_n):
    packed = jnp.concatenate(parts, axis=1)
    every = lax.all_gather(packed, ("row", "col"), axis=0, tiled=True)
    every = every.reshape(rows_n, D, packed.shape[1])
    if rows_n == 2:
        return every
    pieces, at = [], 0
    for part in parts:
        width = part.shape[1]
        one = every[:, :, at : at + width].reshape(2, rows_n // 2, D, width)
        pieces.append(one.transpose(0, 2, 1, 3).reshape(2, D, rows_n // 2 * width))
        at += width
    return jnp.concatenate(pieces, axis=2)


def scatter_parts(full, halves, rows_n, cols_n):
    widths = [h * 2 // rows_n for h in halves]
    if rows_n != 2:
        pieces, at = [], 0
        for half, width in zip(halves, widths):
            one = full[:, :, at : at + half].reshape(2, D, rows_n // 2, width)
            pieces.append(one.transpose(0, 2, 1, 3).reshape(rows_n, D, width))
            at += half
        full = jnp.concatenate(pieces, axis=2)
    flat = full.reshape(rows_n * D, sum(widths))
    mine = lax.psum_scatter(flat, ("row", "col"), scatter_dimension=0, tiled=True)
    mine = mine.astype(f32)
    out, at = [], 0
    for width in widths:
        out.append(mine[:, at : at + width])
        at += width
    return out


VEC_HALVES = (HALF, HALF, HALF, FHALF, HALF, HALF, HALF, HALF, HALF)


def on_device(
    rows_n,
    cols_n,
    hidden,
    cotangent,
    rand_blocks,
    w_query,
    w_key,
    w_value,
    w_out,
    w_up,
    w_down,
    *vectors,
):
    zs = cols_n // 4
    staged = rows_n == 2 and cols_n % 8 == 0
    hide = hidden_pairs(rand_blocks[0])
    if staged:
        vec = jnp.concatenate(vectors).astype(f32)[None]
        s1 = jnp.concatenate([w_query, w_key, w_value], axis=1)
        s2 = jnp.concatenate([w_out.T, w_up, w_down.T], axis=1)
        q, k, v, w1, h2, vec = front(zs, hidden, s1, s2, vec)
        ctx, p, w2 = attend(q, k, v, hide, zs, h2)
        w1, w2 = w1.reshape(2, D, QKV_W), w2.reshape(2, D, REST_W)
    else:
        vec = lax.all_gather(jnp.concatenate(vectors).astype(f32), "row", axis=0, tiled=False)
        if rows_n != 2:
            pieces, at = [], 0
            for half in VEC_HALVES:
                width = half * 2 // rows_n
                pieces.append(vec[:, at : at + width].reshape(2, half))
                at += width
            vec = jnp.concatenate(pieces, axis=1)
        vec = vec.reshape(2, 1, VEC_W)
        w1 = gather_parts([w_query, w_key, w_value], rows_n, cols_n)
        w2 = gather_parts([w_out.T, w_up, w_down.T], rows_n, cols_n)
        q, k, v = qkv(hidden, w1, vec)
        ctx, p = attend(q, k, v, hide)
    output, resid, dctx, dw2, vs2 = middle(ctx, hidden, cotangent, w2, vec)
    if staged:
        spread = (2, zs, 2, 2, D // cols_n)
        g2 = dw2.reshape(spread + (REST_W,))
        dq, dk, dv, h2 = attend_back(q, k, v, dctx, p, zs, g2)
    else:
        dq, dk, dv = attend_back(q, k, v, dctx, p)
    hgrad, dw1, vs1 = last(hidden, dq, dk, dv, resid, w1)
    vs = jnp.concatenate([vs1, vs2[:, :, 2 * HALF :]], axis=2)
    if staged:
        m1, m2, vs = final(zs, dw1.reshape(spread + (QKV_W,)), h2, vs)
        g_q, g_k, g_v = (m1[:, n * HALF : (n + 1) * HALF] for n in range(3))
        g_out = m2[:, :HALF].T
        g_up = m2[:, HALF : HALF + FHALF]
        g_down = m2[:, HALF + FHALF :].T
        sums, at = [], 0
        for width in VEC_HALVES:
            sums.append(vs[0, at : at + width])
            at += width
        return (output, hgrad, g_q, g_k, g_v, g_out, g_up, g_down, *sums)
    g_out, g_up, g_down = scatter_parts(dw2, (HALF, FHALF, FHALF), rows_n, cols_n)
    g_q, g_k, g_v = scatter_parts(dw1, (HALF, HALF, HALF), rows_n, cols_n)
    vs = lax.psum(vs.reshape(2, VEC_W), ("col", "row"))
    row = lax.axis_index("row")
    sums, at = [], 0
    for half in VEC_HALVES:
        width = half * 2 // rows_n
        both = vs[:, at : at + half].reshape(rows_n, width)
        sums.append(lax.dynamic_index_in_dim(both, row, 0, keepdims=False))
        at += half
    return (output, hgrad, g_q, g_k, g_v, g_out.T, g_up, g_down.T, *sums)


def solution(mesh):
    rows_n, cols_n = mesh.shape["row"], mesh.shape["col"]
    tokens = P(("col", "row"), None)
    placed = (
        tokens,
        tokens,
        P(("col", "row"), None, None, None),
        P("col", "row"),
        P("col", "row"),
        P("col", "row"),
        P("row", "col"),
        P("col", "row"),
        P("row", "col"),
    ) + (P("row"),) * 9
    return jax.shard_map(
        functools.partial(on_device, rows_n, cols_n),
        mesh=mesh,
        in_specs=placed,
        out_specs=(
            tokens,
            tokens,
            P("col", "row"),
            P("col", "row"),
            P("col", "row"),
            P("row", "col"),
            P("col", "row"),
            P("row", "col"),
        )
        + (P("row"),) * 9,
        check_vma=False,
    )
```

```python
import functools

import jax
import jax.numpy as jnp
from jax import lax
from jax.experimental import pallas as pl
from jax.experimental.pallas import tpu as pltpu
from jax.sharding import PartitionSpec as P

D = 768
H = 12
FF = 3072
BLK = 64
LENGTH = 1024
BLOCKS = LENGTH // BLK
HD = D // H
RAND = 3
EPS = 1e-12
NEG = -1e30
VMEM_BYTES = 64 * 1000 * 1000

HALF = D // 2
FHALF = FF // 2
QKV_W = 3 * HALF
REST_W = HALF + 2 * FHALF
VEC_W = 8 * HALF + FHALF
V_QB, V_VB, V_OB, V_UB = 0, HALF, 2 * HALF, 3 * HALF
V_DB = V_UB + FHALF
V_G1, V_S1, V_G2, V_S2 = V_DB + HALF, V_DB + 2 * HALF, V_DB + 3 * HALF, V_DB + 4 * HALF

f32 = jnp.float32
bf16 = jnp.bfloat16


def dot(a, b):
    return jnp.dot(a, b, preferred_element_type=f32)


def dot_nt(a, b):
    return lax.dot_general(a, b, (((1,), (1,)), ((), ())), preferred_element_type=f32)


def dot_tn(a, b):
    return lax.dot_general(a, b, (((0,), (0,)), ((), ())), preferred_element_type=f32)


def params(**kw):
    return pltpu.CompilerParams(vmem_limit_bytes=VMEM_BYTES, **kw)


def qkv_kernel(x_ref, w_ref, vec_ref, q_ref, k_ref, v_ref):
    r = pl.program_id(0)
    j = pl.program_id(1)
    acc = dot(x_ref[...], w_ref[0])
    vec = vec_ref[0]

    @pl.when(j == 0)
    def _():
        q_ref[...] = ((acc + vec[:, V_QB : V_QB + HALF]).astype(bf16).astype(f32) * 0.125).astype(bf16)

    @pl.when(j == 1)
    def _():
        k_ref[...] = acc.astype(bf16)

    @pl.when(j == 2)
    def _():
        v_ref[...] = (acc + vec[:, V_VB : V_VB + HALF]).astype(bf16)


def qkv(x, w, vec):
    out = jax.ShapeDtypeStruct((LENGTH, D), bf16)
    col = pl.BlockSpec((LENGTH, HALF), lambda r, j: (0, r))
    return pl.pallas_call(
        qkv_kernel,
        grid=(2, 3),
        in_specs=[
            pl.BlockSpec((LENGTH, D), lambda r, j: (0, 0)),
            pl.BlockSpec((1, D, HALF), lambda r, j: (r, 0, j)),
            pl.BlockSpec((1, 1, VEC_W), lambda r, j: (r, 0, 0)),
        ],
        out_specs=[col, col, col],
        out_shape=[out, out, out],
        compiler_params=params(),
        name="qkv",
    )(x, w, vec)


MESH = pl.DeviceIdType.MESH


class Place:
    def __init__(self, zs):
        c = lax.axis_index("col")
        y = lax.axis_index("row")
        self.zs = zs
        self.core, self.x, self.y, self.z = c % 2, c // 2 % 2, y, c // 4
        self.by_core = {"col": c + 1 - 2 * self.core, "row": y}
        self.by_x = {"col": c + 2 - 4 * self.x, "row": y}
        self.by_y = {"col": c, "row": 1 - y}
        self.within = c % 4

    def ahead(self, d):
        return (self.z + d) % self.zs

    def by_z(self, d):
        return {"col": self.ahead(d) * 4 + self.within, "row": self.y}


def greet(partners):
    barrier = pltpu.get_barrier_semaphore()
    for to in partners:
        pl.semaphore_signal(barrier, inc=1, device_id=to, device_id_type=MESH)
    pl.semaphore_wait(barrier, len(partners))


def remote(src, dst, send, recv, i, to):
    return pltpu.make_async_remote_copy(
        src_ref=src,
        dst_ref=dst,
        send_sem=send.at[i],
        recv_sem=recv.at[i],
        device_id=to,
        device_id_type=MESH,
    )


def add_low(a, b):
    return (a.astype(f32) + b.astype(f32)).astype(bf16)


def plane_scratch(zs, rows, width):
    half = zs // 2
    return [
        pltpu.VMEM((2, zs, 2, rows, width), bf16),
        pltpu.VMEM((2, zs, 2, rows, width), bf16),
        pltpu.VMEM((2, half, rows, width), bf16),
        pltpu.VMEM((half, 2, rows, width), bf16),
        pltpu.VMEM((half, rows, width), bf16),
        pltpu.VMEM((half, rows, width), bf16),
        pltpu.SemaphoreType.DMA((5,)),
        pltpu.SemaphoreType.DMA((5,)),
        pltpu.SemaphoreType.DMA,
    ]


class PlaneSum:
    def __init__(self, at, g, own, b1, b2x, b2y, b3y, b3x, send, recv, local):
        half = at.zs // 2
        self.at, self.half = at, half
        self.own, self.b1, self.b2x, self.b2y, self.b3y, self.b3x = own, b1, b2x, b2y, b3y, b3x
        self.g, self.send, self.recv, self.local = g, send, recv, local

    def keep(self):
        return pltpu.make_async_copy(self.g.at[:, :, :, self.at.core], self.own, self.local)

    def to_core(self):
        at = self.at
        return remote(self.g.at[:, :, :, 1 - at.core], self.b1, self.send, self.recv, 0, at.by_core)

    def second(self):
        at, half, sems = self.at, self.half, (self.send, self.recv)
        return (
            remote(self.b1.at[:, 0:half, 1 - at.x], self.b2x, *sems, 1, at.by_x),
            remote(self.b1.at[1 - at.y, half:], self.b2y, *sems, 2, at.by_y),
        )

    def third(self):
        at, sems = self.at, (self.send, self.recv)
        return (
            remote(self.b2x.at[1 - at.y], self.b3y, *sems, 3, at.by_y),
            remote(self.b2y.at[:, 1 - at.x], self.b3x, *sems, 4, at.by_x),
        )

    def stage1(self):
        if self.own is not None:
            self.keep().start()
        self.to_core().start()

    def stage2(self):
        if self.own is not None:
            self.keep().wait()
        self.to_core().wait()
        b1, own, core = self.b1, self.own, self.at.core

        @pl.loop(0, self.at.zs)
        def _(z):
            for y in range(2):
                for x in range(2):
                    mine = self.g[y, z, x, core] if own is None else own[y, z, x]
                    b1[y, z, x] = add_low(b1[y, z, x], mine)

        for copy in self.second():
            copy.start()

    def stage3(self):
        for copy in self.second():
            copy.wait()
        b1, b2x, b2y, half = self.b1, self.b2x, self.b2y, self.half

        @pl.loop(0, half)
        def _(z):
            for n in range(2):
                b2x[n, z] = add_low(b2x[n, z], b1[n, z, self.at.x])
                b2y[z, n] = add_low(b2y[z, n], b1[self.at.y, half + z, n])

        for copy in self.third():
            copy.start()

    def finish(self, out):
        for copy in self.third():
            copy.wait()
        half = self.half

        @pl.loop(0, half)
        def _(z):
            out[z] = add_low(self.b3y[z], self.b2x[self.at.y, z])
            out[half + z] = add_low(self.b3x[z], self.b2y[z, self.at.x])


def line_scratch(zs, rows, width):
    return [
        pltpu.VMEM((zs - 1, rows, width), bf16),
        pltpu.SemaphoreType.DMA((zs - 1,)),
        pltpu.SemaphoreType.DMA((zs - 1,)),
    ]


class LineSum:
    def __init__(self, at, h, held, send, recv):
        self.at, self.h, self.held = at, h, held
        self.copies = [
            remote(h.at[at.ahead(d)], held.at[d - 1], send, recv, d - 1, at.by_z(d))
            for d in range(1, at.zs)
        ]

    def start(self):
        for copy in self.copies:
            copy.start()

    def finish(self, out):
        for copy in self.copies:
            copy.wait()
        total = self.h[self.at.z].astype(f32)
        for d in range(1, self.at.zs):
            total = total + self.held[d - 1].astype(f32)
        out[...] = total


class PlaneGather:
    def __init__(self, at, h, g, send, recv):
        self.at, self.h, self.g, self.send, self.recv = at, h, g, send, recv

    def move(self, i, to, src, *where):
        dst = self.g.at[where]
        return remote(dst if src is None else src, dst, self.send, self.recv, i, to)

    def stage1(self):
        at, half = self.at, self.at.zs // 2
        y, x, core = at.y, at.x, at.core
        every, low, high = slice(None), slice(0, half), slice(half, at.zs)
        return (
            self.move(0, at.by_y, self.h.at[low], y, low, x, core),
            self.move(1, at.by_x, self.h.at[high], y, high, x, core),
            self.move(2, at.by_core, self.h, y, every, x, core),
        )

    def stage2(self):
        at, half = self.at, self.at.zs // 2
        y, x, core = at.y, at.x, at.core
        every, low, high = slice(None), slice(0, half), slice(half, at.zs)
        return (
            self.move(3, at.by_x, None, every, low, x, core),
            self.move(4, at.by_y, None, y, high, every, core),
            self.move(5, at.by_core, None, 1 - y, low, x, core),
            self.move(6, at.by_core, None, y, high, 1 - x, core),
        )

    def stage3(self):
        at, half = self.at, self.at.zs // 2
        y, x, core = at.y, at.x, at.core
        every, low, high = slice(None), slice(0, half), slice(half, at.zs)
        return (
            self.move(7, at.by_core, None, every, low, 1 - x, core),
            self.move(8, at.by_core, None, 1 - y, high, every, core),
        )


def start_all(copies):
    for copy in copies:
        copy.start()


def wait_all(copies):
    for copy in copies:
        copy.wait()


def front_kernel(
    zs, x_ref, wq_ref, wk_ref, wv_ref, wo_ref, wu_ref, wd_ref, *refs,
):
    vector_refs, refs = refs[:9], refs[9:]
    q_ref, k_ref, v_ref, g_ref, h_ref, vo_ref, line, s2, vec_s = refs[:9]
    psend, precv, lsend, lrecv, vsend, vrecv, local = refs[9:]
    at = Place(zs)
    mine = [
        pltpu.make_async_copy(ref, line.at[at.z, :, n * HALF : (n + 1) * HALF], local.at[n])
        for n, ref in enumerate((wq_ref, wk_ref, wv_ref))
    ]
    start_all(mine)
    greet([at.by_core, at.by_x, at.by_y] + [at.by_z(d) for d in range(1, zs)])
    wait_all(mine)
    along = [
        remote(line.at[at.z], line.at[at.z], lsend, lrecv, d - 1, at.by_z(d))
        for d in range(1, zs)
    ]
    start_all(along)
    off = 0
    for ref in vector_refs:
        width = ref.shape[0]
        vec_s[:, off : off + width] = ref[...].astype(f32).reshape(1, width)
        off += width
    s2[:, :HALF] = wo_ref[...].T
    s2[:, HALF : HALF + FHALF] = wu_ref[...]
    s2[:, HALF + FHALF :] = wd_ref[...].T
    vo_ref[at.y] = vec_s[...]
    h_ref[at.z] = s2[...]
    vec = remote(vec_s, vo_ref.at[at.y], vsend, vrecv, 0, at.by_y)
    vec.start()
    wait_all(along)
    after = [
        remote(s2, h_ref.at[at.z], lsend, lrecv, zs - 2 + d, at.by_z(d)) for d in range(1, zs)
    ]
    start_all(after)
    gather = PlaneGather(at, line, g_ref, psend, precv)
    keep = pltpu.make_async_copy(line, g_ref.at[at.y, :, at.x, at.core], local.at[3])
    keep.start()
    one = gather.stage1()
    start_all(one)
    keep.wait()
    wait_all(one)
    two = gather.stage2()
    start_all(two)
    wait_all(two)
    three = gather.stage3()
    start_all(three)
    vec.wait()
    wait_all(three)

    @pl.loop(0, LENGTH // QROWS)
    def _(n):
        rows = pl.ds(pl.multiple_of(n * QROWS, QROWS), QROWS)
        x = x_ref[rows, :]
        for r in range(2):
            w = g_ref[r].reshape(D, QKV_W)
            out = slice(r * HALF, (r + 1) * HALF)
            q = dot(x, w[:, :HALF]) + vo_ref[r, :, V_QB : V_QB + HALF]
            q_ref[rows, out] = (q.astype(bf16).astype(f32) * 0.125).astype(bf16)
            k_ref[rows, out] = dot(x, w[:, HALF : 2 * HALF]).astype(bf16)
            v = dot(x, w[:, 2 * HALF :]) + vo_ref[r, :, V_VB : V_VB + HALF]
            v_ref[rows, out] = v.astype(bf16)

    wait_all(after)


QROWS = 256


def front(zs, x, weights, vectors):
    rows = weights[0].shape[0]
    w1, w2 = QKV_W, REST_W
    vmem = pl.BlockSpec(memory_space=pltpu.VMEM)
    out = jax.ShapeDtypeStruct((LENGTH, D), bf16)
    return pl.pallas_call(
        functools.partial(front_kernel, zs),
        in_specs=[vmem] * 16,
        out_specs=[vmem] * 6,
        out_shape=[
            out,
            out,
            out,
            jax.ShapeDtypeStruct((2, zs, 2, 2, rows, w1), bf16),
            jax.ShapeDtypeStruct((zs, rows, w2), bf16),
            jax.ShapeDtypeStruct((2, 1, VEC_W), f32),
        ],
        scratch_shapes=[
            pltpu.VMEM((zs, rows, w1), bf16),
            pltpu.VMEM((rows, w2), bf16),
            pltpu.VMEM((1, VEC_W), f32),
            pltpu.SemaphoreType.DMA((9,)),
            pltpu.SemaphoreType.DMA((9,)),
            pltpu.SemaphoreType.DMA((2 * zs - 2,)),
            pltpu.SemaphoreType.DMA((2 * zs - 2,)),
            pltpu.SemaphoreType.DMA((1,)),
            pltpu.SemaphoreType.DMA((1,)),
            pltpu.SemaphoreType.DMA((4,)),
        ],
        compiler_params=params(collective_id=3, has_side_effects=True),
        name="front",
    )(x, *weights, *vectors)


QT = 256
QTILES = LENGTH // QT


def head_lanes(a, x):
    lane = lax.broadcasted_iota(jnp.int32, x.shape, 1)
    return jnp.where((lane < HD) if a == 0 else (lane >= HD), x, jnp.zeros_like(x))


def both_heads(top, low):
    row = lax.broadcasted_iota(jnp.int32, top.shape, 0)
    return jnp.where(row < HD, top, low)


def hidden_pairs(rand):
    rows = jnp.arange(BLOCKS)[:, None]
    cols = jnp.arange(BLOCKS)[None, :]
    edge = (rows == 0) | (rows == BLOCKS - 1) | (cols == 0) | (cols == BLOCKS - 1)
    near = jnp.abs(rows - cols) <= 1
    chosen = (rand[:, :, :, None] == jnp.arange(BLOCKS)).any(axis=2)
    chosen = jnp.pad(chosen.transpose(1, 2, 0), ((0, 0), (0, 0), (1, 1)))
    table = jnp.where(chosen | (edge | near)[None], 0.0, NEG).astype(f32)
    return jnp.repeat(table, BLK, axis=2)


def attend_kernel(q_ref, k_ref, v_ref, hide_ref, c_ref, p_ref):
    kall = k_ref[...]
    vT = v_ref[...].T

    @pl.loop(0, QTILES)
    def _(n):
        at = pl.ds(pl.multiple_of(n * QT, QT), QT)
        q = q_ref[at, :]
        outs = []
        for a in range(2):
            s = dot_nt(kall, head_lanes(a, q)).reshape(BLOCKS, BLK, QT)
            s = (s + hide_ref[a, :, at][:, None, :]).reshape(LENGTH, QT)
            e = jnp.exp(s - jnp.max(s, axis=0, keepdims=True))
            p = (e * (1.0 / jnp.sum(e, axis=0, keepdims=True))).astype(bf16)
            p_ref[a, :, at] = p
            outs.append(dot(vT, p))
        c_ref[at, :] = both_heads(*outs).T.astype(bf16)


def attend_gather_kernel(zs, q_ref, k_ref, v_ref, hide_ref, h_ref, c_ref, p_ref, g_ref, send, recv, local):
    step = pl.program_id(0)
    at = Place(zs)
    gather = PlaneGather(at, h_ref, g_ref, send, recv)

    def keep():
        return pltpu.make_async_copy(h_ref, g_ref.at[at.y, :, at.x, at.core], local)

    @pl.when(step == 0)
    def _():
        greet([at.by_core, at.by_x, at.by_y])
        start_all(gather.stage1())
        keep().start()

    @pl.when(step == 2)
    def _():
        keep().wait()
        wait_all(gather.stage1())
        start_all(gather.stage2())

    attend_kernel(q_ref, k_ref, v_ref, hide_ref, c_ref, p_ref)

    @pl.when(step == H // 2 - 1)
    def _():
        wait_all(gather.stage2())
        start_all(gather.stage3())
        wait_all(gather.stage3())


def attend(q, k, v, hide, zs=0, h2=None):
    pair = pl.BlockSpec((LENGTH, 2 * HD), lambda h: (0, h))
    if zs:
        return pl.pallas_call(
            functools.partial(attend_gather_kernel, zs),
            grid=(H // 2,),
            in_specs=[
                pair,
                pair,
                pair,
                pl.BlockSpec((2, BLOCKS, LENGTH), lambda h: (h, 0, 0)),
                pl.BlockSpec(memory_space=pltpu.VMEM),
            ],
            out_specs=[
                pair,
                pl.BlockSpec((2, LENGTH, LENGTH), lambda h: (h, 0, 0)),
                pl.BlockSpec(memory_space=pl.ANY),
            ],
            out_shape=[
                jax.ShapeDtypeStruct((LENGTH, D), bf16),
                jax.ShapeDtypeStruct((H, LENGTH, LENGTH), bf16),
                jax.ShapeDtypeStruct((2, zs, 2, 2) + h2.shape[1:], bf16),
            ],
            scratch_shapes=[
                pltpu.SemaphoreType.DMA((9,)),
                pltpu.SemaphoreType.DMA((9,)),
                pltpu.SemaphoreType.DMA,
            ],
            compiler_params=params(collective_id=4, has_side_effects=True),
            name="attend_gather",
        )(q, k, v, hide, h2)
    return pl.pallas_call(
        attend_kernel,
        grid=(H // 2,),
        in_specs=[pair, pair, pair, pl.BlockSpec((2, BLOCKS, LENGTH), lambda h: (h, 0, 0))],
        out_specs=[pair, pl.BlockSpec((2, LENGTH, LENGTH), lambda h: (h, 0, 0))],
        out_shape=[
            jax.ShapeDtypeStruct((LENGTH, D), bf16),
            jax.ShapeDtypeStruct((H, LENGTH, LENGTH), bf16),
        ],
        compiler_params=params(),
        name="attend",
    )(q, k, v, hide)


def attend_sum_kernel(zs, q_ref, k_ref, v_ref, d_ref, p_ref, g_ref, dq_ref, dk_ref, dv_ref, h_ref, ds_s, *plane):
    step = pl.program_id(0)
    at = Place(zs)

    @pl.when(step == 0)
    def _():
        greet([at.by_core, at.by_x, at.by_y])
        PlaneSum(at, g_ref, *plane).stage1()

    @pl.when(step == 2)
    def _():
        PlaneSum(at, g_ref, *plane).stage2()

    @pl.when(step == 5)
    def _():
        PlaneSum(at, g_ref, *plane).stage3()

    attend_back_kernel(q_ref, k_ref, v_ref, d_ref, p_ref, dq_ref, dk_ref, dv_ref, ds_s)

    @pl.when(step == 5)
    def _():
        PlaneSum(at, g_ref, *plane).finish(h_ref)


def attend_back_kernel(q_ref, k_ref, v_ref, d_ref, p_ref, dq_ref, dk_ref, dv_ref, ds_s):
    vall = v_ref[...]
    kT = k_ref[...].T

    @pl.loop(0, QTILES)
    def _(n):
        at = pl.ds(pl.multiple_of(n * QT, QT), QT)
        d = d_ref[at, :]
        outs = []
        for a in range(2):
            dots = dot_nt(vall, head_lanes(a, d))
            p = p_ref[a, :, at].astype(f32)
            ds = (p * (dots - jnp.sum(dots * p, axis=0, keepdims=True))).astype(bf16)
            ds_s[a, :, at] = ds
            outs.append(dot(kT, ds))
        dq_ref[at, :] = (both_heads(*outs).T * 0.125).astype(bf16)

    dk_ref[...] = (
        dot(ds_s[0], head_lanes(0, q_ref[...])) + dot(ds_s[1], head_lanes(1, q_ref[...]))
    ).astype(bf16)
    dv_ref[...] = (
        dot(p_ref[0], head_lanes(0, d_ref[...])) + dot(p_ref[1], head_lanes(1, d_ref[...]))
    ).astype(bf16)


def attend_back(q, k, v, d, p, zs=0, g=None):
    pair = pl.BlockSpec((LENGTH, 2 * HD), lambda h: (0, h))
    out = jax.ShapeDtypeStruct((LENGTH, D), bf16)
    if zs:
        held = (zs,) + g.shape[4:]
        return pl.pallas_call(
            functools.partial(attend_sum_kernel, zs),
            grid=(H // 2,),
            in_specs=[
                pair,
                pair,
                pair,
                pair,
                pl.BlockSpec((2, LENGTH, LENGTH), lambda h: (h, 0, 0)),
                pl.BlockSpec(memory_space=pl.ANY),
            ],
            out_specs=[pair, pair, pair, pl.BlockSpec(held, lambda h: (0, 0, 0))],
            out_shape=[out, out, out, jax.ShapeDtypeStruct(held, bf16)],
            scratch_shapes=[pltpu.VMEM((2, LENGTH, LENGTH), bf16), *plane_scratch(*held)],
            compiler_params=params(collective_id=2, has_side_effects=True),
            name="attend_sum",
        )(q, k, v, d, p, g)
    return pl.pallas_call(
        attend_back_kernel,
        grid=(H // 2,),
        in_specs=[pair, pair, pair, pair, pl.BlockSpec((2, LENGTH, LENGTH), lambda h: (h, 0, 0))],
        out_specs=[pair, pair, pair],
        out_shape=[out, out, out],
        scratch_shapes=[pltpu.VMEM((2, LENGTH, LENGTH), bf16)],
        compiler_params=params(),
        name="attend_back",
    )(q, k, v, d, p)


TOK = 256
TSTEPS = LENGTH // TOK
FC = 768
TILES = REST_W // HALF


def gelu_parts(x):
    z = jnp.abs(x) * 0.7071067811865476
    t = 1.0 / (1.0 + 0.5 * z)
    poly = 0.17087277
    for c in (
        -0.82215223,
        1.48851587,
        -1.13520398,
        0.27886807,
        -0.18628806,
        0.09678418,
        0.37409196,
        1.00002368,
        -1.26551223,
    ):
        poly = poly * t + c
    tail = 0.5 * t * jnp.exp(poly - z * z)
    cdf = jnp.where(x >= 0, 1.0 - tail, tail)
    pdf = jnp.exp(-0.5 * x * x) * 0.3989422804014327
    return cdf, pdf


def norm(z, gain, shift):
    mean = jnp.mean(z, axis=1, keepdims=True)
    cen = z - mean
    var = jnp.mean(cen * cen, axis=1, keepdims=True)
    inv = lax.rsqrt(var + EPS)
    unit = cen * inv
    return unit * gain + shift, unit, inv


def norm_back(grad, unit, inv, gain):
    g = grad * gain
    return inv * (
        g - jnp.mean(g, axis=1, keepdims=True) - unit * jnp.mean(g * unit, axis=1, keepdims=True)
    )


def mid_kernel(
    ctx_ref,
    hid_ref,
    cot_ref,
    w_ref,
    vec_ref,
    out_ref,
    resid_ref,
    dctx_ref,
    dw_ref,
    vs_ref,
    act_s,
    bg_s,
    dg_s,
    flT_s,
    brT_s,
    agT_s,
):
    step = pl.program_id(0)

    def vec(off, width=HALF):
        return jnp.concatenate(
            [vec_ref[0, :, off : off + width], vec_ref[1, :, off : off + width]], axis=1
        )

    def add_vec(off, value, width=HALF):
        total = jnp.sum(value, axis=0, keepdims=True)
        vs_ref[0, :, off : off + width] += total[:, :width]
        vs_ref[1, :, off : off + width] += total[:, width:]

    @pl.when(step == 0)
    def _():
        vs_ref[...] = jnp.zeros_like(vs_ref)

    @pl.when(step < TSTEPS)
    def _():
        rows = pl.ds(pl.multiple_of(step * TOK, TOK), TOK)
        ctx = ctx_ref[rows, :]
        att = dot_nt(ctx[:, :HALF], w_ref[0, :, :HALF]) + dot_nt(
            ctx[:, HALF:], w_ref[1, :, :HALF]
        )
        z = hid_ref[...].astype(f32) + (att + vec(V_OB))
        gain1 = vec(V_G1)
        first, unit1, inv1 = norm(z, gain1, vec(V_S1))
        low = first.astype(bf16)
        flT_s[:, rows] = low.T
        branch = None
        for r in range(2):
            for c in range(0, FHALF, FC):
                at = r * FHALF + c
                before = (
                    dot(low, w_ref[r, :, HALF + c : HALF + c + FC])
                    + vec_ref[r, :, V_UB + c : V_UB + c + FC]
                )
                cdf, pdf = gelu_parts(before)
                act = (before * cdf).astype(bf16)
                act_s[rows, at : at + FC] = act
                dg_s[:, at : at + FC] = cdf + before * pdf
                part = dot_nt(act, w_ref[r, :, HALF + FHALF + c : HALF + FHALF + c + FC])
                branch = part if branch is None else branch + part
        gain2 = vec(V_G2)
        output, unit2, inv2 = norm(first + (branch + vec(V_DB)), gain2, vec(V_S2))
        out_ref[...] = output
        cot = cot_ref[...].astype(f32)
        grad2 = norm_back(cot, unit2, inv2, gain2)
        add_vec(V_G2, cot * unit2)
        add_vec(V_S2, cot)
        bgrad = grad2.astype(bf16)
        add_vec(V_DB, bgrad.astype(f32))
        brT_s[:, rows] = bgrad.T
        fgrad = grad2
        for r in range(2):
            for c in range(0, FHALF, FC):
                at = r * FHALF + c
                dact = dot(bgrad, w_ref[r, :, HALF + FHALF + c : HALF + FHALF + c + FC])
                dbef = (dact * dg_s[:, at : at + FC]).astype(bf16)
                bg_s[rows, at : at + FC] = dbef
                vs_ref[r, :, V_UB + c : V_UB + c + FC] += jnp.sum(
                    dbef.astype(f32), axis=0, keepdims=True
                )
                fgrad = fgrad + dot_nt(dbef, w_ref[r, :, HALF + c : HALF + c + FC])
        add_vec(V_G1, fgrad * unit1)
        add_vec(V_S1, fgrad)
        resid = norm_back(fgrad, unit1, inv1, gain1)
        resid_ref[...] = resid
        agrad = resid.astype(bf16)
        add_vec(V_OB, agrad.astype(f32))
        agT_s[:, rows] = agrad.T
        for r in range(2):
            dctx_ref[:, r * HALF : (r + 1) * HALF] = dot(agrad, w_ref[r, :, :HALF]).astype(bf16)

    idx = step - TSTEPS
    r = idx // TILES
    j = idx % TILES

    @pl.when((idx >= 0) & (j == 0))
    def _():
        cols = pl.ds(pl.multiple_of(r * HALF, HALF), HALF)
        dw_ref[0] = dot(agT_s[...], ctx_ref[:, cols]).astype(bf16)

    @pl.when((idx >= 0) & (j >= 1) & (j <= 4))
    def _():
        cols = pl.ds(pl.multiple_of(r * FHALF + (j - 1) * HALF, HALF), HALF)
        dw_ref[0] = dot(flT_s[...], bg_s[:, cols]).astype(bf16)

    @pl.when((idx >= 0) & (j >= 5))
    def _():
        cols = pl.ds(pl.multiple_of(r * FHALF + (j - 5) * HALF, HALF), HALF)
        dw_ref[0] = dot(brT_s[...], act_s[:, cols]).astype(bf16)


def middle(ctx, hid, cot, w, vec):
    def tok(s):
        return (jnp.minimum(s, TSTEPS - 1), 0)

    def tile(s):
        idx = jnp.maximum(s - TSTEPS, 0)
        return (idx // TILES, 0, idx % TILES)

    rows = pl.BlockSpec((TOK, D), tok)
    return pl.pallas_call(
        mid_kernel,
        grid=(TSTEPS + 2 * TILES,),
        in_specs=[
            pl.BlockSpec((LENGTH, D), lambda s: (0, 0), pipeline_mode=pl.Buffered(1)),
            rows,
            rows,
            pl.BlockSpec((2, D, REST_W), lambda s: (0, 0, 0), pipeline_mode=pl.Buffered(1)),
            pl.BlockSpec((2, 1, VEC_W), lambda s: (0, 0, 0), pipeline_mode=pl.Buffered(1)),
        ],
        out_specs=[
            rows,
            rows,
            rows,
            pl.BlockSpec((1, D, HALF), tile),
            pl.BlockSpec((2, 1, VEC_W), lambda s: (0, 0, 0)),
        ],
        out_shape=[
            jax.ShapeDtypeStruct((LENGTH, D), f32),
            jax.ShapeDtypeStruct((LENGTH, D), f32),
            jax.ShapeDtypeStruct((LENGTH, D), bf16),
            jax.ShapeDtypeStruct((2, D, REST_W), bf16),
            jax.ShapeDtypeStruct((2, 1, VEC_W), f32),
        ],
        scratch_shapes=[
            pltpu.VMEM((LENGTH, FF), bf16),
            pltpu.VMEM((LENGTH, FF), bf16),
            pltpu.VMEM((TOK, FF), f32),
            pltpu.VMEM((D, LENGTH), bf16),
            pltpu.VMEM((D, LENGTH), bf16),
            pltpu.VMEM((D, LENGTH), bf16),
        ],
        compiler_params=params(),
        name="middle",
    )(ctx, hid, cot, w, vec)


LTOK = 512
LSTEPS = LENGTH // LTOK


def last_kernel(hid_ref, dq_ref, dk_ref, dv_ref, resid_ref, w_ref, hg_ref, dw_ref, vs_ref, hT_s):
    step = pl.program_id(0)

    @pl.when(step == 0)
    def _():
        hT_s[...] = hid_ref[...].T
        for ref, off in ((dq_ref, 0), (dv_ref, HALF)):
            total = jnp.sum(ref[...].astype(f32), axis=0, keepdims=True)
            vs_ref[0, :, off : off + HALF] = total[:, :HALF]
            vs_ref[1, :, off : off + HALF] = total[:, HALF:]

    @pl.when(step < LSTEPS)
    def _():
        rows = pl.ds(pl.multiple_of(step * LTOK, LTOK), LTOK)
        acc = resid_ref[...]
        for m, ref in enumerate((dq_ref, dk_ref, dv_ref)):
            for r in range(2):
                acc = acc + dot_nt(
                    ref[rows, r * HALF : (r + 1) * HALF],
                    w_ref[r, :, m * HALF : (m + 1) * HALF],
                )
        hg_ref[...] = acc

    idx = step - LSTEPS
    cols = pl.ds(pl.multiple_of(jnp.maximum(idx, 0) // 3 * HALF, HALF), HALF)
    for m, ref in enumerate((dq_ref, dk_ref, dv_ref)):

        @pl.when((idx >= 0) & (idx % 3 == m))
        def _(ref=ref):
            dw_ref[0] = dot(hT_s[...], ref[:, cols]).astype(bf16)


def last(hid, dq, dk, dv, resid, w):
    whole = pl.BlockSpec((LENGTH, D), lambda s: (0, 0), pipeline_mode=pl.Buffered(1))
    rows = pl.BlockSpec((LTOK, D), lambda s: (jnp.minimum(s, LSTEPS - 1), 0))

    def tile(s):
        idx = jnp.maximum(s - LSTEPS, 0)
        return (idx // 3, 0, idx % 3)

    return pl.pallas_call(
        last_kernel,
        grid=(LSTEPS + 6,),
        in_specs=[
            whole,
            whole,
            whole,
            whole,
            rows,
            pl.BlockSpec((2, D, QKV_W), lambda s: (0, 0, 0), pipeline_mode=pl.Buffered(1)),
        ],
        out_specs=[
            rows,
            pl.BlockSpec((1, D, HALF), tile),
            pl.BlockSpec((2, 1, 2 * HALF), lambda s: (0, 0, 0)),
        ],
        out_shape=[
            jax.ShapeDtypeStruct((LENGTH, D), f32),
            jax.ShapeDtypeStruct((2, D, QKV_W), bf16),
            jax.ShapeDtypeStruct((2, 1, 2 * HALF), f32),
        ],
        scratch_shapes=[pltpu.VMEM((D, LENGTH), bf16)],
        compiler_params=params(),
        name="last",
    )(hid, dq, dk, dv, resid, w)


def last_sum_kernel(
    zs, hid_ref, dq_ref, dk_ref, dv_ref, resid_ref, w_ref, h_ref, v_ref,
    hg_ref, o1_ref, o2_ref, vo_ref,
    hT, g, w, resid, vs, mid, local, *scratch,
):
    plane, (v1, v2, v3, v4, va, vb, vsend, vrecv), line1, line2 = (
        scratch[:7],
        scratch[7:15],
        scratch[15:18],
        scratch[18:21],
    )
    at = Place(zs)
    loads = [
        pltpu.make_async_copy(w_ref, w, local.at[0]),
        pltpu.make_async_copy(resid_ref, resid, local.at[1]),
    ]
    start_all(loads)
    greet([at.by_core, at.by_x, at.by_y] + [at.by_z(d) for d in range(1, zs)])
    first = PlaneSum(at, g, None, *plane, None)
    second = LineSum(at, h_ref, *line2)
    second.start()

    hT[...] = hid_ref[...].T
    half = zs // 2

    @pl.loop(0, 2)
    def _(n):
        rows = hT[pl.ds(pl.multiple_of(n * HALF, HALF), HALF), :]
        for r in range(2):
            for m, ref in enumerate((dq_ref, dk_ref, dv_ref)):
                tile = dot(rows, ref[:, r * HALF : (r + 1) * HALF]).astype(bf16)
                g[r, pl.ds(n * half, half), :, :, :, m * HALF : (m + 1) * HALF] = tile.reshape(
                    (half,) + g.shape[2:5] + (HALF,)
                )

    first.stage1()
    vs[...] = v_ref[...]
    for ref, off in ((dq_ref, V_QB), (dv_ref, V_VB)):
        total = jnp.sum(ref[...].astype(f32), axis=0, keepdims=True)
        vs[0, :, off : off + HALF] = total[:, :HALF]
        vs[1, :, off : off + HALF] = total[:, HALF:]
    vec1 = remote(vs, v1, vsend, vrecv, 0, at.by_core)
    vec1.start()
    wait_all(loads)

    def input_grad(n):
        rows = pl.ds(pl.multiple_of(n * QROWS, QROWS), QROWS)
        acc = resid[rows, :]
        for m, ref in enumerate((dq_ref, dk_ref, dv_ref)):
            for r in range(2):
                acc = acc + dot_nt(
                    ref[rows, r * HALF : (r + 1) * HALF], w[r, :, m * HALF : (m + 1) * HALF]
                )
        hg_ref[rows, :] = acc

    tiles = LENGTH // QROWS
    pl.loop(0, tiles // 2)(input_grad)
    vec1.wait()
    va[...] = vs[...] + v1[...]
    vec2 = remote(va, v2, vsend, vrecv, 1, at.by_x)
    vec2.start()
    first.stage2()
    pl.loop(tiles // 2, tiles)(input_grad)
    vec2.wait()
    vb[...] = va[...] + v2[...]
    vec3 = remote(vb.at[1 - at.y], v3, vsend, vrecv, 2, at.by_y)
    vec3.start()
    first.stage3()
    vec3.wait()
    v4[0] = vb[at.y] + v3[...]
    vec4 = [
        remote(v4.at[0], v4.at[d], vsend, vrecv, 2 + d, at.by_z(d)) for d in range(1, zs)
    ]
    start_all(vec4)
    second.finish(o2_ref)
    first.finish(mid)
    third = LineSum(at, mid, *line1)
    third.start()
    wait_all(vec4)
    total = v4[at.z % zs]
    for z in range(1, zs):
        total = total + v4[(at.z + zs - z) % zs]
    vo_ref[...] = total
    third.finish(o1_ref)


def last_sum(zs, hid, dq, dk, dv, resid, w, h, v):
    rows = D // (4 * zs)
    w1 = w.shape[2]
    w2 = h.shape[2]
    width = v.shape[2]
    vmem = pl.BlockSpec(memory_space=pltpu.VMEM)
    far = pl.BlockSpec(memory_space=pl.ANY)
    return pl.pallas_call(
        functools.partial(last_sum_kernel, zs),
        in_specs=[vmem, vmem, vmem, vmem, far, far, vmem, vmem],
        out_specs=[vmem] * 4,
        out_shape=[
            jax.ShapeDtypeStruct((LENGTH, D), f32),
            jax.ShapeDtypeStruct((rows, w1), f32),
            jax.ShapeDtypeStruct((rows, w2), f32),
            jax.ShapeDtypeStruct((1, width), f32),
        ],
        scratch_shapes=[
            pltpu.VMEM((D, LENGTH), bf16),
            pltpu.VMEM((2, zs, 2, 2, rows, w1), bf16),
            pltpu.VMEM(w.shape, bf16),
            pltpu.VMEM((LENGTH, D), f32),
            pltpu.VMEM((2, 1, width), f32),
            pltpu.VMEM((zs, rows, w1), bf16),
            pltpu.SemaphoreType.DMA((2,)),
            *plane_scratch(zs, rows, w1)[1:-1],
            pltpu.VMEM((2, 1, width), f32),
            pltpu.VMEM((2, 1, width), f32),
            pltpu.VMEM((1, width), f32),
            pltpu.VMEM((zs, 1, width), f32),
            pltpu.VMEM((2, 1, width), f32),
            pltpu.VMEM((2, 1, width), f32),
            pltpu.SemaphoreType.DMA((zs + 2,)),
            pltpu.SemaphoreType.DMA((zs + 2,)),
            *line_scratch(zs, rows, w1),
            *line_scratch(zs, rows, w2),
        ],
        compiler_params=params(collective_id=1, has_side_effects=True),
        name="last_sum",
    )(hid, dq, dk, dv, resid, w, h, v)


def gather_parts(parts, rows_n, cols_n):
    packed = jnp.concatenate(parts, axis=1)
    every = lax.all_gather(packed, ("row", "col"), axis=0, tiled=True)
    every = every.reshape(rows_n, D, packed.shape[1])
    if rows_n == 2:
        return every
    pieces, at = [], 0
    for part in parts:
        width = part.shape[1]
        one = every[:, :, at : at + width].reshape(2, rows_n // 2, D, width)
        pieces.append(one.transpose(0, 2, 1, 3).reshape(2, D, rows_n // 2 * width))
        at += width
    return jnp.concatenate(pieces, axis=2)


def scatter_parts(full, halves, rows_n, cols_n):
    widths = [h * 2 // rows_n for h in halves]
    if rows_n != 2:
        pieces, at = [], 0
        for half, width in zip(halves, widths):
            one = full[:, :, at : at + half].reshape(2, D, rows_n // 2, width)
            pieces.append(one.transpose(0, 2, 1, 3).reshape(rows_n, D, width))
            at += half
        full = jnp.concatenate(pieces, axis=2)
    flat = full.reshape(rows_n * D, sum(widths))
    mine = lax.psum_scatter(flat, ("row", "col"), scatter_dimension=0, tiled=True)
    mine = mine.astype(f32)
    out, at = [], 0
    for width in widths:
        out.append(mine[:, at : at + width])
        at += width
    return out


VEC_HALVES = (HALF, HALF, HALF, FHALF, HALF, HALF, HALF, HALF, HALF)


def on_device(
    rows_n,
    cols_n,
    hidden,
    cotangent,
    rand_blocks,
    w_query,
    w_key,
    w_value,
    w_out,
    w_up,
    w_down,
    *vectors,
):
    zs = cols_n // 4
    staged = rows_n == 2 and cols_n % 8 == 0
    hide = hidden_pairs(rand_blocks[0])
    if staged:
        weights = (w_query, w_key, w_value, w_out, w_up, w_down)
        q, k, v, w1, h2, vec = front(zs, hidden, weights, vectors)
        ctx, p, w2 = attend(q, k, v, hide, zs, h2)
        w1, w2 = w1.reshape(2, D, QKV_W), w2.reshape(2, D, REST_W)
    else:
        vec = lax.all_gather(jnp.concatenate(vectors).astype(f32), "row", axis=0, tiled=False)
        if rows_n != 2:
            pieces, at = [], 0
            for half in VEC_HALVES:
                width = half * 2 // rows_n
                pieces.append(vec[:, at : at + width].reshape(2, half))
                at += width
            vec = jnp.concatenate(pieces, axis=1)
        vec = vec.reshape(2, 1, VEC_W)
        w1 = gather_parts([w_query, w_key, w_value], rows_n, cols_n)
        w2 = gather_parts([w_out.T, w_up, w_down.T], rows_n, cols_n)
        q, k, v = qkv(hidden, w1, vec)
        ctx, p = attend(q, k, v, hide)
    output, resid, dctx, dw2, vs2 = middle(ctx, hidden, cotangent, w2, vec)
    if staged:
        g2 = dw2.reshape(2, zs, 2, 2, D // cols_n, REST_W)
        dq, dk, dv, h2 = attend_back(q, k, v, dctx, p, zs, g2)
        hgrad, m1, m2, vs = last_sum(zs, hidden, dq, dk, dv, resid, w1, h2, vs2)
        g_q, g_k, g_v = (m1[:, n * HALF : (n + 1) * HALF] for n in range(3))
        g_out = m2[:, :HALF].T
        g_up = m2[:, HALF : HALF + FHALF]
        g_down = m2[:, HALF + FHALF :].T
        sums, at = [], 0
        for width in VEC_HALVES:
            sums.append(vs[0, at : at + width])
            at += width
        return (output, hgrad, g_q, g_k, g_v, g_out, g_up, g_down, *sums)
    dq, dk, dv = attend_back(q, k, v, dctx, p)
    hgrad, dw1, vs1 = last(hidden, dq, dk, dv, resid, w1)
    vs = jnp.concatenate([vs1, vs2[:, :, 2 * HALF :]], axis=2)
    g_out, g_up, g_down = scatter_parts(dw2, (HALF, FHALF, FHALF), rows_n, cols_n)
    g_q, g_k, g_v = scatter_parts(dw1, (HALF, HALF, HALF), rows_n, cols_n)
    vs = lax.psum(vs.reshape(2, VEC_W), ("col", "row"))
    row = lax.axis_index("row")
    sums, at = [], 0
    for half in VEC_HALVES:
        width = half * 2 // rows_n
        both = vs[:, at : at + half].reshape(rows_n, width)
        sums.append(lax.dynamic_index_in_dim(both, row, 0, keepdims=False))
        at += half
    return (output, hgrad, g_q, g_k, g_v, g_out.T, g_up, g_down.T, *sums)


def solution(mesh):
    rows_n, cols_n = mesh.shape["row"], mesh.shape["col"]
    tokens = P(("col", "row"), None)
    placed = (
        tokens,
        tokens,
        P(("col", "row"), None, None, None),
        P("col", "row"),
        P("col", "row"),
        P("col", "row"),
        P("row", "col"),
        P("col", "row"),
        P("row", "col"),
    ) + (P("row"),) * 9
    return jax.shard_map(
        functools.partial(on_device, rows_n, cols_n),
        mesh=mesh,
        in_specs=placed,
        out_specs=(
            tokens,
            tokens,
            P("col", "row"),
            P("col", "row"),
            P("col", "row"),
            P("row", "col"),
            P("col", "row"),
            P("row", "col"),
        )
        + (P("row"),) * 9,
        check_vma=False,
    )
```

```python
import functools

import jax
import jax.numpy as jnp
from jax import lax
from jax.experimental import pallas as pl
from jax.experimental.pallas import tpu as pltpu
from jax.sharding import PartitionSpec as P

D = 768
H = 12
FF = 3072
BLK = 64
LENGTH = 1024
BLOCKS = LENGTH // BLK
HD = D // H
RAND = 3
EPS = 1e-12
NEG = -1e30
VMEM_BYTES = 64 * 1000 * 1000

HALF = D // 2
FHALF = FF // 2
QKV_W = 3 * HALF
REST_W = HALF + 2 * FHALF
VEC_W = 8 * HALF + FHALF
V_QB, V_VB, V_OB, V_UB = 0, HALF, 2 * HALF, 3 * HALF
V_DB = V_UB + FHALF
V_G1, V_S1, V_G2, V_S2 = V_DB + HALF, V_DB + 2 * HALF, V_DB + 3 * HALF, V_DB + 4 * HALF

f32 = jnp.float32
bf16 = jnp.bfloat16


def dot(a, b):
    return jnp.dot(a, b, preferred_element_type=f32)


def dot_nt(a, b):
    return lax.dot_general(a, b, (((1,), (1,)), ((), ())), preferred_element_type=f32)


def dot_tn(a, b):
    return lax.dot_general(a, b, (((0,), (0,)), ((), ())), preferred_element_type=f32)


def params(**kw):
    return pltpu.CompilerParams(vmem_limit_bytes=VMEM_BYTES, **kw)


def qkv_kernel(x_ref, w_ref, vec_ref, q_ref, k_ref, v_ref):
    r = pl.program_id(0)
    j = pl.program_id(1)
    acc = dot(x_ref[...], w_ref[0])
    vec = vec_ref[0]

    @pl.when(j == 0)
    def _():
        q_ref[...] = ((acc + vec[:, V_QB : V_QB + HALF]).astype(bf16).astype(f32) * 0.125).astype(bf16)

    @pl.when(j == 1)
    def _():
        k_ref[...] = acc.astype(bf16)

    @pl.when(j == 2)
    def _():
        v_ref[...] = (acc + vec[:, V_VB : V_VB + HALF]).astype(bf16)


def qkv(x, w, vec):
    out = jax.ShapeDtypeStruct((LENGTH, D), bf16)
    col = pl.BlockSpec((LENGTH, HALF), lambda r, j: (0, r))
    return pl.pallas_call(
        qkv_kernel,
        grid=(2, 3),
        in_specs=[
            pl.BlockSpec((LENGTH, D), lambda r, j: (0, 0)),
            pl.BlockSpec((1, D, HALF), lambda r, j: (r, 0, j)),
            pl.BlockSpec((1, 1, VEC_W), lambda r, j: (r, 0, 0)),
        ],
        out_specs=[col, col, col],
        out_shape=[out, out, out],
        compiler_params=params(),
        name="qkv",
    )(x, w, vec)


MESH = pl.DeviceIdType.MESH


class Place:
    def __init__(self, zs):
        c = lax.axis_index("col")
        y = lax.axis_index("row")
        self.zs = zs
        self.core, self.x, self.y, self.z = c % 2, c // 2 % 2, y, c // 4
        self.by_core = {"col": c + 1 - 2 * self.core, "row": y}
        self.by_x = {"col": c + 2 - 4 * self.x, "row": y}
        self.by_y = {"col": c, "row": 1 - y}
        self.within = c % 4

    def ahead(self, d):
        return (self.z + d) % self.zs

    def by_z(self, d):
        return {"col": self.ahead(d) * 4 + self.within, "row": self.y}


def greet(partners):
    barrier = pltpu.get_barrier_semaphore()
    for to in partners:
        pl.semaphore_signal(barrier, inc=1, device_id=to, device_id_type=MESH)
    pl.semaphore_wait(barrier, len(partners))


def remote(src, dst, send, recv, i, to):
    return pltpu.make_async_remote_copy(
        src_ref=src,
        dst_ref=dst,
        send_sem=send.at[i],
        recv_sem=recv.at[i],
        device_id=to,
        device_id_type=MESH,
    )


def add_low(a, b):
    return (a.astype(f32) + b.astype(f32)).astype(bf16)


def chunks_of(zs):
    return 2 if zs % 4 == 0 else 1


def plane_scratch(zs, rows, width):
    half = zs // 2
    return [
        pltpu.VMEM((2, zs, 2, rows, width), bf16),
        pltpu.VMEM((2, zs, 2, rows, width), bf16),
        pltpu.VMEM((2, half, rows, width), bf16),
        pltpu.VMEM((half, 2, rows, width), bf16),
        pltpu.VMEM((half, rows, width), bf16),
        pltpu.VMEM((half, rows, width), bf16),
        pltpu.SemaphoreType.DMA((6 * chunks_of(zs),)),
        pltpu.SemaphoreType.DMA((6 * chunks_of(zs),)),
        pltpu.SemaphoreType.DMA,
    ]


class PlaneSum:
    def __init__(self, at, g, own, b1, b2x, b2y, b3y, b3x, send, recv, local):
        self.at, self.half, self.chunks = at, at.zs // 2, chunks_of(at.zs)
        self.own, self.b1, self.b2x, self.b2y, self.b3y, self.b3x = own, b1, b2x, b2y, b3y, b3x
        self.g, self.send, self.recv, self.local = g, send, recv, local
        self.size = self.half // self.chunks

    def spans(self, i):
        lo = i * self.size
        return slice(lo, lo + self.size), slice(self.half + lo, self.half + lo + self.size)

    def keep(self):
        return pltpu.make_async_copy(self.g.at[:, :, :, self.at.core], self.own, self.local)

    def first(self, i):
        at = self.at
        return [
            remote(
                self.g.at[:, span, :, 1 - at.core], self.b1.at[:, span],
                self.send, self.recv, 6 * i + n, at.by_core,
            )
            for n, span in enumerate(self.spans(i))
        ]

    def second(self, i):
        at, sems = self.at, (self.send, self.recv)
        low, high = self.spans(i)
        return (
            remote(self.b1.at[:, low, 1 - at.x], self.b2x.at[:, low], *sems, 6 * i + 2, at.by_x),
            remote(self.b1.at[1 - at.y, high], self.b2y.at[low], *sems, 6 * i + 3, at.by_y),
        )

    def third(self, i):
        at, sems = self.at, (self.send, self.recv)
        low, _ = self.spans(i)
        return (
            remote(self.b2x.at[1 - at.y, low], self.b3y.at[low], *sems, 6 * i + 4, at.by_y),
            remote(self.b2y.at[low, 1 - at.x], self.b3x.at[low], *sems, 6 * i + 5, at.by_x),
        )

    def stage1(self):
        if self.own is not None:
            self.keep().start()
        for i in range(self.chunks):
            start_all(self.first(i))

    def stage2(self, i):
        if self.own is not None and i == 0:
            self.keep().wait()
        wait_all(self.first(i))
        b1, own, core = self.b1, self.own, self.at.core

        @pl.loop(i * self.size, (i + 1) * self.size)
        def _(n):
            for z in (n, self.half + n):
                for y in range(2):
                    for x in range(2):
                        mine = self.g[y, z, x, core] if own is None else own[y, z, x]
                        b1[y, z, x] = add_low(b1[y, z, x], mine)

        start_all(self.second(i))

    def stage3(self, i):
        wait_all(self.second(i))
        b1, b2x, b2y, half = self.b1, self.b2x, self.b2y, self.half

        @pl.loop(i * self.size, (i + 1) * self.size)
        def _(z):
            for n in range(2):
                b2x[n, z] = add_low(b2x[n, z], b1[n, z, self.at.x])
                b2y[z, n] = add_low(b2y[z, n], b1[self.at.y, half + z, n])

        start_all(self.third(i))

    def finish(self, i, out):
        wait_all(self.third(i))
        half = self.half

        @pl.loop(i * self.size, (i + 1) * self.size)
        def _(z):
            out[z] = add_low(self.b3y[z], self.b2x[self.at.y, z])
            out[half + z] = add_low(self.b3x[z], self.b2y[z, self.at.x])


def line_scratch(zs, rows, width):
    return [
        pltpu.VMEM((zs - 1, rows, width), bf16),
        pltpu.SemaphoreType.DMA((zs - 1,)),
        pltpu.SemaphoreType.DMA((zs - 1,)),
    ]


class LineSum:
    def __init__(self, at, h, held, send, recv):
        self.at, self.h, self.held = at, h, held
        self.copies = [
            remote(h.at[at.ahead(d)], held.at[d - 1], send, recv, d - 1, at.by_z(d))
            for d in range(1, at.zs)
        ]

    def start(self):
        for copy in self.copies:
            copy.start()

    def finish(self, out):
        for copy in self.copies:
            copy.wait()
        total = self.h[self.at.z].astype(f32)
        for d in range(1, self.at.zs):
            total = total + self.held[d - 1].astype(f32)
        out[...] = total


class PlaneGather:
    def __init__(self, at, h, g, send, recv, cols=slice(None), sem=0):
        self.at, self.h, self.g, self.send, self.recv = at, h, g, send, recv
        self.cols, self.h_cols, self.sem = cols, cols, sem

    def move(self, i, to, src, *where):
        dst = self.g.at[where + (slice(None), self.cols)]
        src = dst if src is None else self.h.at[src, :, self.h_cols]
        return remote(src, dst, self.send, self.recv, self.sem + i, to)

    def stage1(self):
        at, half = self.at, self.at.zs // 2
        y, x, core = at.y, at.x, at.core
        every, low, high = slice(None), slice(0, half), slice(half, at.zs)
        return (
            self.move(0, at.by_y, low, y, low, x, core),
            self.move(1, at.by_x, high, y, high, x, core),
            self.move(2, at.by_core, every, y, every, x, core),
        )

    def stage2(self):
        at, half = self.at, self.at.zs // 2
        y, x, core = at.y, at.x, at.core
        every, low, high = slice(None), slice(0, half), slice(half, at.zs)
        return (
            self.move(3, at.by_x, None, every, low, x, core),
            self.move(4, at.by_y, None, y, high, every, core),
            self.move(5, at.by_core, None, 1 - y, low, x, core),
            self.move(6, at.by_core, None, y, high, 1 - x, core),
        )

    def stage3(self):
        at, half = self.at, self.at.zs // 2
        y, x, core = at.y, at.x, at.core
        every, low, high = slice(None), slice(0, half), slice(half, at.zs)
        return (
            self.move(7, at.by_core, None, every, low, 1 - x, core),
            self.move(8, at.by_core, None, 1 - y, high, every, core),
        )


def start_all(copies):
    for copy in copies:
        copy.start()


def wait_all(copies):
    for copy in copies:
        copy.wait()


def front_kernel(
    zs, x_ref, wq_ref, wk_ref, wv_ref, wo_ref, wu_ref, wd_ref, *refs,
):
    vector_refs, refs = refs[:9], refs[9:]
    q_ref, k_ref, v_ref, g_ref, h_ref, vo_ref, line, s2, vec_s = refs[:9]
    psend, precv, lsend, lrecv, vsend, vrecv, local = refs[9:]
    at = Place(zs)
    mine = [
        pltpu.make_async_copy(ref, line.at[at.z, :, n * HALF : (n + 1) * HALF], local.at[n])
        for n, ref in enumerate((wq_ref, wk_ref, wv_ref))
    ]
    start_all(mine)
    greet([at.by_core, at.by_x, at.by_y] + [at.by_z(d) for d in range(1, zs)])
    wait_all(mine)
    along = [
        remote(line.at[at.z], line.at[at.z], lsend, lrecv, d - 1, at.by_z(d))
        for d in range(1, zs)
    ]
    start_all(along)
    off = 0
    for ref in vector_refs:
        width = ref.shape[0]
        vec_s[:, off : off + width] = ref[...].astype(f32).reshape(1, width)
        off += width
    s2[:, :HALF] = wo_ref[...]
    s2[:, HALF : HALF + FHALF] = wu_ref[...]
    s2[:, HALF + FHALF :] = wd_ref[...]
    vo_ref[at.y] = vec_s[...]
    h_ref[at.z] = s2[...]
    vec = remote(vec_s, vo_ref.at[at.y], vsend, vrecv, 0, at.by_y)
    vec.start()
    wait_all(along)
    after = [
        remote(
            s2.at[:, :EARLY], h_ref.at[at.z, :, :EARLY], lsend, lrecv, zs - 2 + d, at.by_z(d)
        )
        for d in range(1, zs)
    ]
    start_all(after)
    gather = PlaneGather(at, line, g_ref, psend, precv)
    keep = pltpu.make_async_copy(line, g_ref.at[at.y, :, at.x, at.core], local.at[3])
    keep.start()
    one = gather.stage1()
    start_all(one)
    keep.wait()
    wait_all(one)
    two = gather.stage2()
    start_all(two)
    wait_all(two)
    three = gather.stage3()
    start_all(three)
    vec.wait()
    wait_all(three)

    @pl.loop(0, LENGTH // QROWS)
    def _(n):
        rows = pl.ds(pl.multiple_of(n * QROWS, QROWS), QROWS)
        x = x_ref[rows, :]
        for r in range(2):
            w = g_ref[r].reshape(D, QKV_W)
            out = slice(r * HALF, (r + 1) * HALF)
            q = dot(x, w[:, :HALF]) + vo_ref[r, :, V_QB : V_QB + HALF]
            q_ref[rows, out] = (q.astype(bf16).astype(f32) * 0.125).astype(bf16)
            k_ref[rows, out] = dot(x, w[:, HALF : 2 * HALF]).astype(bf16)
            v = dot(x, w[:, 2 * HALF :]) + vo_ref[r, :, V_VB : V_VB + HALF]
            v_ref[rows, out] = v.astype(bf16)

    wait_all(after)


QROWS = 256
EARLY = HALF + FHALF


def front(zs, x, weights, vectors):
    rows = weights[0].shape[0]
    w1, w2 = QKV_W, REST_W
    vmem = pl.BlockSpec(memory_space=pltpu.VMEM)
    out = jax.ShapeDtypeStruct((LENGTH, D), bf16)
    return pl.pallas_call(
        functools.partial(front_kernel, zs),
        in_specs=[vmem] * 16,
        out_specs=[vmem] * 6,
        out_shape=[
            out,
            out,
            out,
            jax.ShapeDtypeStruct((2, zs, 2, 2, rows, w1), bf16),
            jax.ShapeDtypeStruct((zs, rows, w2), bf16),
            jax.ShapeDtypeStruct((2, 1, VEC_W), f32),
        ],
        scratch_shapes=[
            pltpu.VMEM((zs, rows, w1), bf16),
            pltpu.VMEM((rows, w2), bf16),
            pltpu.VMEM((1, VEC_W), f32),
            pltpu.SemaphoreType.DMA((9,)),
            pltpu.SemaphoreType.DMA((9,)),
            pltpu.SemaphoreType.DMA((2 * zs - 2,)),
            pltpu.SemaphoreType.DMA((2 * zs - 2,)),
            pltpu.SemaphoreType.DMA((1,)),
            pltpu.SemaphoreType.DMA((1,)),
            pltpu.SemaphoreType.DMA((4,)),
        ],
        compiler_params=params(collective_id=3, has_side_effects=True),
        name="front",
    )(x, *weights, *vectors)


QT = 256
QTILES = LENGTH // QT


def head_lanes(a, x):
    lane = lax.broadcasted_iota(jnp.int32, x.shape, 1)
    return jnp.where((lane < HD) if a == 0 else (lane >= HD), x, jnp.zeros_like(x))


def both_heads(top, low):
    row = lax.broadcasted_iota(jnp.int32, top.shape, 0)
    return jnp.where(row < HD, top, low)


def hidden_pairs(rand):
    rows = jnp.arange(BLOCKS)[:, None]
    cols = jnp.arange(BLOCKS)[None, :]
    edge = (rows == 0) | (rows == BLOCKS - 1) | (cols == 0) | (cols == BLOCKS - 1)
    near = jnp.abs(rows - cols) <= 1
    chosen = (rand[:, :, :, None] == jnp.arange(BLOCKS)).any(axis=2)
    chosen = jnp.pad(chosen.transpose(1, 2, 0), ((0, 0), (0, 0), (1, 1)))
    table = jnp.where(chosen | (edge | near)[None], 0.0, NEG).astype(f32)
    return jnp.repeat(table, BLK, axis=2)


def attend_kernel(q_ref, k_ref, v_ref, hide_ref, c_ref, p_ref):
    kall = k_ref[...]
    vT = v_ref[...].T

    @pl.loop(0, QTILES)
    def _(n):
        at = pl.ds(pl.multiple_of(n * QT, QT), QT)
        q = q_ref[at, :]
        outs = []
        for a in range(2):
            s = dot_nt(kall, head_lanes(a, q)).reshape(BLOCKS, BLK, QT)
            s = (s + hide_ref[a, :, at][:, None, :]).reshape(LENGTH, QT)
            e = jnp.exp(s - jnp.max(s, axis=0, keepdims=True))
            p = (e * (1.0 / jnp.sum(e, axis=0, keepdims=True))).astype(bf16)
            p_ref[a, :, at] = p
            outs.append(dot(vT, p))
        c_ref[at, :] = both_heads(*outs).T.astype(bf16)


def attend_gather_kernel(
    zs, q_ref, k_ref, v_ref, hide_ref, h_ref, c_ref, p_ref, g_ref, rest, send, recv, lsend, lrecv, local
):
    step = pl.program_id(0)
    at = Place(zs)
    early = PlaneGather(at, h_ref, g_ref, send, recv, slice(0, EARLY))
    late = PlaneGather(at, rest, g_ref, send, recv, slice(EARLY, REST_W), 9)
    late.h_cols = slice(None)

    def keep(part):
        cols = part.cols
        src = part.h.at[:, :, part.h_cols]
        return pltpu.make_async_copy(
            src, g_ref.at[at.y, :, at.x, at.core, :, cols], local.at[0 if part is early else 1]
        )

    def fetch():
        return pltpu.make_async_copy(h_ref.at[at.z, :, EARLY:], rest.at[at.z], local.at[2])

    def along():
        return [
            remote(h_ref.at[at.z, :, EARLY:], rest.at[at.z], lsend, lrecv, d - 1, at.by_z(d))
            for d in range(1, zs)
        ]

    @pl.when(step == 0)
    def _():
        greet([at.by_core, at.by_x, at.by_y] + [at.by_z(d) for d in range(1, zs)])
        start_all(early.stage1())
        start_all(along())
        keep(early).start()
        fetch().start()

    @pl.when(step == 1)
    def _():
        keep(early).wait()
        wait_all(early.stage1())
        start_all(early.stage2())

    @pl.when(step == 2)
    def _():
        fetch().wait()
        wait_all(along())
        keep(late).start()
        start_all(late.stage1())

    @pl.when(step == 4)
    def _():
        keep(late).wait()
        wait_all(late.stage1())
        start_all(late.stage2())
        wait_all(early.stage2())
        start_all(early.stage3())

    attend_kernel(q_ref, k_ref, v_ref, hide_ref, c_ref, p_ref)

    @pl.when(step == H // 2 - 1)
    def _():
        wait_all(early.stage3())
        wait_all(late.stage2())
        start_all(late.stage3())
        wait_all(late.stage3())


def attend(q, k, v, hide, zs=0, h2=None):
    pair = pl.BlockSpec((LENGTH, 2 * HD), lambda h: (0, h))
    if zs:
        return pl.pallas_call(
            functools.partial(attend_gather_kernel, zs),
            grid=(H // 2,),
            in_specs=[
                pair,
                pair,
                pair,
                pl.BlockSpec((2, BLOCKS, LENGTH), lambda h: (h, 0, 0)),
                pl.BlockSpec(memory_space=pltpu.VMEM),
            ],
            out_specs=[
                pair,
                pl.BlockSpec((2, LENGTH, LENGTH), lambda h: (h, 0, 0)),
                pl.BlockSpec(memory_space=pl.ANY),
            ],
            out_shape=[
                jax.ShapeDtypeStruct((LENGTH, D), bf16),
                jax.ShapeDtypeStruct((H, LENGTH, LENGTH), bf16),
                jax.ShapeDtypeStruct((2, zs, 2, 2) + h2.shape[1:], bf16),
            ],
            scratch_shapes=[
                pltpu.VMEM(h2.shape[:2] + (REST_W - EARLY,), bf16),
                pltpu.SemaphoreType.DMA((18,)),
                pltpu.SemaphoreType.DMA((18,)),
                pltpu.SemaphoreType.DMA((zs - 1,)),
                pltpu.SemaphoreType.DMA((zs - 1,)),
                pltpu.SemaphoreType.DMA((3,)),
            ],
            compiler_params=params(collective_id=4, has_side_effects=True),
            name="attend_gather",
        )(q, k, v, hide, h2)
    return pl.pallas_call(
        attend_kernel,
        grid=(H // 2,),
        in_specs=[pair, pair, pair, pl.BlockSpec((2, BLOCKS, LENGTH), lambda h: (h, 0, 0))],
        out_specs=[pair, pl.BlockSpec((2, LENGTH, LENGTH), lambda h: (h, 0, 0))],
        out_shape=[
            jax.ShapeDtypeStruct((LENGTH, D), bf16),
            jax.ShapeDtypeStruct((H, LENGTH, LENGTH), bf16),
        ],
        compiler_params=params(),
        name="attend",
    )(q, k, v, hide)


def attend_sum_kernel(zs, q_ref, k_ref, v_ref, d_ref, p_ref, g_ref, dq_ref, dk_ref, dv_ref, h_ref, ds_s, *plane):
    step = pl.program_id(0)
    at = Place(zs)

    @pl.when(step == 0)
    def _():
        greet([at.by_core, at.by_x, at.by_y])
        PlaneSum(at, g_ref, *plane).stage1()

    for i in range(chunks_of(zs)):

        @pl.when(step == 1 + i)
        def _(i=i):
            PlaneSum(at, g_ref, *plane).stage2(i)

        @pl.when(step == 3 + 2 * i)
        def _(i=i):
            PlaneSum(at, g_ref, *plane).stage3(i)

    attend_back_kernel(q_ref, k_ref, v_ref, d_ref, p_ref, dq_ref, dk_ref, dv_ref, ds_s)

    @pl.when(step == H // 2 - 1)
    def _():
        for i in range(chunks_of(zs)):
            PlaneSum(at, g_ref, *plane).finish(i, h_ref)


def attend_back_kernel(q_ref, k_ref, v_ref, d_ref, p_ref, dq_ref, dk_ref, dv_ref, ds_s):
    vall = v_ref[...]
    kT = k_ref[...].T

    @pl.loop(0, QTILES)
    def _(n):
        at = pl.ds(pl.multiple_of(n * QT, QT), QT)
        d = d_ref[at, :]
        outs = []
        for a in range(2):
            dots = dot_nt(vall, head_lanes(a, d))
            p = p_ref[a, :, at].astype(f32)
            ds = (p * (dots - jnp.sum(dots * p, axis=0, keepdims=True))).astype(bf16)
            ds_s[a, :, at] = ds
            outs.append(dot(kT, ds))
        dq_ref[at, :] = (both_heads(*outs).T * 0.125).astype(bf16)

    dk_ref[...] = (
        dot(ds_s[0], head_lanes(0, q_ref[...])) + dot(ds_s[1], head_lanes(1, q_ref[...]))
    ).astype(bf16)
    dv_ref[...] = (
        dot(p_ref[0], head_lanes(0, d_ref[...])) + dot(p_ref[1], head_lanes(1, d_ref[...]))
    ).astype(bf16)


def attend_back(q, k, v, d, p, zs=0, g=None):
    pair = pl.BlockSpec((LENGTH, 2 * HD), lambda h: (0, h))
    out = jax.ShapeDtypeStruct((LENGTH, D), bf16)
    if zs:
        held = (zs,) + g.shape[4:]
        return pl.pallas_call(
            functools.partial(attend_sum_kernel, zs),
            grid=(H // 2,),
            in_specs=[
                pair,
                pair,
                pair,
                pair,
                pl.BlockSpec((2, LENGTH, LENGTH), lambda h: (h, 0, 0)),
                pl.BlockSpec(memory_space=pl.ANY),
            ],
            out_specs=[pair, pair, pair, pl.BlockSpec(held, lambda h: (0, 0, 0))],
            out_shape=[out, out, out, jax.ShapeDtypeStruct(held, bf16)],
            scratch_shapes=[pltpu.VMEM((2, LENGTH, LENGTH), bf16), *plane_scratch(*held)],
            compiler_params=params(collective_id=2, has_side_effects=True),
            name="attend_sum",
        )(q, k, v, d, p, g)
    return pl.pallas_call(
        attend_back_kernel,
        grid=(H // 2,),
        in_specs=[pair, pair, pair, pair, pl.BlockSpec((2, LENGTH, LENGTH), lambda h: (h, 0, 0))],
        out_specs=[pair, pair, pair],
        out_shape=[out, out, out],
        scratch_shapes=[pltpu.VMEM((2, LENGTH, LENGTH), bf16)],
        compiler_params=params(),
        name="attend_back",
    )(q, k, v, d, p)


TOK = 256
TSTEPS = LENGTH // TOK
FC = 768
TILES = REST_W // HALF


def gelu_parts(x):
    z = jnp.abs(x) * 0.7071067811865476
    t = 1.0 / (1.0 + 0.5 * z)
    poly = 0.17087277
    for c in (
        -0.82215223,
        1.48851587,
        -1.13520398,
        0.27886807,
        -0.18628806,
        0.09678418,
        0.37409196,
        1.00002368,
        -1.26551223,
    ):
        poly = poly * t + c
    tail = 0.5 * t * jnp.exp(poly - z * z)
    cdf = jnp.where(x >= 0, 1.0 - tail, tail)
    pdf = jnp.exp(-0.5 * x * x) * 0.3989422804014327
    return cdf, pdf


def norm(z, gain, shift):
    mean = jnp.mean(z, axis=1, keepdims=True)
    cen = z - mean
    var = jnp.mean(cen * cen, axis=1, keepdims=True)
    inv = lax.rsqrt(var + EPS)
    unit = cen * inv
    return unit * gain + shift, unit, inv


def norm_back(grad, unit, inv, gain):
    g = grad * gain
    return inv * (
        g - jnp.mean(g, axis=1, keepdims=True) - unit * jnp.mean(g * unit, axis=1, keepdims=True)
    )


def mid_kernel(
    ctx_ref,
    hid_ref,
    cot_ref,
    w_ref,
    vec_ref,
    out_ref,
    resid_ref,
    dctx_ref,
    dw_ref,
    vs_ref,
    act_s,
    bg_s,
    dg_s,
    flT_s,
    brT_s,
    agT_s,
):
    step = pl.program_id(0)

    def vec(off, width=HALF):
        return jnp.concatenate(
            [vec_ref[0, :, off : off + width], vec_ref[1, :, off : off + width]], axis=1
        )

    def add_vec(off, value, width=HALF):
        total = jnp.sum(value, axis=0, keepdims=True)
        vs_ref[0, :, off : off + width] += total[:, :width]
        vs_ref[1, :, off : off + width] += total[:, width:]

    @pl.when(step == 0)
    def _():
        vs_ref[...] = jnp.zeros_like(vs_ref)

    @pl.when(step < TSTEPS)
    def _():
        rows = pl.ds(pl.multiple_of(step * TOK, TOK), TOK)
        ctx = ctx_ref[rows, :]
        att = dot_nt(ctx[:, :HALF], w_ref[0, :, :HALF]) + dot_nt(
            ctx[:, HALF:], w_ref[1, :, :HALF]
        )
        z = hid_ref[...].astype(f32) + (att + vec(V_OB))
        gain1 = vec(V_G1)
        first, unit1, inv1 = norm(z, gain1, vec(V_S1))
        low = first.astype(bf16)
        flT_s[:, rows] = low.T
        branch = None
        for r in range(2):
            for c in range(0, FHALF, FC):
                at = r * FHALF + c
                before = (
                    dot(low, w_ref[r, :, HALF + c : HALF + c + FC])
                    + vec_ref[r, :, V_UB + c : V_UB + c + FC]
                )
                cdf, pdf = gelu_parts(before)
                act = (before * cdf).astype(bf16)
                act_s[rows, at : at + FC] = act
                dg_s[:, at : at + FC] = cdf + before * pdf
                part = dot_nt(act, w_ref[r, :, HALF + FHALF + c : HALF + FHALF + c + FC])
                branch = part if branch is None else branch + part
        gain2 = vec(V_G2)
        output, unit2, inv2 = norm(first + (branch + vec(V_DB)), gain2, vec(V_S2))
        out_ref[...] = output
        cot = cot_ref[...].astype(f32)
        grad2 = norm_back(cot, unit2, inv2, gain2)
        add_vec(V_G2, cot * unit2)
        add_vec(V_S2, cot)
        bgrad = grad2.astype(bf16)
        add_vec(V_DB, bgrad.astype(f32))
        brT_s[:, rows] = bgrad.T
        fgrad = grad2
        for r in range(2):
            for c in range(0, FHALF, FC):
                at = r * FHALF + c
                dact = dot(bgrad, w_ref[r, :, HALF + FHALF + c : HALF + FHALF + c + FC])
                dbef = (dact * dg_s[:, at : at + FC]).astype(bf16)
                bg_s[rows, at : at + FC] = dbef
                vs_ref[r, :, V_UB + c : V_UB + c + FC] += jnp.sum(
                    dbef.astype(f32), axis=0, keepdims=True
                )
                fgrad = fgrad + dot_nt(dbef, w_ref[r, :, HALF + c : HALF + c + FC])
        add_vec(V_G1, fgrad * unit1)
        add_vec(V_S1, fgrad)
        resid = norm_back(fgrad, unit1, inv1, gain1)
        resid_ref[...] = resid
        agrad = resid.astype(bf16)
        add_vec(V_OB, agrad.astype(f32))
        agT_s[:, rows] = agrad.T
        for r in range(2):
            dctx_ref[:, r * HALF : (r + 1) * HALF] = dot(agrad, w_ref[r, :, :HALF]).astype(bf16)

    idx = step - TSTEPS
    r = idx // TILES
    j = idx % TILES

    @pl.when((idx >= 0) & (j == 0))
    def _():
        cols = pl.ds(pl.multiple_of(r * HALF, HALF), HALF)
        dw_ref[0] = dot(agT_s[...], ctx_ref[:, cols]).astype(bf16)

    @pl.when((idx >= 0) & (j >= 1) & (j <= 4))
    def _():
        cols = pl.ds(pl.multiple_of(r * FHALF + (j - 1) * HALF, HALF), HALF)
        dw_ref[0] = dot(flT_s[...], bg_s[:, cols]).astype(bf16)

    @pl.when((idx >= 0) & (j >= 5))
    def _():
        cols = pl.ds(pl.multiple_of(r * FHALF + (j - 5) * HALF, HALF), HALF)
        dw_ref[0] = dot(brT_s[...], act_s[:, cols]).astype(bf16)


def middle(ctx, hid, cot, w, vec):
    def tok(s):
        return (jnp.minimum(s, TSTEPS - 1), 0)

    def tile(s):
        idx = jnp.maximum(s - TSTEPS, 0)
        return (idx // TILES, 0, idx % TILES)

    rows = pl.BlockSpec((TOK, D), tok)
    return pl.pallas_call(
        mid_kernel,
        grid=(TSTEPS + 2 * TILES,),
        in_specs=[
            pl.BlockSpec((LENGTH, D), lambda s: (0, 0), pipeline_mode=pl.Buffered(1)),
            rows,
            rows,
            pl.BlockSpec((2, D, REST_W), lambda s: (0, 0, 0), pipeline_mode=pl.Buffered(1)),
            pl.BlockSpec((2, 1, VEC_W), lambda s: (0, 0, 0), pipeline_mode=pl.Buffered(1)),
        ],
        out_specs=[
            rows,
            rows,
            rows,
            pl.BlockSpec((1, D, HALF), tile),
            pl.BlockSpec((2, 1, VEC_W), lambda s: (0, 0, 0)),
        ],
        out_shape=[
            jax.ShapeDtypeStruct((LENGTH, D), f32),
            jax.ShapeDtypeStruct((LENGTH, D), f32),
            jax.ShapeDtypeStruct((LENGTH, D), bf16),
            jax.ShapeDtypeStruct((2, D, REST_W), bf16),
            jax.ShapeDtypeStruct((2, 1, VEC_W), f32),
        ],
        scratch_shapes=[
            pltpu.VMEM((LENGTH, FF), bf16),
            pltpu.VMEM((LENGTH, FF), bf16),
            pltpu.VMEM((TOK, FF), f32),
            pltpu.VMEM((D, LENGTH), bf16),
            pltpu.VMEM((D, LENGTH), bf16),
            pltpu.VMEM((D, LENGTH), bf16),
        ],
        compiler_params=params(),
        name="middle",
    )(ctx, hid, cot, w, vec)


LTOK = 512
LSTEPS = LENGTH // LTOK


def last_kernel(hid_ref, dq_ref, dk_ref, dv_ref, resid_ref, w_ref, hg_ref, dw_ref, vs_ref, hT_s):
    step = pl.program_id(0)

    @pl.when(step == 0)
    def _():
        hT_s[...] = hid_ref[...].T
        for ref, off in ((dq_ref, 0), (dv_ref, HALF)):
            total = jnp.sum(ref[...].astype(f32), axis=0, keepdims=True)
            vs_ref[0, :, off : off + HALF] = total[:, :HALF]
            vs_ref[1, :, off : off + HALF] = total[:, HALF:]

    @pl.when(step < LSTEPS)
    def _():
        rows = pl.ds(pl.multiple_of(step * LTOK, LTOK), LTOK)
        acc = resid_ref[...]
        for m, ref in enumerate((dq_ref, dk_ref, dv_ref)):
            for r in range(2):
                acc = acc + dot_nt(
                    ref[rows, r * HALF : (r + 1) * HALF],
                    w_ref[r, :, m * HALF : (m + 1) * HALF],
                )
        hg_ref[...] = acc

    idx = step - LSTEPS
    cols = pl.ds(pl.multiple_of(jnp.maximum(idx, 0) // 3 * HALF, HALF), HALF)
    for m, ref in enumerate((dq_ref, dk_ref, dv_ref)):

        @pl.when((idx >= 0) & (idx % 3 == m))
        def _(ref=ref):
            dw_ref[0] = dot(hT_s[...], ref[:, cols]).astype(bf16)


def last(hid, dq, dk, dv, resid, w):
    whole = pl.BlockSpec((LENGTH, D), lambda s: (0, 0), pipeline_mode=pl.Buffered(1))
    rows = pl.BlockSpec((LTOK, D), lambda s: (jnp.minimum(s, LSTEPS - 1), 0))

    def tile(s):
        idx = jnp.maximum(s - LSTEPS, 0)
        return (idx // 3, 0, idx % 3)

    return pl.pallas_call(
        last_kernel,
        grid=(LSTEPS + 6,),
        in_specs=[
            whole,
            whole,
            whole,
            whole,
            rows,
            pl.BlockSpec((2, D, QKV_W), lambda s: (0, 0, 0), pipeline_mode=pl.Buffered(1)),
        ],
        out_specs=[
            rows,
            pl.BlockSpec((1, D, HALF), tile),
            pl.BlockSpec((2, 1, 2 * HALF), lambda s: (0, 0, 0)),
        ],
        out_shape=[
            jax.ShapeDtypeStruct((LENGTH, D), f32),
            jax.ShapeDtypeStruct((2, D, QKV_W), bf16),
            jax.ShapeDtypeStruct((2, 1, 2 * HALF), f32),
        ],
        scratch_shapes=[pltpu.VMEM((D, LENGTH), bf16)],
        compiler_params=params(),
        name="last",
    )(hid, dq, dk, dv, resid, w)


def last_sum_kernel(
    zs, hid_ref, dq_ref, dk_ref, dv_ref, resid_ref, w_ref, h_ref, v_ref,
    hg_ref, o1_ref, o2_ref, vo_ref,
    hT, g, w, resid, vs, mid, local, *scratch,
):
    plane, (v1, v2, v3, v4, va, vb, vsend, vrecv), line1, line2 = (
        scratch[:7],
        scratch[7:15],
        scratch[15:18],
        scratch[18:21],
    )
    at = Place(zs)
    loads = [
        pltpu.make_async_copy(w_ref, w, local.at[0]),
        pltpu.make_async_copy(resid_ref, resid, local.at[1]),
    ]
    start_all(loads)
    greet([at.by_core, at.by_x, at.by_y] + [at.by_z(d) for d in range(1, zs)])
    first = PlaneSum(at, g, None, *plane, None)
    second = LineSum(at, h_ref, *line2)
    second.start()

    hT[...] = hid_ref[...].T
    half = zs // 2

    @pl.loop(0, 2)
    def _(n):
        rows = hT[pl.ds(pl.multiple_of(n * HALF, HALF), HALF), :]
        for r in range(2):
            for m, ref in enumerate((dq_ref, dk_ref, dv_ref)):
                tile = dot(rows, ref[:, r * HALF : (r + 1) * HALF]).astype(bf16)
                g[r, pl.ds(n * half, half), :, :, :, m * HALF : (m + 1) * HALF] = tile.reshape(
                    (half,) + g.shape[2:5] + (HALF,)
                )

    first.stage1()
    vs[...] = v_ref[...]
    for ref, off in ((dq_ref, V_QB), (dv_ref, V_VB)):
        total = jnp.sum(ref[...].astype(f32), axis=0, keepdims=True)
        vs[0, :, off : off + HALF] = total[:, :HALF]
        vs[1, :, off : off + HALF] = total[:, HALF:]
    vec1 = remote(vs, v1, vsend, vrecv, 0, at.by_core)
    vec1.start()
    wait_all(loads)

    def input_grad(n):
        rows = pl.ds(pl.multiple_of(n * QROWS, QROWS), QROWS)
        acc = resid[rows, :]
        for m, ref in enumerate((dq_ref, dk_ref, dv_ref)):
            for r in range(2):
                acc = acc + dot_nt(
                    ref[rows, r * HALF : (r + 1) * HALF], w[r, :, m * HALF : (m + 1) * HALF]
                )
        hg_ref[rows, :] = acc

    tiles = LENGTH // QROWS
    pl.loop(0, tiles // 2)(input_grad)
    vec1.wait()
    va[...] = vs[...] + v1[...]
    vec2 = remote(va, v2, vsend, vrecv, 1, at.by_x)
    vec2.start()
    for i in range(first.chunks):
        first.stage2(i)
    pl.loop(tiles // 2, tiles)(input_grad)
    vec2.wait()
    vb[...] = va[...] + v2[...]
    vec3 = remote(vb.at[1 - at.y], v3, vsend, vrecv, 2, at.by_y)
    vec3.start()
    for i in range(first.chunks):
        first.stage3(i)
    vec3.wait()
    v4[0] = vb[at.y] + v3[...]
    vec4 = [
        remote(v4.at[0], v4.at[d], vsend, vrecv, 2 + d, at.by_z(d)) for d in range(1, zs)
    ]
    start_all(vec4)
    second.finish(o2_ref)
    for i in range(first.chunks):
        first.finish(i, mid)
    third = LineSum(at, mid, *line1)
    third.start()
    wait_all(vec4)
    total = v4[at.z % zs]
    for z in range(1, zs):
        total = total + v4[(at.z + zs - z) % zs]
    vo_ref[...] = total
    third.finish(o1_ref)


def last_sum(zs, hid, dq, dk, dv, resid, w, h, v):
    rows = D // (4 * zs)
    w1 = w.shape[2]
    w2 = h.shape[2]
    width = v.shape[2]
    vmem = pl.BlockSpec(memory_space=pltpu.VMEM)
    far = pl.BlockSpec(memory_space=pl.ANY)
    return pl.pallas_call(
        functools.partial(last_sum_kernel, zs),
        in_specs=[vmem, vmem, vmem, vmem, far, far, vmem, vmem],
        out_specs=[vmem] * 4,
        out_shape=[
            jax.ShapeDtypeStruct((LENGTH, D), f32),
            jax.ShapeDtypeStruct((rows, w1), f32),
            jax.ShapeDtypeStruct((rows, w2), f32),
            jax.ShapeDtypeStruct((1, width), f32),
        ],
        scratch_shapes=[
            pltpu.VMEM((D, LENGTH), bf16),
            pltpu.VMEM((2, zs, 2, 2, rows, w1), bf16),
            pltpu.VMEM(w.shape, bf16),
            pltpu.VMEM((LENGTH, D), f32),
            pltpu.VMEM((2, 1, width), f32),
            pltpu.VMEM((zs, rows, w1), bf16),
            pltpu.SemaphoreType.DMA((2,)),
            *plane_scratch(zs, rows, w1)[1:-1],
            pltpu.VMEM((2, 1, width), f32),
            pltpu.VMEM((2, 1, width), f32),
            pltpu.VMEM((1, width), f32),
            pltpu.VMEM((zs, 1, width), f32),
            pltpu.VMEM((2, 1, width), f32),
            pltpu.VMEM((2, 1, width), f32),
            pltpu.SemaphoreType.DMA((zs + 2,)),
            pltpu.SemaphoreType.DMA((zs + 2,)),
            *line_scratch(zs, rows, w1),
            *line_scratch(zs, rows, w2),
        ],
        compiler_params=params(collective_id=1, has_side_effects=True),
        name="last_sum",
    )(hid, dq, dk, dv, resid, w, h, v)


def gather_parts(parts, rows_n, cols_n):
    packed = jnp.concatenate(parts, axis=1)
    every = lax.all_gather(packed, ("row", "col"), axis=0, tiled=True)
    every = every.reshape(rows_n, D, packed.shape[1])
    if rows_n == 2:
        return every
    pieces, at = [], 0
    for part in parts:
        width = part.shape[1]
        one = every[:, :, at : at + width].reshape(2, rows_n // 2, D, width)
        pieces.append(one.transpose(0, 2, 1, 3).reshape(2, D, rows_n // 2 * width))
        at += width
    return jnp.concatenate(pieces, axis=2)


def scatter_parts(full, halves, rows_n, cols_n):
    widths = [h * 2 // rows_n for h in halves]
    if rows_n != 2:
        pieces, at = [], 0
        for half, width in zip(halves, widths):
            one = full[:, :, at : at + half].reshape(2, D, rows_n // 2, width)
            pieces.append(one.transpose(0, 2, 1, 3).reshape(rows_n, D, width))
            at += half
        full = jnp.concatenate(pieces, axis=2)
    flat = full.reshape(rows_n * D, sum(widths))
    mine = lax.psum_scatter(flat, ("row", "col"), scatter_dimension=0, tiled=True)
    mine = mine.astype(f32)
    out, at = [], 0
    for width in widths:
        out.append(mine[:, at : at + width])
        at += width
    return out


VEC_HALVES = (HALF, HALF, HALF, FHALF, HALF, HALF, HALF, HALF, HALF)


def on_device(
    rows_n,
    cols_n,
    hidden,
    cotangent,
    rand_blocks,
    w_query,
    w_key,
    w_value,
    w_out,
    w_up,
    w_down,
    *vectors,
):
    zs = cols_n // 4
    staged = rows_n == 2 and cols_n % 8 == 0
    hide = hidden_pairs(rand_blocks[0])
    if staged:
        weights = (w_query, w_key, w_value, w_out.T, w_up, w_down.T)
        q, k, v, w1, h2, vec = front(zs, hidden, weights, vectors)
        ctx, p, w2 = attend(q, k, v, hide, zs, h2)
        w1, w2 = w1.reshape(2, D, QKV_W), w2.reshape(2, D, REST_W)
    else:
        vec = lax.all_gather(jnp.concatenate(vectors).astype(f32), "row", axis=0, tiled=False)
        if rows_n != 2:
            pieces, at = [], 0
            for half in VEC_HALVES:
                width = half * 2 // rows_n
                pieces.append(vec[:, at : at + width].reshape(2, half))
                at += width
            vec = jnp.concatenate(pieces, axis=1)
        vec = vec.reshape(2, 1, VEC_W)
        w1 = gather_parts([w_query, w_key, w_value], rows_n, cols_n)
        w2 = gather_parts([w_out.T, w_up, w_down.T], rows_n, cols_n)
        q, k, v = qkv(hidden, w1, vec)
        ctx, p = attend(q, k, v, hide)
    output, resid, dctx, dw2, vs2 = middle(ctx, hidden, cotangent, w2, vec)
    if staged:
        g2 = dw2.reshape(2, zs, 2, 2, D // cols_n, REST_W)
        dq, dk, dv, h2 = attend_back(q, k, v, dctx, p, zs, g2)
        hgrad, m1, m2, vs = last_sum(zs, hidden, dq, dk, dv, resid, w1, h2, vs2)
        g_q, g_k, g_v = (m1[:, n * HALF : (n + 1) * HALF] for n in range(3))
        g_out = m2[:, :HALF].T
        g_up = m2[:, HALF : HALF + FHALF]
        g_down = m2[:, HALF + FHALF :].T
        sums, at = [], 0
        for width in VEC_HALVES:
            sums.append(vs[0, at : at + width])
            at += width
        return (output, hgrad, g_q, g_k, g_v, g_out, g_up, g_down, *sums)
    dq, dk, dv = attend_back(q, k, v, dctx, p)
    hgrad, dw1, vs1 = last(hidden, dq, dk, dv, resid, w1)
    vs = jnp.concatenate([vs1, vs2[:, :, 2 * HALF :]], axis=2)
    g_out, g_up, g_down = scatter_parts(dw2, (HALF, FHALF, FHALF), rows_n, cols_n)
    g_q, g_k, g_v = scatter_parts(dw1, (HALF, HALF, HALF), rows_n, cols_n)
    vs = lax.psum(vs.reshape(2, VEC_W), ("col", "row"))
    row = lax.axis_index("row")
    sums, at = [], 0
    for half in VEC_HALVES:
        width = half * 2 // rows_n
        both = vs[:, at : at + half].reshape(rows_n, width)
        sums.append(lax.dynamic_index_in_dim(both, row, 0, keepdims=False))
        at += half
    return (output, hgrad, g_q, g_k, g_v, g_out.T, g_up, g_down.T, *sums)


def solution(mesh):
    rows_n, cols_n = mesh.shape["row"], mesh.shape["col"]
    tokens = P(("col", "row"), None)
    placed = (
        tokens,
        tokens,
        P(("col", "row"), None, None, None),
        P("col", "row"),
        P("col", "row"),
        P("col", "row"),
        P("row", "col"),
        P("col", "row"),
        P("row", "col"),
    ) + (P("row"),) * 9
    return jax.shard_map(
        functools.partial(on_device, rows_n, cols_n),
        mesh=mesh,
        in_specs=placed,
        out_specs=(
            tokens,
            tokens,
            P("col", "row"),
            P("col", "row"),
            P("col", "row"),
            P("row", "col"),
            P("col", "row"),
            P("row", "col"),
        )
        + (P("row"),) * 9,
        check_vma=False,
    )
```
